256 devices in a mesh: grid: 32 (over z, y), atom: 8 (over x, core).
Axes of the slice: x: 4, y: 4, z: 8, core: 2. Of those that a mesh axis runs over, the one named last changes fastest.
Arguments:
- weights: float32 [4194304], P(('grid', 'atom')), may hold values from 0.25 to 4
- target: float32 [4194304], P(('grid', 'atom')), may hold values from -6 to 6
- coupling: float32 [4194304], P(('grid', 'atom')), may hold values from -0.9 to 0.9
- multipole_basis: float32 [25, 4194304], P(None, ('grid', 'atom')), may hold values from -6 to 6
- rho_hist: float32 [8, 4194304], P(None, ('grid', 'atom')), may hold values from -6 to 6
- res_hist: float32 [8, 4194304], P(None, ('grid', 'atom')), may hold values from -6 to 6
- batch_atom: int32 [16384], P(('grid', 'atom')), may hold values from 0 to 4095
- owner_slot: int32 [4096], replicated, may hold values from 0 to 4095, each once
- slot_index: int32 [2], replicated, may hold values from 0 to 7
Outputs:
- density: float32 [4194304], P(('grid', 'atom'))
- moments: float32 [25, 4096], P(None, 'atom')
The draws below stay inside these ranges and needn't reach their ends.
Inputs may be any that keep to these rules, and one draw needn't show every extreme that they name: `owner_slot`: each slot 0 to 4095 belongs to exactly one atom.
All inputs are finite; a program needn't handle non-finite values.
Results may differ from the reference program's by a relative error of at most 0.00011.
Values sent between devices are 32-bit elements; how exact they have to be, the bound alone decides.
A program may use at most 64 MiB of HBM per device.

```python
import math
import jax
import jax.numpy as jnp
import numpy as np
from jax import lax

H = 8
LM = 25
BATCH = 256
ITERS = 2
POINTS = 4194304
BATCHES = 16384
ATOMS = 4096
ATOM_PTS = 1024


def place_ends(result, key, least, largest):
    spot = [jax.random.randint(jax.random.fold_in(key, axis), (), 0, length) for axis, length in enumerate(result.shape)]
    longest = result.shape.index(max(result.shape))
    neighbour = spot[:longest] + [(spot[longest] + 1) % result.shape[longest]] + spot[longest + 1:]
    return result.at[tuple(spot)].set(least).at[tuple(neighbour)].set(largest)


def levels(own_key, dims, pieces, smallest, top_value):
    def one(position, shards_of):
        heights = jax.random.uniform(jax.random.fold_in(jax.random.fold_in(own_key, 6), position), (shards_of,), jnp.float32, smallest / len(pieces), top_value / len(pieces))
        return jnp.repeat(jnp.exp(heights), dims[position] // shards_of).reshape((-1,) + (1,) * (len(dims) - position - 1))

    gain = one(*pieces[0])
    for cut in pieces[1:]:
        gain = gain * one(*cut)
    return gain


def noise(stream_key, shape, scale, reach, shards=(), held_as=jnp.bfloat16):
    gain = levels(stream_key, shape, shards, -0.22, 0.18) if shards else 1.0
    entries = jax.random.normal(stream_key, shape, jnp.float32) * scale * gain
    return jnp.minimum(jnp.maximum(entries, -reach), reach).astype(held_as)


def setup_inputs(seed: int = 0) -> dict:
    splits = jax.random.split(jax.random.key(seed), 10)
    return {
        "weights": jnp.clip(jnp.exp(math.log(4.0) - 2.7725887 * jax.random.uniform(splits[0], (POINTS,), jnp.float32) ** levels(splits[0], (POINTS,), ((0, 256),), -0.2, 0.2)), 0.25, 4.0),
        "target": noise(splits[1], (POINTS,), 1.0, 6.0, ((0, 256),), jnp.float32),
        "coupling": jnp.clip(jax.random.uniform(splits[2], (POINTS,), jnp.float32, -0.9, 0.9) * levels(splits[2], (POINTS,), ((0, 256),), -0.4, 0.0), -0.9, 0.9),
        "multipole_basis": noise(splits[3], (LM, POINTS), 1.0, 6.0, ((1, 256),), jnp.float32),
        "rho_hist": noise(splits[4], (H, POINTS), 1.0, 6.0, ((1, 256),), jnp.float32),
        "res_hist": noise(splits[5], (H, POINTS), 1.0, 6.0, ((1, 256),), jnp.float32),
        "batch_atom": place_ends(jax.random.randint(splits[6], (BATCHES,), 0, ATOMS), jax.random.fold_in(splits[6], 1), 0, ATOMS - 1).astype(jnp.int32),
        "owner_slot": jax.random.permutation(splits[7], ATOMS).astype(jnp.int32),
        "slot_index": jax.random.randint(splits[8], (ITERS,), 0, H).astype(jnp.int32),
    }


damping_table = np.array([1.0 / (1 + degree) for degree in range(5) for order in range(2 * degree + 1)], dtype=np.float32)
mixing_beta = 0.5
ridge_share = 0.1

def mixing_weights(intersect):
    hist_len = intersect.shape[0]
    ridge_val = ridge_share * jnp.trace(intersect) / hist_len
    shifted = intersect + ridge_val * jnp.eye(hist_len, dtype=intersect.dtype)
    factor = jnp.linalg.cholesky(shifted)
    forward = []
    for row_at in range(hist_len):
        entry_val = 1.0
        for col_at in range(row_at):
            entry_val = entry_val - factor[row_at, col_at] * forward[col_at]
        forward.append(entry_val / factor[row_at, row_at])
    backward = [None] * hist_len
    for row_at in reversed(range(hist_len)):
        entry_val = forward[row_at]
        for col_at in range(row_at + 1, hist_len):
            entry_val = entry_val - factor[col_at, row_at] * backward[col_at]
        backward[row_at] = entry_val / factor[row_at, row_at]
    solved = jnp.stack(backward)
    return solved / jnp.sum(solved)

def reference(weights, target, coupling, multipole_basis, rho_hist, res_hist, batch_atom, owner_slot, slot_index):
    hi_prec = lax.Precision.HIGHEST
    damping = jnp.asarray(damping_table, dtype=weights.dtype)
    batch_slot = owner_slot[batch_atom].astype(jnp.int32)
    basis_blocks = multipole_basis.reshape(LM, BATCHES, BATCH)
    density = None
    moments = None
    for iteration in range(ITERS):
        intersect = jnp.dot(res_hist * weights[None, :], res_hist.T, precision=hi_prec)
        coeffs = mixing_weights(intersect)
        rho_mix = jnp.dot(coeffs, rho_hist, precision=hi_prec)
        res_mix = jnp.dot(coeffs, res_hist, precision=hi_prec)
        per_batch = lax.optimization_barrier(jnp.sum((weights * res_mix).reshape(1, BATCHES, BATCH) * basis_blocks, axis=2))
        moments = jax.ops.segment_sum(per_batch.T, batch_slot, num_segments=ATOMS).T / jnp.sqrt(jnp.float32(ATOM_PTS)).astype(weights.dtype)
        at_batch = damping[:, None] * moments[:, batch_slot]
        correct = lax.optimization_barrier(jnp.sum(at_batch[:, :, None] * basis_blocks, axis=0)).reshape(POINTS)
        density = rho_mix + mixing_beta * (res_mix - correct)
        res_new = target + coupling * jnp.tanh(density) - density
        where = slot_index[iteration]
        rho_hist = rho_hist.at[where].set(density)
        res_hist = res_hist.at[where].set(res_new)
    return (density, moments)
```

```python
import functools
import math

import jax
import jax.numpy as jnp
from jax import lax
from jax.experimental import pallas as pl
from jax.experimental.pallas import tpu as pltpu
from jax.sharding import PartitionSpec as P

MESH = pl.DeviceIdType.MESH
LANES = 128
SUBS = 8
mixing_beta = 0.5
ridge_share = 0.1
F32 = jnp.float32


def solve_coeffs(entry, hist_len):
    trace = entry[0][0]
    for i in range(1, hist_len):
        trace = trace + entry[i][i]
    ridge = (ridge_share / hist_len) * trace
    low = [[entry[i][j] for j in range(i + 1)] for i in range(hist_len)]
    for i in range(hist_len):
        low[i][i] = low[i][i] + ridge
    inverse = [None] * hist_len
    factor = [[None] * hist_len for _ in range(hist_len)]
    forward = [jnp.ones_like(trace) for _ in range(hist_len)]
    for j in range(hist_len):
        inverse[j] = 1.0 / low[j][j]
        for i in range(j + 1, hist_len):
            factor[i][j] = low[i][j] * inverse[j]
        for i in range(j + 1, hist_len):
            forward[i] = forward[i] - factor[i][j] * forward[j]
            for k in range(j + 1, i + 1):
                low[i][k] = low[i][k] - factor[i][j] * low[k][j]
    backward = [forward[i] * inverse[i] for i in range(hist_len)]
    for j in reversed(range(hist_len)):
        for i in range(j):
            backward[i] = backward[i] - factor[j][i] * backward[j]
    total = backward[0]
    for i in range(1, hist_len):
        total = total + backward[i]
    return [backward[i] / total for i in range(hist_len)]


def split(x):
    pieces = []
    for _ in range(3):
        piece = x.astype(jnp.bfloat16).astype(F32)
        pieces.append(piece)
        x = x - piece
    return pieces


def kernel(
    cfg,
    batch_atom,
    owner_slot,
    slot_index,
    w_hbm,
    target_hbm,
    coupling_hbm,
    basis_hbm,
    rho_hbm,
    res_hbm,
    density_out,
    moments_out,
    w,
    target,
    coupling,
    basis,
    rho,
    res,
    fresh,
    fresh_w,
    stack_rows,
    plane_rows,
    stack_moments,
    part_send,
    part_recv,
    own_send,
    own_recv,
    chunks,
    source_cols,
    mask,
    hist_moments,
    base_rows,
    correct,
    load_sem,
    send_sem,
    recv_sem,
):
    iters, hist_len, harmonics, batches, width, owned, planes, lines, members, scale = cfg
    tiles = w.shape[0]
    per_batch = width // LANES
    half = LANES // 2
    rows = batches // 4
    plane = lines * members
    near_lanes = plane * batches
    shares = chunks.shape[0]
    depth = shares // lines
    share = owned // shares
    my_group = lax.axis_index("grid")
    my_member = lax.axis_index("atom")
    my_plane = lax.div(my_group, lines)
    my_line = lax.rem(my_group, lines)
    spot = my_line * members + my_member
    my_share = my_line * depth + lax.rem(my_plane, depth)

    def in_stack(at):
        return at * lines + my_line, my_member

    def in_plane(at):
        return my_plane * lines + lax.div(at, members), lax.rem(at, members)

    def in_shares(at):
        return (lax.div(my_plane, depth) * depth + lax.rem(at, depth)) * lines + lax.div(at, depth), my_member

    groups = ((planes, my_plane, in_stack), (plane, spot, in_plane), (shares, my_share, in_shares))
    barrier = pltpu.get_barrier_semaphore()
    for count, mine, where in groups:

        @pl.loop(1, count)
        def _(step):
            pl.semaphore_signal(barrier, inc=1, device_id=where(lax.rem(mine + step, count)), device_id_type=MESH)

    loads = [
        pltpu.make_async_copy(src, dst, load_sem.at[k])
        for k, (src, dst) in enumerate(
            ((res_hbm, res), (w_hbm, w), (basis_hbm, basis), (rho_hbm, rho), (target_hbm, target), (coupling_hbm, coupling))
        )
    ]
    for load in loads:
        load.start()

    lane = lax.broadcasted_iota(jnp.int32, (SUBS, LANES), 1)
    sub = lax.broadcasted_iota(jnp.int32, (SUBS, LANES), 0)
    quarter = lane // 32
    lane_row = lax.broadcasted_iota(jnp.int32, (1, LANES), 1)
    low_row = lane_row < half
    low = lax.broadcasted_iota(jnp.int32, (2 * SUBS, LANES), 1) < half

    slot_row = jnp.zeros((1, LANES), F32)
    for b in range(batches):
        slot_row = jnp.where(lane_row == half + b, owner_slot[batch_atom[b]].astype(F32), slot_row)

    def lane_tile(t):
        return pl.ds(pl.multiple_of(t * LANES, LANES), LANES)

    def copy_to(src, dst, which, group, target_at, source_at):
        return pltpu.make_async_remote_copy(
            src_ref=src,
            dst_ref=dst,
            send_sem=send_sem.at[which, target_at],
            recv_sem=recv_sem.at[which, source_at],
            device_id=groups[group][2](target_at),
            device_id_type=MESH,
        )

    def exchange(buf, which, group):
        count, mine, _ = groups[group]

        @pl.loop(1, count)
        def _(step):
            copy_to(buf.at[mine], buf.at[mine], which, group, lax.rem(mine + step, count), mine).start()

        return waiter(buf, buf, which, group)

    def waiter(src, dst, which, group):
        count, mine, _ = groups[group]

        def wait():
            @pl.loop(1, count)
            def _(step):
                at = lax.rem(mine + step, count)
                copy_to(src.at[at], dst.at[at], which, group, at, at).wait_recv()

            @pl.loop(1, count)
            def _(step):
                at = lax.rem(mine + step, count)
                copy_to(src.at[at], dst.at[at], which, group, at, at).wait_send()

        return wait

    def tree(parts):
        parts = list(parts)
        while len(parts) > 1:
            parts = [parts[k] + parts[k + 1] if k + 1 < len(parts) else parts[k] for k in range(0, len(parts), 2)]
        return parts[0]

    def total(buf, count):
        return tree(buf[k] for k in range(count))

    def splat(row, k):
        return jnp.broadcast_to(row[:, k : k + 1], (1, LANES))

    def weigh(first, last):
        @pl.loop(first, last)
        def _(r):
            xs, ys = [], []
            for q in range(4):
                b = q * rows + r
                at = pl.ds(pl.multiple_of(b * width, width), width)
                gain = jnp.concatenate([w[pl.ds(b * per_batch + v, 1), :] for v in range(per_batch)], axis=1)
                xs.extend(split(res[:, at] * gain))
                ys.append(jnp.concatenate([basis[0:24, at], jnp.broadcast_to(basis[24:25, at], (SUBS, width))], axis=0))
            x = jnp.concatenate(xs, axis=0).astype(jnp.bfloat16)
            out = None
            for y in split(jnp.concatenate(ys, axis=0)):
                part = lax.dot_general(
                    x, y.astype(jnp.bfloat16), (((1,), (1,)), ((), ())), preferred_element_type=F32
                )
                out = part if out is None else out + part
            tile = jnp.zeros((SUBS, LANES), F32)
            for q in range(4):
                block = out[24 * q : 24 * q + 8] + out[24 * q + 8 : 24 * q + 16] + out[24 * q + 16 : 24 * q + 24]
                tile = jnp.where(quarter == q, block, tile)
            hist_moments[r] = tile

    shifts = hist_len // 2 + 1
    entry = None
    per_iter = 4
    for iteration in range(iters):
        stack_row = stack_rows.at[iteration]
        plane_row = plane_rows.at[iteration]
        stack_moment = stack_moments.at[iteration]
        sent = part_send.at[iteration]
        received = part_recv.at[iteration]
        which = per_iter * iteration
        last = iteration == iters - 1

        if iteration == 0:
            loads[0].wait()
            loads[1].wait()

            def gram(step, acc):
                acc = list(acc)
                for u in range(8):
                    t = step * 8 + u
                    x = res[:, lane_tile(t)]
                    y = x * w[pl.ds(t, 1), :]
                    for r in range(shifts):
                        acc[r] = acc[r] + y * (pltpu.roll(x, r, 0) if r else x)
                return tuple(acc)

            acc = lax.fori_loop(0, tiles // 8, gram, tuple(jnp.zeros((SUBS, LANES), F32) for _ in range(shifts)))
            packed = jnp.zeros((SUBS, LANES), F32)
            for r in range(shifts):
                packed = jnp.where(lane == hist_len * r + sub, jnp.sum(acc[r], axis=1, keepdims=True), packed)
            stack_row[pl.ds(my_plane, 1)] = (jnp.sum(packed, axis=0, keepdims=True) + slot_row)[None]
            pl.semaphore_wait(barrier, sum(count - 1 for count, _, _ in groups))
        else:
            slot = slot_index[iteration - 1]
            replaced = sub == slot

            def refresh(step, acc):
                for u in range(8):
                    t = step * 8 + u
                    new_res = jnp.where(replaced, fresh[pl.ds(t, 1), :], res[:, lane_tile(t)])
                    new_rho = jnp.where(replaced, density_out[pl.ds(t, 1), :], rho[:, lane_tile(t)])
                    res[:, lane_tile(t)] = new_res
                    rho[:, lane_tile(t)] = new_rho
                    acc = acc + fresh_w[pl.ds(t, 1), :] * new_res
                return acc

            acc = lax.fori_loop(0, tiles // 8, refresh, jnp.zeros((SUBS, LANES), F32))
            packed = jnp.where(lane == sub, jnp.sum(acc, axis=1, keepdims=True), 0.0)
            stack_row[pl.ds(my_plane, 1)] = jnp.sum(packed, axis=0, keepdims=True)[None]
        wait = exchange(stack_row, which, 0)

        if iteration == 0:
            loads[2].wait()
        weigh(0, rows // 2)

        wait()
        plane_row[pl.ds(spot, 1)] = jnp.where(low_row, total(stack_row, planes), slot_row)[None]
        wait = exchange(plane_row, which + 1, 1)

        if iteration == 0:
            ids = jnp.concatenate([stack_row[k] for k in range(planes)] * (LANES // planes), axis=0)
            ids = jnp.transpose(ids)
            for k in range(planes):
                source_cols[k * batches : (k + 1) * batches] = jnp.broadcast_to(
                    ids[half : half + batches, k : k + 1], (batches, LANES)
                )
        weigh(rows // 2, rows)

        wait()
        row = total(plane_row, plane)
        if iteration == 0:
            entry = [[None] * (i + 1) for i in range(hist_len)]
            for i in range(hist_len):
                for j in range(i + 1):
                    r = i - j
                    at = hist_len * r + i if r < shifts else hist_len * (hist_len - r) + j
                    entry[i][j] = splat(row, at)
        else:
            news = [splat(row, k) for k in range(hist_len)]
            slot_vec = jnp.zeros((1, LANES), jnp.int32) + slot
            entry = [
                [
                    jnp.where(slot_vec == i, news[j], jnp.where(slot_vec == j, news[i], entry[i][j]))
                    for j in range(i + 1)
                ]
                for i in range(hist_len)
            ]
        coeffs = solve_coeffs(entry, hist_len)
        coeff_col = jnp.zeros((SUBS, LANES), F32)
        for i in range(hist_len):
            coeff_col = jnp.where(sub == i, coeffs[i], coeff_col)

        mixed = jnp.concatenate(
            [jnp.sum(coeff_col * hist_moments[r], axis=0, keepdims=True) for r in range(rows)], axis=0
        )
        turned = jnp.concatenate(
            [
                pltpu.roll(mixed, (LANES - 32 * q - 16 * h) % LANES, 1) if q + h else mixed
                for h in range(2)
                for q in range(4)
            ],
            axis=0,
        )
        stack_moment[pl.ds(my_plane, 1)] = jnp.transpose(turned)[0 : 2 * SUBS][None]
        wait = exchange(stack_moment, which + 2, 0)

        if iteration == 0:

            def fill(lanes, wanted):
                for k in range(mask.shape[0] // (2 * SUBS)):
                    at = slice(2 * SUBS * k, 2 * SUBS * (k + 1))
                    mask[at, lanes] = jnp.where(source_cols[at] == wanted, 1.0, 0.0).astype(jnp.bfloat16)

            @pl.loop(0, near_lanes // LANES)
            def _(t):
                pair = jnp.where(low_row, pltpu.roll(plane_row[2 * t], half, 1), plane_row[2 * t + 1])
                fill(lane_tile(t), pair)

            @pl.loop(0, plane * share // LANES)
            def _(t):
                at = t * (LANES // share) + lane_row // share
                held = (at % members) * owned + ((at // members) * depth + lax.rem(my_plane, depth)) * share
                fill(lane_tile(t + near_lanes // LANES), (held + lane_row % share).astype(F32))

            for load in loads[3:]:
                load.wait()

        def base_step(step, carry):
            for u in range(8):
                t = step * 8 + u
                part = coeff_col * (rho[:, lane_tile(t)] + mixing_beta * res[:, lane_tile(t)])
                base_rows[pl.ds(t, 1), :] = jnp.sum(part, axis=0, keepdims=True)
            return carry

        lax.fori_loop(0, tiles // 8, base_step, 0)
        wait()

        blocks = []
        for k in range(0, planes, 2):
            one, two = stack_moment[k], stack_moment[k + 1]
            upper = jnp.where(low, one, pltpu.roll(two, half, 1))
            lower = jnp.where(low, pltpu.roll(one, half, 1), two)
            blocks.append(jnp.concatenate([upper, lower], axis=0))
        everywhere = jnp.concatenate(blocks, axis=1)
        pieces = jnp.concatenate(split(everywhere), axis=0).astype(jnp.bfloat16)

        def gathered(first, count):
            out = jnp.dot(
                pieces, mask[:, pl.ds(pl.multiple_of(first, count), count)], preferred_element_type=F32
            )
            return out[0:32] + out[32:64] + out[64:96]

        quad = 4

        @pl.loop(0, plane // quad)
        def _(step):
            first = lax.rem(lax.div(spot, quad) + step, plane // quad) * quad
            out = gathered(first * batches, quad * batches)
            for k in range(0, quad, 2):
                upper = out[0:16, k * batches : (k + 2) * batches]
                lower = out[16:32, k * batches : (k + 2) * batches]
                sent[first + k] = jnp.where(low, upper, pltpu.roll(lower, half, 1))
                sent[first + k + 1] = jnp.where(low, pltpu.roll(upper, half, 1), lower)
            for k in range(quad):

                @pl.when(first + k != spot)
                def _():
                    copy_to(sent.at[first + k], received.at[spot], which + 3, 1, first + k, spot).start()

        received[pl.ds(spot, 1)] = sent[pl.ds(spot, 1)]
        wait = waiter(sent, received, which + 3, 1)

        if last:
            many = 2 * LANES // share
            each = LANES // share

            @pl.loop(0, plane // many)
            def _(step):
                first = lax.rem(lax.div(spot, many) + step, plane // many) * many
                out = gathered(near_lanes + first * share, many * share)
                for k in range(many):
                    tile = out[:, k // each * LANES : (k // each + 1) * LANES]
                    kept = jnp.zeros((SUBS, LANES), F32)
                    for g in range(4):
                        piece = tile[g * SUBS : (g + 1) * SUBS]
                        turn = (g - k % each) * 32 % LANES
                        kept = jnp.where(quarter == g, pltpu.roll(piece, turn, 1) if turn else piece, kept)
                    own_send[first + k] = kept
                for k in range(many):

                    @pl.when(first + k != spot)
                    def _():
                        copy_to(own_send.at[first + k], own_recv.at[spot], per_iter * iters, 1, first + k, spot).start()

            own_recv[pl.ds(spot, 1)] = own_send[pl.ds(spot, 1)]
            own_wait = waiter(own_send, own_recv, per_iter * iters, 1)

        wait()
        summed = total(received, plane)
        at_batch = jnp.concatenate([summed, pltpu.roll(summed, half, 1)], axis=0) * scale
        if last:
            own_wait()
            chunks[pl.ds(my_share, 1)] = (total(own_recv, plane) * scale)[None]
            own_wait = exchange(chunks, per_iter * iters + 1, 2)

        comp = lax.broadcasted_iota(jnp.int32, (32, LANES), 0)
        degree = sum((comp >= (l + 1) * (l + 1)).astype(F32) for l in range(4))
        damped = jnp.where(comp < harmonics, at_batch * (mixing_beta / (1.0 + degree)), 0.0)

        def density_step(step, ahead):
            for u in range(16):
                b = step * 16 + u
                col = jnp.broadcast_to(ahead[:, u : u + 1], (32, LANES))
                for v in range(per_batch):
                    t = b * per_batch + v
                    part = col[24:32] * basis[24:25, lane_tile(t)]
                    for g in range(3):
                        part = part + col[g * SUBS : (g + 1) * SUBS] * basis[g * SUBS : (g + 1) * SUBS, lane_tile(t)]
                    correct[pl.ds(t, 1), :] = jnp.sum(part, axis=0, keepdims=True)
            return pltpu.roll(ahead, LANES - 16, 1)

        lax.fori_loop(0, batches // 16, density_step, damped)
        density = base_rows[...] - correct[...]
        density_out[...] = density
        if last:
            own_wait()
            each = LANES // share
            for t in range(owned // LANES):
                held = [chunks[t * each + k] for k in range(each)]
                for g in range(4):
                    tile = jnp.zeros((SUBS, LANES), F32)
                    for k in range(each):
                        turn = (k - g) * 32 % LANES
                        tile = jnp.where(quarter == k, pltpu.roll(held[k], turn, 1) if turn else held[k], tile)
                    top = min(SUBS, harmonics - g * SUBS)
                    moments_out[g * SUBS : g * SUBS + top, t * LANES : (t + 1) * LANES] = tile[0:top]
        else:
            new = target[...] + coupling[...] * jnp.tanh(density) - density
            fresh[...] = new
            fresh_w[...] = new * w[...]


def finish(density, moments, density_out, moments_out):
    density_out[...] = density[...]
    moments_out[...] = moments[...]


def local(weights, target, coupling, multipole_basis, rho_hist, res_hist, batch_atom, owner_slot, slot_index):
    harmonics, points = multipole_basis.shape
    hist_len = res_hist.shape[0]
    batches = batch_atom.shape[0]
    groups = lax.axis_size("grid")
    members = lax.axis_size("atom")
    lines = 4
    planes = groups // lines
    plane = lines * members
    shares = 4 * lines
    owned = owner_slot.shape[0] // members
    scale = 1.0 / math.sqrt(points * groups // owned)
    iters = slot_index.shape[0]
    cfg = (iters, hist_len, harmonics, batches, points // batches, owned, planes, lines, members, scale)
    tiles = points // LANES
    flat = (tiles, LANES)
    any_space = pl.BlockSpec(memory_space=pl.ANY)
    smem = pl.BlockSpec(memory_space=pltpu.SMEM)
    vmem = pl.BlockSpec(memory_space=pltpu.VMEM)
    density, moments = pl.pallas_call(
        functools.partial(kernel, cfg),
        out_shape=(jax.ShapeDtypeStruct(flat, F32), jax.ShapeDtypeStruct((harmonics, owned), F32)),
        in_specs=[smem] * 3 + [any_space] * 6,
        out_specs=(vmem, vmem),
        scratch_shapes=[
            pltpu.VMEM(flat, F32),
            pltpu.VMEM(flat, F32),
            pltpu.VMEM(flat, F32),
            pltpu.VMEM((harmonics, points), F32),
            pltpu.VMEM((hist_len, points), F32),
            pltpu.VMEM((hist_len, points), F32),
            pltpu.VMEM(flat, F32),
            pltpu.VMEM(flat, F32),
            pltpu.VMEM((iters, planes, 1, LANES), F32),
            pltpu.VMEM((iters, plane, 1, LANES), F32),
            pltpu.VMEM((iters, planes, 2 * SUBS, LANES), F32),
            pltpu.VMEM((iters, plane, 2 * SUBS, LANES), F32),
            pltpu.VMEM((iters, plane, 2 * SUBS, LANES), F32),
            pltpu.VMEM((plane, SUBS, LANES), F32),
            pltpu.VMEM((plane, SUBS, LANES), F32),
            pltpu.VMEM((shares, SUBS, LANES), F32),
            pltpu.VMEM((planes * batches, LANES), F32),
            pltpu.VMEM((planes * batches, plane * (batches + owned // shares)), jnp.bfloat16),
            pltpu.VMEM((batches // 4, SUBS, LANES), F32),
            pltpu.VMEM(flat, F32),
            pltpu.VMEM(flat, F32),
            pltpu.SemaphoreType.DMA((6,)),
            pltpu.SemaphoreType.DMA((4 * iters + 2, plane)),
            pltpu.SemaphoreType.DMA((4 * iters + 2, plane)),
        ],
        compiler_params=pltpu.CompilerParams(
            collective_id=0, has_side_effects=True, vmem_limit_bytes=67043328
        ),
    )(
        batch_atom,
        owner_slot,
        slot_index,
        weights.reshape(flat),
        target.reshape(flat),
        coupling.reshape(flat),
        multipole_basis,
        rho_hist,
        res_hist,
    )
    density, moments = pl.pallas_call(
        finish,
        out_shape=(jax.ShapeDtypeStruct(flat, F32), jax.ShapeDtypeStruct((harmonics, owned), F32)),
        in_specs=[vmem] * 2,
        out_specs=(vmem, vmem),
    )(density, moments)
    return density.reshape(points), moments


def solution(mesh):
    both = ("grid", "atom")
    placed = (P(both), P(both), P(both), P(None, both), P(None, both), P(None, both), P(both), P(), P())
    return jax.shard_map(
        local,
        mesh=mesh,
        in_specs=placed,
        out_specs=(P(both), P(None, "atom")),
        check_vma=False,
    )
```

```python
import functools
import math

import jax
import jax.numpy as jnp
from jax import lax
from jax.experimental import pallas as pl
from jax.experimental.pallas import tpu as pltpu
from jax.sharding import PartitionSpec as P

MESH = pl.DeviceIdType.MESH
LANES = 128
SUBS = 8
mixing_beta = 0.5
ridge_share = 0.1
F32 = jnp.float32


def solve_coeffs(entry, hist_len):
    trace = entry[0][0]
    for i in range(1, hist_len):
        trace = trace + entry[i][i]
    ridge = (ridge_share / hist_len) * trace
    low = [[entry[i][j] for j in range(i + 1)] for i in range(hist_len)]
    for i in range(hist_len):
        low[i][i] = low[i][i] + ridge
    inverse = [None] * hist_len
    factor = [[None] * hist_len for _ in range(hist_len)]
    forward = [jnp.ones_like(trace) for _ in range(hist_len)]
    for j in range(hist_len):
        inverse[j] = 1.0 / low[j][j]
        for i in range(j + 1, hist_len):
            factor[i][j] = low[i][j] * inverse[j]
        for i in range(j + 1, hist_len):
            forward[i] = forward[i] - factor[i][j] * forward[j]
            for k in range(j + 1, i + 1):
                low[i][k] = low[i][k] - factor[i][j] * low[k][j]
    backward = [forward[i] * inverse[i] for i in range(hist_len)]
    for j in reversed(range(hist_len)):
        for i in range(j):
            backward[i] = backward[i] - factor[j][i] * backward[j]
    total = backward[0]
    for i in range(1, hist_len):
        total = total + backward[i]
    return [backward[i] / total for i in range(hist_len)]


def split(x):
    pieces = []
    for _ in range(3):
        piece = x.astype(jnp.bfloat16).astype(F32)
        pieces.append(piece)
        x = x - piece
    return pieces


def kernel(
    cfg,
    batch_atom,
    owner_slot,
    slot_index,
    w_hbm,
    target_hbm,
    coupling_hbm,
    basis_hbm,
    rho_hbm,
    res_hbm,
    density_out,
    moments_out,
    w,
    target,
    coupling,
    basis,
    rho,
    res,
    fresh,
    fresh_w,
    stack_rows,
    plane_rows,
    stack_moments,
    part_send,
    part_recv,
    own_send,
    own_recv,
    chunks,
    source_cols,
    mask,
    hist_moments,
    base_rows,
    correct,
    load_sem,
    send_sem,
    recv_sem,
):
    iters, hist_len, harmonics, batches, width, owned, planes, lines, members, scale = cfg
    tiles = w.shape[0]
    per_batch = width // LANES
    half = LANES // 2
    rows = batches // 4
    plane = lines * members
    near_lanes = plane * batches
    shares = chunks.shape[0]
    depth = shares // lines
    share = owned // shares
    my_group = lax.axis_index("grid")
    my_member = lax.axis_index("atom")
    my_plane = lax.div(my_group, lines)
    my_line = lax.rem(my_group, lines)
    spot = my_line * members + my_member
    my_share = my_line * depth + lax.rem(my_plane, depth)

    def in_stack(at):
        return at * lines + my_line, my_member

    def in_plane(at):
        return my_plane * lines + lax.div(at, members), lax.rem(at, members)

    def in_shares(at):
        return (lax.div(my_plane, depth) * depth + lax.rem(at, depth)) * lines + lax.div(at, depth), my_member

    groups = ((planes, my_plane, in_stack), (plane, spot, in_plane), (shares, my_share, in_shares))
    barrier = pltpu.get_barrier_semaphore()
    for count, mine, where in groups:

        @pl.loop(1, count)
        def _(step):
            pl.semaphore_signal(barrier, inc=1, device_id=where(lax.rem(mine + step, count)), device_id_type=MESH)

    loads = [
        pltpu.make_async_copy(src, dst, load_sem.at[k])
        for k, (src, dst) in enumerate(
            ((res_hbm, res), (w_hbm, w), (basis_hbm, basis), (rho_hbm, rho), (target_hbm, target), (coupling_hbm, coupling))
        )
    ]
    for load in loads:
        load.start()

    lane = lax.broadcasted_iota(jnp.int32, (SUBS, LANES), 1)
    sub = lax.broadcasted_iota(jnp.int32, (SUBS, LANES), 0)
    quarter = lane // 32
    lane_row = lax.broadcasted_iota(jnp.int32, (1, LANES), 1)
    low_row = lane_row < half
    low = lax.broadcasted_iota(jnp.int32, (2 * SUBS, LANES), 1) < half

    slot_row = jnp.zeros((1, LANES), F32)
    for b in range(batches):
        slot_row = jnp.where(lane_row == half + b, owner_slot[batch_atom[b]].astype(F32), slot_row)

    def lane_tile(t):
        return pl.ds(pl.multiple_of(t * LANES, LANES), LANES)

    def copy_to(src, dst, which, group, target_at):
        return pltpu.make_async_remote_copy(
            src_ref=src,
            dst_ref=dst,
            send_sem=send_sem.at[which],
            recv_sem=recv_sem.at[which],
            device_id=groups[group][2](target_at),
            device_id_type=MESH,
        )

    def exchange(buf, which, group):
        count, mine, _ = groups[group]

        @pl.loop(1, count)
        def _(step):
            copy_to(buf.at[mine], buf.at[mine], which, group, lax.rem(mine + step, count)).start()

        return waiter(buf, buf, which, group)

    sends = []

    def waiter(src, dst, which, group):
        all_but_one = pl.ds(0, groups[group][0] - 1)
        sends.append((src.at[all_but_one], send_sem.at[which]))

        def wait():
            arrived = dst.at[all_but_one]
            pltpu.make_async_copy(arrived, arrived, recv_sem.at[which]).wait()

        return wait

    def tree(parts):
        parts = list(parts)
        while len(parts) > 1:
            parts = [parts[k] + parts[k + 1] if k + 1 < len(parts) else parts[k] for k in range(0, len(parts), 2)]
        return parts[0]

    def total(buf, count):
        return tree(buf[k] for k in range(count))

    def splat(row, k):
        return jnp.broadcast_to(row[:, k : k + 1], (1, LANES))

    def weigh(first, last):
        @pl.loop(first, last)
        def _(r):
            xs, ys = [], []
            for q in range(4):
                b = q * rows + r
                at = pl.ds(pl.multiple_of(b * width, width), width)
                gain = jnp.concatenate([w[pl.ds(b * per_batch + v, 1), :] for v in range(per_batch)], axis=1)
                xs.extend(split(res[:, at] * gain))
                ys.append(jnp.concatenate([basis[0:24, at], jnp.broadcast_to(basis[24:25, at], (SUBS, width))], axis=0))
            x = jnp.concatenate(xs, axis=0).astype(jnp.bfloat16)
            out = None
            for y in split(jnp.concatenate(ys, axis=0)):
                part = lax.dot_general(
                    x, y.astype(jnp.bfloat16), (((1,), (1,)), ((), ())), preferred_element_type=F32
                )
                out = part if out is None else out + part
            tile = jnp.zeros((SUBS, LANES), F32)
            for q in range(4):
                block = out[24 * q : 24 * q + 8] + out[24 * q + 8 : 24 * q + 16] + out[24 * q + 16 : 24 * q + 24]
                tile = jnp.where(quarter == q, block, tile)
            hist_moments[r] = tile

    shifts = hist_len // 2 + 1
    entry = None
    per_iter = 4
    for iteration in range(iters):
        stack_row = stack_rows.at[iteration]
        plane_row = plane_rows.at[iteration]
        stack_moment = stack_moments.at[iteration]
        sent = part_send.at[iteration]
        received = part_recv.at[iteration]
        which = per_iter * iteration
        last = iteration == iters - 1

        if iteration == 0:
            loads[0].wait()
            loads[1].wait()

            def gram(step, acc):
                acc = list(acc)
                for u in range(8):
                    t = step * 8 + u
                    x = res[:, lane_tile(t)]
                    y = x * w[pl.ds(t, 1), :]
                    for r in range(shifts):
                        acc[r] = acc[r] + y * (pltpu.roll(x, r, 0) if r else x)
                return tuple(acc)

            acc = lax.fori_loop(0, tiles // 8, gram, tuple(jnp.zeros((SUBS, LANES), F32) for _ in range(shifts)))
            packed = jnp.zeros((SUBS, LANES), F32)
            for r in range(shifts):
                packed = jnp.where(lane == hist_len * r + sub, jnp.sum(acc[r], axis=1, keepdims=True), packed)
            stack_row[pl.ds(my_plane, 1)] = (jnp.sum(packed, axis=0, keepdims=True) + slot_row)[None]
            pl.semaphore_wait(barrier, sum(count - 1 for count, _, _ in groups))
        else:
            slot = slot_index[iteration - 1]
            replaced = sub == slot

            def refresh(step, acc):
                for u in range(8):
                    t = step * 8 + u
                    new_res = jnp.where(replaced, fresh[pl.ds(t, 1), :], res[:, lane_tile(t)])
                    new_rho = jnp.where(replaced, density_out[pl.ds(t, 1), :], rho[:, lane_tile(t)])
                    res[:, lane_tile(t)] = new_res
                    rho[:, lane_tile(t)] = new_rho
                    acc = acc + fresh_w[pl.ds(t, 1), :] * new_res
                return acc

            acc = lax.fori_loop(0, tiles // 8, refresh, jnp.zeros((SUBS, LANES), F32))
            packed = jnp.where(lane == sub, jnp.sum(acc, axis=1, keepdims=True), 0.0)
            stack_row[pl.ds(my_plane, 1)] = jnp.sum(packed, axis=0, keepdims=True)[None]
        wait = exchange(stack_row, which, 0)

        if iteration == 0:
            loads[2].wait()
        weigh(0, rows // 2)

        wait()
        plane_row[pl.ds(spot, 1)] = jnp.where(low_row, total(stack_row, planes), slot_row)[None]
        wait = exchange(plane_row, which + 1, 1)

        if iteration == 0:
            ids = jnp.concatenate([stack_row[k] for k in range(planes)] * (LANES // planes), axis=0)
            ids = jnp.transpose(ids)
            for k in range(planes):
                source_cols[k * batches : (k + 1) * batches] = jnp.broadcast_to(
                    ids[half : half + batches, k : k + 1], (batches, LANES)
                )
        weigh(rows // 2, rows)

        wait()
        row = total(plane_row, plane)
        if iteration == 0:
            entry = [[None] * (i + 1) for i in range(hist_len)]
            for i in range(hist_len):
                for j in range(i + 1):
                    r = i - j
                    at = hist_len * r + i if r < shifts else hist_len * (hist_len - r) + j
                    entry[i][j] = splat(row, at)
        else:
            news = [splat(row, k) for k in range(hist_len)]
            slot_vec = jnp.zeros((1, LANES), jnp.int32) + slot
            entry = [
                [
                    jnp.where(slot_vec == i, news[j], jnp.where(slot_vec == j, news[i], entry[i][j]))
                    for j in range(i + 1)
                ]
                for i in range(hist_len)
            ]
        coeffs = solve_coeffs(entry, hist_len)
        coeff_col = jnp.zeros((SUBS, LANES), F32)
        for i in range(hist_len):
            coeff_col = jnp.where(sub == i, coeffs[i], coeff_col)

        mixed = jnp.concatenate(
            [jnp.sum(coeff_col * hist_moments[r], axis=0, keepdims=True) for r in range(rows)], axis=0
        )
        turned = jnp.concatenate(
            [
                pltpu.roll(mixed, (LANES - 32 * q - 16 * h) % LANES, 1) if q + h else mixed
                for h in range(2)
                for q in range(4)
            ],
            axis=0,
        )
        stack_moment[pl.ds(my_plane, 1)] = jnp.transpose(turned)[0 : 2 * SUBS][None]
        wait = exchange(stack_moment, which + 2, 0)

        if iteration == 0:

            def fill(lanes, wanted):
                for k in range(mask.shape[0] // (2 * SUBS)):
                    at = slice(2 * SUBS * k, 2 * SUBS * (k + 1))
                    mask[at, lanes] = jnp.where(source_cols[at] == wanted, 1.0, 0.0).astype(jnp.bfloat16)

            @pl.loop(0, near_lanes // LANES)
            def _(t):
                pair = jnp.where(low_row, pltpu.roll(plane_row[2 * t], half, 1), plane_row[2 * t + 1])
                fill(lane_tile(t), pair)

            @pl.loop(0, plane * share // LANES)
            def _(t):
                at = t * (LANES // share) + lane_row // share
                held = (at % members) * owned + ((at // members) * depth + lax.rem(my_plane, depth)) * share
                fill(lane_tile(t + near_lanes // LANES), (held + lane_row % share).astype(F32))

            for load in loads[3:]:
                load.wait()

        def base_step(step, carry):
            for u in range(8):
                t = step * 8 + u
                part = coeff_col * (rho[:, lane_tile(t)] + mixing_beta * res[:, lane_tile(t)])
                base_rows[pl.ds(t, 1), :] = jnp.sum(part, axis=0, keepdims=True)
            return carry

        lax.fori_loop(0, tiles // 8, base_step, 0)
        wait()

        blocks = []
        for k in range(0, planes, 2):
            one, two = stack_moment[k], stack_moment[k + 1]
            upper = jnp.where(low, one, pltpu.roll(two, half, 1))
            lower = jnp.where(low, pltpu.roll(one, half, 1), two)
            blocks.append(jnp.concatenate([upper, lower], axis=0))
        everywhere = jnp.concatenate(blocks, axis=1)
        pieces = jnp.concatenate(split(everywhere), axis=0).astype(jnp.bfloat16)

        def gathered(first, count):
            out = jnp.dot(
                pieces, mask[:, pl.ds(pl.multiple_of(first, count), count)], preferred_element_type=F32
            )
            return out[0:32] + out[32:64] + out[64:96]

        quad = 4

        @pl.loop(0, plane // quad)
        def _(step):
            first = lax.rem(lax.div(spot, quad) + step, plane // quad) * quad
            out = gathered(first * batches, quad * batches)
            for k in range(0, quad, 2):
                upper = out[0:16, k * batches : (k + 2) * batches]
                lower = out[16:32, k * batches : (k + 2) * batches]
                sent[first + k] = jnp.where(low, upper, pltpu.roll(lower, half, 1))
                sent[first + k + 1] = jnp.where(low, pltpu.roll(upper, half, 1), lower)
            for k in range(quad):

                @pl.when(first + k != spot)
                def _():
                    copy_to(sent.at[first + k], received.at[spot], which + 3, 1, first + k).start()

        received[pl.ds(spot, 1)] = sent[pl.ds(spot, 1)]
        wait = waiter(sent, received, which + 3, 1)

        if last:
            many = 2 * LANES // share
            each = LANES // share

            @pl.loop(0, plane // many)
            def _(step):
                first = lax.rem(lax.div(spot, many) + step, plane // many) * many
                out = gathered(near_lanes + first * share, many * share)
                for k in range(many):
                    tile = out[:, k // each * LANES : (k // each + 1) * LANES]
                    kept = jnp.zeros((SUBS, LANES), F32)
                    for g in range(4):
                        piece = tile[g * SUBS : (g + 1) * SUBS]
                        turn = (g - k % each) * 32 % LANES
                        kept = jnp.where(quarter == g, pltpu.roll(piece, turn, 1) if turn else piece, kept)
                    own_send[first + k] = kept
                for k in range(many):

                    @pl.when(first + k != spot)
                    def _():
                        copy_to(own_send.at[first + k], own_recv.at[spot], per_iter * iters, 1, first + k).start()

            own_recv[pl.ds(spot, 1)] = own_send[pl.ds(spot, 1)]
            own_wait = waiter(own_send, own_recv, per_iter * iters, 1)

        wait()
        summed = total(received, plane)
        at_batch = jnp.concatenate([summed, pltpu.roll(summed, half, 1)], axis=0) * scale
        if last:
            own_wait()
            chunks[pl.ds(my_share, 1)] = (total(own_recv, plane) * scale)[None]
            own_wait = exchange(chunks, per_iter * iters + 1, 2)

        comp = lax.broadcasted_iota(jnp.int32, (32, LANES), 0)
        degree = sum((comp >= (l + 1) * (l + 1)).astype(F32) for l in range(4))
        damped = jnp.where(comp < harmonics, at_batch * (mixing_beta / (1.0 + degree)), 0.0)

        def density_step(step, ahead):
            for u in range(16):
                b = step * 16 + u
                col = jnp.broadcast_to(ahead[:, u : u + 1], (32, LANES))
                for v in range(per_batch):
                    t = b * per_batch + v
                    part = col[24:32] * basis[24:25, lane_tile(t)]
                    for g in range(3):
                        part = part + col[g * SUBS : (g + 1) * SUBS] * basis[g * SUBS : (g + 1) * SUBS, lane_tile(t)]
                    correct[pl.ds(t, 1), :] = jnp.sum(part, axis=0, keepdims=True)
            return pltpu.roll(ahead, LANES - 16, 1)

        lax.fori_loop(0, batches // 16, density_step, damped)
        density = base_rows[...] - correct[...]
        density_out[...] = density
        if last:
            own_wait()
            each = LANES // share
            for t in range(owned // LANES):
                held = [chunks[t * each + k] for k in range(each)]
                for g in range(4):
                    tile = jnp.zeros((SUBS, LANES), F32)
                    for k in range(each):
                        turn = (k - g) * 32 % LANES
                        tile = jnp.where(quarter == k, pltpu.roll(held[k], turn, 1) if turn else held[k], tile)
                    top = min(SUBS, harmonics - g * SUBS)
                    moments_out[g * SUBS : g * SUBS + top, t * LANES : (t + 1) * LANES] = tile[0:top]
        else:
            new = target[...] + coupling[...] * jnp.tanh(density) - density
            fresh[...] = new
            fresh_w[...] = new * w[...]

    for src, sem in sends:
        pltpu.make_async_copy(src, src, sem).wait()


def finish(density, moments, density_out, moments_out):
    density_out[...] = density[...]
    moments_out[...] = moments[...]


def local(weights, target, coupling, multipole_basis, rho_hist, res_hist, batch_atom, owner_slot, slot_index):
    harmonics, points = multipole_basis.shape
    hist_len = res_hist.shape[0]
    batches = batch_atom.shape[0]
    groups = lax.axis_size("grid")
    members = lax.axis_size("atom")
    lines = 4
    planes = groups // lines
    plane = lines * members
    shares = 4 * lines
    owned = owner_slot.shape[0] // members
    scale = 1.0 / math.sqrt(points * groups // owned)
    iters = slot_index.shape[0]
    cfg = (iters, hist_len, harmonics, batches, points // batches, owned, planes, lines, members, scale)
    tiles = points // LANES
    flat = (tiles, LANES)
    any_space = pl.BlockSpec(memory_space=pl.ANY)
    smem = pl.BlockSpec(memory_space=pltpu.SMEM)
    vmem = pl.BlockSpec(memory_space=pltpu.VMEM)
    density, moments = pl.pallas_call(
        functools.partial(kernel, cfg),
        out_shape=(jax.ShapeDtypeStruct(flat, F32), jax.ShapeDtypeStruct((harmonics, owned), F32)),
        in_specs=[smem] * 3 + [any_space] * 6,
        out_specs=(vmem, vmem),
        scratch_shapes=[
            pltpu.VMEM(flat, F32),
            pltpu.VMEM(flat, F32),
            pltpu.VMEM(flat, F32),
            pltpu.VMEM((harmonics, points), F32),
            pltpu.VMEM((hist_len, points), F32),
            pltpu.VMEM((hist_len, points), F32),
            pltpu.VMEM(flat, F32),
            pltpu.VMEM(flat, F32),
            pltpu.VMEM((iters, planes, 1, LANES), F32),
            pltpu.VMEM((iters, plane, 1, LANES), F32),
            pltpu.VMEM((iters, planes, 2 * SUBS, LANES), F32),
            pltpu.VMEM((iters, plane, 2 * SUBS, LANES), F32),
            pltpu.VMEM((iters, plane, 2 * SUBS, LANES), F32),
            pltpu.VMEM((plane, SUBS, LANES), F32),
            pltpu.VMEM((plane, SUBS, LANES), F32),
            pltpu.VMEM((shares, SUBS, LANES), F32),
            pltpu.VMEM((planes * batches, LANES), F32),
            pltpu.VMEM((planes * batches, plane * (batches + owned // shares)), jnp.bfloat16),
            pltpu.VMEM((batches // 4, SUBS, LANES), F32),
            pltpu.VMEM(flat, F32),
            pltpu.VMEM(flat, F32),
            pltpu.SemaphoreType.DMA((6,)),
            pltpu.SemaphoreType.DMA((4 * iters + 2,)),
            pltpu.SemaphoreType.DMA((4 * iters + 2,)),
        ],
        compiler_params=pltpu.CompilerParams(
            collective_id=0, has_side_effects=True, vmem_limit_bytes=67043328
        ),
    )(
        batch_atom,
        owner_slot,
        slot_index,
        weights.reshape(flat),
        target.reshape(flat),
        coupling.reshape(flat),
        multipole_basis,
        rho_hist,
        res_hist,
    )
    density, moments = pl.pallas_call(
        finish,
        out_shape=(jax.ShapeDtypeStruct(flat, F32), jax.ShapeDtypeStruct((harmonics, owned), F32)),
        in_specs=[vmem] * 2,
        out_specs=(vmem, vmem),
    )(density, moments)
    return density.reshape(points), moments


def solution(mesh):
    both = ("grid", "atom")
    placed = (P(both), P(both), P(both), P(None, both), P(None, both), P(None, both), P(both), P(), P())
    return jax.shard_map(
        local,
        mesh=mesh,
        in_specs=placed,
        out_specs=(P(both), P(None, "atom")),
        check_vma=False,
    )
```

```python
import functools
import math

import jax
import jax.numpy as jnp
from jax import lax
from jax.experimental import pallas as pl
from jax.experimental.pallas import tpu as pltpu
from jax.sharding import PartitionSpec as P

MESH = pl.DeviceIdType.MESH
LANES = 128
SUBS = 8
mixing_beta = 0.5
ridge_share = 0.1
F32 = jnp.float32


def solve_coeffs(entry, hist_len):
    trace = entry[0][0]
    for i in range(1, hist_len):
        trace = trace + entry[i][i]
    ridge = (ridge_share / hist_len) * trace
    low = [[entry[i][j] for j in range(i + 1)] for i in range(hist_len)]
    for i in range(hist_len):
        low[i][i] = low[i][i] + ridge
    inverse = [None] * hist_len
    factor = [[None] * hist_len for _ in range(hist_len)]
    forward = [jnp.ones_like(trace) for _ in range(hist_len)]
    for j in range(hist_len):
        inverse[j] = 1.0 / low[j][j]
        for i in range(j + 1, hist_len):
            factor[i][j] = low[i][j] * inverse[j]
        for i in range(j + 1, hist_len):
            forward[i] = forward[i] - factor[i][j] * forward[j]
            for k in range(j + 1, i + 1):
                low[i][k] = low[i][k] - factor[i][j] * low[k][j]
    backward = [forward[i] * inverse[i] for i in range(hist_len)]
    for j in reversed(range(hist_len)):
        for i in range(j):
            backward[i] = backward[i] - factor[j][i] * backward[j]
    total = backward[0]
    for i in range(1, hist_len):
        total = total + backward[i]
    return [backward[i] / total for i in range(hist_len)]


def split(x):
    pieces = []
    for _ in range(3):
        piece = x.astype(jnp.bfloat16).astype(F32)
        pieces.append(piece)
        x = x - piece
    return pieces


def kernel(
    cfg,
    batch_atom,
    owner_slot,
    slot_index,
    w_hbm,
    target_hbm,
    coupling_hbm,
    basis_hbm,
    rho_hbm,
    res_hbm,
    density_out,
    moments_out,
    w,
    target,
    coupling,
    basis,
    rho,
    res,
    fresh,
    fresh_w,
    stack_rows,
    sheet_rows,
    id_rows,
    hist_all,
    fresh_all,
    part_send,
    part_recv,
    own_send,
    own_recv,
    chunks,
    source_cols,
    mask,
    hist_moments,
    base_rows,
    correct,
    load_sem,
    send_sem,
    recv_sem,
    pass_sem,
):
    iters, hist_len, harmonics, batches, width, owned, planes, lines, spans, cores, scale = cfg
    tiles = w.shape[0]
    per_batch = width // LANES
    half = LANES // 2
    rows = batches // 4
    stack = planes * cores
    sheet = lines * spans
    near_lanes = sheet * batches
    shares = chunks.shape[0]
    depth = shares // lines
    share = owned // shares
    my_group = lax.axis_index("grid")
    my_member = lax.axis_index("atom")
    my_plane = lax.div(my_group, lines)
    my_line = lax.rem(my_group, lines)
    my_span = lax.div(my_member, cores)
    my_core = lax.rem(my_member, cores)
    in_stack = my_plane * cores + my_core
    in_sheet = my_line * spans + my_span
    my_share = my_line * depth + lax.rem(my_plane, depth)

    def ring(step, count):
        return min(step, count - step)

    def stack_peer(step):
        plane, core = lax.rem(my_plane + step[0], planes), lax.rem(my_core + step[1], cores)
        return plane * cores + core, (plane * lines + my_line, my_span * cores + core)

    def sheet_peer(step):
        line, span = lax.rem(my_line + step[0], lines), lax.rem(my_span + step[1], spans)
        return line * spans + span, (my_plane * lines + line, span * cores + my_core)

    def share_peer(step):
        line, plane = lax.rem(my_line + step[0], lines), lax.rem(my_plane + step[1], depth)
        device = (lax.div(my_plane, depth) * depth + plane) * lines + line, my_member
        return line * depth + plane, device

    def far_first(across, along):
        steps = [(a, b) for a in range(across) for b in range(along) if a or b]
        return sorted(steps, key=lambda step: -ring(step[0], across) - ring(step[1], along))

    stack_group = (stack, in_stack, stack_peer, far_first(planes, cores))
    sheet_group = (sheet, in_sheet, sheet_peer, far_first(lines, spans))
    share_group = (shares, my_share, share_peer, far_first(lines, depth))
    groups = (stack_group, sheet_group, share_group)
    barrier = pltpu.get_barrier_semaphore()
    for _, _, peer, steps in groups:
        for step in steps:
            pl.semaphore_signal(barrier, inc=1, device_id=peer(step)[1], device_id_type=MESH)

    loads = [
        pltpu.make_async_copy(src, dst, load_sem.at[k])
        for k, (src, dst) in enumerate(
            ((res_hbm, res), (w_hbm, w), (basis_hbm, basis), (rho_hbm, rho), (target_hbm, target), (coupling_hbm, coupling))
        )
    ]
    for load in loads:
        load.start()

    lane = lax.broadcasted_iota(jnp.int32, (SUBS, LANES), 1)
    sub = lax.broadcasted_iota(jnp.int32, (SUBS, LANES), 0)
    quarter = lane // 32
    lane_row = lax.broadcasted_iota(jnp.int32, (1, LANES), 1)
    low_row = lane_row < half
    low = lax.broadcasted_iota(jnp.int32, (2 * SUBS, LANES), 1) < half
    low_wide = lax.broadcasted_iota(jnp.int32, (32, LANES), 1) < half

    slot_row = jnp.zeros((1, LANES), F32)
    for b in range(batches):
        slot_row = jnp.where(lane_row == half + b, owner_slot[batch_atom[b]].astype(F32), slot_row)
    id_rows[pl.ds(in_sheet, 1)] = slot_row[None]

    def lane_tile(t):
        return pl.ds(pl.multiple_of(t * LANES, LANES), LANES)

    kinds = []
    sends = []

    def channel():
        kinds.append(len(kinds))
        return kinds[-1]

    def copy_to(src, dst, which, device, arrival=None):
        return pltpu.make_async_remote_copy(
            src_ref=src,
            dst_ref=dst,
            send_sem=send_sem.at[which],
            recv_sem=recv_sem.at[which] if arrival is None else arrival,
            device_id=device,
            device_id_type=MESH,
        )

    def drained(src, which):
        sends.append((src, send_sem.at[which]))

    def waiter(src, dst, which, count):
        drained(src.at[pl.ds(0, count)], which)

        def wait():
            arrived = dst.at[pl.ds(0, count)]
            pltpu.make_async_copy(arrived, arrived, recv_sem.at[which]).wait()

        return wait

    def exchange(buf, group):
        count, mine, peer, steps = group
        which = channel()
        for step in steps:
            copy_to(buf.at[mine], buf.at[mine], which, peer(step)[1]).start()
        return waiter(buf, buf, which, count - 1)

    def scatter(src, dst, group):
        count, mine, peer, steps = group
        which = channel()

        def send(step):
            at, device = peer(step)
            copy_to(src.at[at], dst.at[mine], which, device).start()

        return send, waiter(src, dst, which, count - 1)

    def tree(parts):
        parts = list(parts)
        while len(parts) > 1:
            parts = [parts[k] + parts[k + 1] if k + 1 < len(parts) else parts[k] for k in range(0, len(parts), 2)]
        return parts[0]

    def total(buf, count):
        return tree(buf[k] for k in range(count))

    def splat(row, k):
        return jnp.broadcast_to(row[:, k : k + 1], (1, LANES))

    def weigh():
        @pl.loop(0, rows // 2)
        def _(step):
            for u in range(2):
                r = step * 2 + u
                xs, ys = [], []
                for q in range(4):
                    b = q * rows + r
                    at = pl.ds(pl.multiple_of(b * width, width), width)
                    gain = jnp.concatenate([w[pl.ds(b * per_batch + v, 1), :] for v in range(per_batch)], axis=1)
                    xs.extend(split(res[:, at] * gain))
                    ys.append(
                        jnp.concatenate([basis[0:24, at], jnp.broadcast_to(basis[24:25, at], (SUBS, width))], axis=0)
                    )
                x = jnp.concatenate(xs, axis=0).astype(jnp.bfloat16)
                out = None
                for y in split(jnp.concatenate(ys, axis=0)):
                    part = lax.dot_general(
                        x, y.astype(jnp.bfloat16), (((1,), (1,)), ((), ())), preferred_element_type=F32
                    )
                    out = part if out is None else out + part
                tile = jnp.zeros((SUBS, LANES), F32)
                for q in range(4):
                    block = out[24 * q : 24 * q + 8] + out[24 * q + 8 : 24 * q + 16] + out[24 * q + 16 : 24 * q + 24]
                    tile = jnp.where(quarter == q, block, tile)
                hist_moments[pl.ds(r, hist_len, stride=rows), :] = tile

    def turn(block, by):
        return pltpu.roll(block, by % LANES, 1) if by % LANES else block

    shifts = hist_len // 2 + 1
    entry = None
    for iteration in range(iters):
        stack_row = stack_rows.at[iteration]
        sheet_row = sheet_rows.at[iteration]
        sent = part_send.at[iteration]
        received = part_recv.at[iteration]
        last = iteration == iters - 1

        if iteration == 0:
            loads[0].wait()
            loads[1].wait()

            def gram(step, acc):
                acc = list(acc)
                for u in range(8):
                    t = step * 8 + u
                    x = res[:, lane_tile(t)]
                    y = x * w[pl.ds(t, 1), :]
                    for r in range(shifts):
                        acc[r] = acc[r] + y * (pltpu.roll(x, r, 0) if r else x)
                return tuple(acc)

            acc = lax.fori_loop(0, tiles // 8, gram, tuple(jnp.zeros((SUBS, LANES), F32) for _ in range(shifts)))
            packed = jnp.zeros((SUBS, LANES), F32)
            for r in range(shifts):
                packed = jnp.where(lane == hist_len * r + sub, jnp.sum(acc[r], axis=1, keepdims=True), packed)
            stack_row[pl.ds(in_stack, 1)] = (jnp.sum(packed, axis=0, keepdims=True) + slot_row)[None]
            pl.semaphore_wait(barrier, sum(group[0] - 1 for group in groups))
        else:
            slot = slot_index[iteration - 1]
            replaced = sub == slot

            def refresh(step, acc):
                for u in range(8):
                    t = step * 8 + u
                    new_res = jnp.where(replaced, fresh[pl.ds(t, 1), :], res[:, lane_tile(t)])
                    new_rho = jnp.where(replaced, density_out[pl.ds(t, 1), :], rho[:, lane_tile(t)])
                    res[:, lane_tile(t)] = new_res
                    rho[:, lane_tile(t)] = new_rho
                    acc = acc + fresh_w[pl.ds(t, 1), :] * new_res
                return acc

            acc = lax.fori_loop(0, tiles // 8, refresh, jnp.zeros((SUBS, LANES), F32))
            packed = jnp.where(lane == sub, jnp.sum(acc, axis=1, keepdims=True), 0.0)
            stack_row[pl.ds(in_stack, 1)] = jnp.sum(packed, axis=0, keepdims=True)[None]
        wait = exchange(stack_row, stack_group)
        if iteration == 0:
            wait_ids = exchange(id_rows, sheet_group)

        if iteration == 0:
            loads[2].wait()
        weigh()
        if iteration == 0:
            mine = hist_all.at[in_stack]
            for pair in range(hist_len // 2):
                turned = jnp.concatenate(
                    [
                        turn(hist_moments[(2 * pair + h) * rows : (2 * pair + h + 1) * rows], -32 * q)
                        for h in range(2)
                        for q in range(4)
                    ],
                    axis=0,
                )
                mine[pair] = jnp.transpose(turned)[0:harmonics]
            passed, across = channel(), channel()
            sibling = stack_peer((0, 1))
            steps = [step for step in stack_group[3] if not step[1]]
            for k, step in enumerate(steps):
                copy_to(mine, mine, across, stack_peer(step)[1], pass_sem.at[k]).start()
            copy_to(mine, mine, passed, sibling[1]).start()
            drained(hist_all.at[pl.ds(0, planes - 1)], across)
            wait_passed = waiter(hist_all, hist_all, passed, planes)
        else:
            fresh_rows = hist_moments[0:rows]
            slot_vec = jnp.zeros((rows, LANES), jnp.int32) + slot
            for i in range(1, hist_len):
                fresh_rows = jnp.where(slot_vec == i, hist_moments[i * rows : (i + 1) * rows], fresh_rows)
            turned = jnp.concatenate([turn(fresh_rows, -32 * q - 16 * h) for h in range(2) for q in range(4)], axis=0)
            new_moment = fresh_all.at[iteration - 1]
            new_moment[pl.ds(in_stack, 1)] = jnp.transpose(turned)[0 : 2 * SUBS][None]
            wait_fresh = exchange(new_moment, stack_group)

        wait()
        sheet_row[pl.ds(in_sheet, 1)] = total(stack_row, stack)[None]
        wait = exchange(sheet_row, sheet_group)

        if iteration == 0:
            ids = jnp.concatenate([stack_row[k] for k in range(stack)] * (LANES // stack), axis=0)
            ids = jnp.transpose(ids)
            for k in range(stack):
                source_cols[k * batches : (k + 1) * batches] = jnp.broadcast_to(
                    ids[half : half + batches, k : k + 1], (batches, LANES)
                )
            wait_ids()

            def fill(lanes, wanted):
                for k in range(mask.shape[0] // (2 * SUBS)):
                    at = slice(2 * SUBS * k, 2 * SUBS * (k + 1))
                    mask[at, lanes] = jnp.where(source_cols[at] == wanted, 1.0, 0.0).astype(jnp.bfloat16)

            @pl.loop(0, near_lanes // LANES)
            def _(t):
                pair = jnp.where(low_row, pltpu.roll(id_rows[2 * t], half, 1), id_rows[2 * t + 1])
                fill(lane_tile(t), pair)

            @pl.loop(0, sheet * share // LANES)
            def _(t):
                at = t * (LANES // share) + lane_row // share
                member = (at % spans) * cores + my_core
                held = member * owned + ((at // spans) * depth + lax.rem(my_plane, depth)) * share
                fill(lane_tile(t + near_lanes // LANES), (held + lane_row % share).astype(F32))

            for load in loads[3:]:
                load.wait()

        wait()
        row = total(sheet_row, sheet)
        if iteration == 0:
            entry = [[None] * (i + 1) for i in range(hist_len)]
            for i in range(hist_len):
                for j in range(i + 1):
                    r = i - j
                    at = hist_len * r + i if r < shifts else hist_len * (hist_len - r) + j
                    entry[i][j] = splat(row, at)
        else:
            news = [splat(row, k) for k in range(hist_len)]
            slot_vec = jnp.zeros((1, LANES), jnp.int32) + slot
            entry = [
                [
                    jnp.where(slot_vec == i, news[j], jnp.where(slot_vec == j, news[i], entry[i][j]))
                    for j in range(i + 1)
                ]
                for i in range(hist_len)
            ]
        coeffs = solve_coeffs(entry, hist_len)
        coeff_col = jnp.zeros((SUBS, LANES), F32)
        for i in range(hist_len):
            coeff_col = jnp.where(sub == i, coeffs[i], coeff_col)

        if iteration == 0:
            for k, step in enumerate(steps):
                back = ((planes - step[0]) % planes, 0)
                block = hist_all.at[stack_peer(back)[0]]
                pltpu.make_async_copy(block, block, pass_sem.at[k]).wait()
                copy_to(block, block, passed, sibling[1]).start()
            wait_passed()
            old = coeffs
        else:
            wait_fresh()
            old = [jnp.where(slot_vec == i, 0.0, coeffs[i]) for i in range(hist_len)]
            new = coeffs[0]
            for i in range(1, hist_len):
                new = jnp.where(slot_vec == i, coeffs[i], new)

        gains = [jnp.where(low_row, old[2 * pair], old[2 * pair + 1]) for pair in range(hist_len // 2)]

        def mixed(at):
            top = tree(gains[pair] * hist_all[at, pair, 0:24] for pair in range(hist_len // 2))
            end = tree(gains[pair] * hist_all[at, pair, 24:25] for pair in range(hist_len // 2))
            return jnp.concatenate([top, jnp.broadcast_to(end, (SUBS, LANES))], axis=0)

        blocks = []
        for k in range(0, stack, 2):
            one, two = mixed(k), mixed(k + 1)
            block = jnp.where(low_wide, one, two) + pltpu.roll(jnp.where(low_wide, two, one), half, 1)
            if iteration:
                one, two = new_moment[k], new_moment[k + 1]
                upper = jnp.where(low, one, pltpu.roll(two, half, 1))
                lower = jnp.where(low, pltpu.roll(one, half, 1), two)
                block = block + new * jnp.concatenate([upper, lower], axis=0)
            blocks.append(block)
        everywhere = jnp.concatenate(blocks, axis=1)
        pieces = jnp.concatenate(split(everywhere), axis=0).astype(jnp.bfloat16)

        def gathered(first, count):
            out = jnp.dot(
                pieces, mask[:, pl.ds(pl.multiple_of(first, count), count)], preferred_element_type=F32
            )
            return out[0:32] + out[32:64] + out[64:96]

        if last:
            many = 2 * LANES // share
            each = LANES // share
            send, wait_own = scatter(own_send, own_recv, sheet_group)
            for first in range(0, sheet, many):
                out = gathered(near_lanes + first * share, many * share)
                for k in range(many):
                    tile = out[:, k // each * LANES : (k // each + 1) * LANES]
                    kept = jnp.zeros((SUBS, LANES), F32)
                    for g in range(4):
                        piece = tile[g * SUBS : (g + 1) * SUBS]
                        kept = jnp.where(quarter == g, turn(piece, (g - k % each) * 32), kept)
                    own_send[first + k] = kept
            own_recv[pl.ds(in_sheet, 1)] = own_send[pl.ds(in_sheet, 1)]
            for step in sheet_group[3]:
                send(step)

        send, wait = scatter(sent, received, sheet_group)
        for line_step in sorted(range(lines), key=lambda step: -ring(step, lines)):
            first = lax.rem(my_line + line_step, lines) * spans
            out = gathered(first * batches, spans * batches)
            for k in range(0, spans, 2):
                upper = out[0:16, k * batches : (k + 2) * batches]
                lower = out[16:32, k * batches : (k + 2) * batches]
                sent[first + k] = jnp.where(low, upper, pltpu.roll(lower, half, 1))
                sent[first + k + 1] = jnp.where(low, pltpu.roll(upper, half, 1), lower)
            for step in sheet_group[3]:
                if step[0] == line_step:
                    send(step)
        received[pl.ds(in_sheet, 1)] = sent[pl.ds(in_sheet, 1)]

        def base_step(step, carry):
            for u in range(8):
                t = step * 8 + u
                part = coeff_col * (rho[:, lane_tile(t)] + mixing_beta * res[:, lane_tile(t)])
                base_rows[pl.ds(t, 1), :] = jnp.sum(part, axis=0, keepdims=True)
            return carry

        lax.fori_loop(0, tiles // 8, base_step, 0)

        if last:
            wait_own()
            chunks[pl.ds(my_share, 1)] = (total(own_recv, sheet) * scale)[None]
            wait_chunks = exchange(chunks, share_group)

        wait()
        summed = total(received, sheet)
        at_batch = jnp.concatenate([summed, pltpu.roll(summed, half, 1)], axis=0) * scale
        comp = lax.broadcasted_iota(jnp.int32, (32, LANES), 0)
        degree = sum((comp >= (l + 1) * (l + 1)).astype(F32) for l in range(4))
        damped = jnp.where(comp < harmonics, at_batch * (mixing_beta / (1.0 + degree)), 0.0)

        def density_step(step, ahead):
            for u in range(16):
                b = step * 16 + u
                col = jnp.broadcast_to(ahead[:, u : u + 1], (32, LANES))
                for v in range(per_batch):
                    t = b * per_batch + v
                    part = col[24:32] * basis[24:25, lane_tile(t)]
                    for g in range(3):
                        part = part + col[g * SUBS : (g + 1) * SUBS] * basis[g * SUBS : (g + 1) * SUBS, lane_tile(t)]
                    correct[pl.ds(t, 1), :] = jnp.sum(part, axis=0, keepdims=True)
            return pltpu.roll(ahead, LANES - 16, 1)

        lax.fori_loop(0, batches // 16, density_step, damped)
        density = base_rows[...] - correct[...]
        density_out[...] = density
        if last:
            wait_chunks()
            each = LANES // share
            for t in range(owned // LANES):
                held = [chunks[t * each + k] for k in range(each)]
                for g in range(4):
                    tile = jnp.zeros((SUBS, LANES), F32)
                    for k in range(each):
                        tile = jnp.where(quarter == k, turn(held[k], (k - g) * 32), tile)
                    top = min(SUBS, harmonics - g * SUBS)
                    moments_out[g * SUBS : g * SUBS + top, t * LANES : (t + 1) * LANES] = tile[0:top]
        else:
            new = target[...] + coupling[...] * jnp.tanh(density) - density
            fresh[...] = new
            fresh_w[...] = new * w[...]
    for src, sem in sends:
        pltpu.make_async_copy(src, src, sem).wait()


def finish(density, moments, density_out, moments_out):
    density_out[...] = density[...]
    moments_out[...] = moments[...]


def local(weights, target, coupling, multipole_basis, rho_hist, res_hist, batch_atom, owner_slot, slot_index):
    harmonics, points = multipole_basis.shape
    hist_len = res_hist.shape[0]
    batches = batch_atom.shape[0]
    groups = lax.axis_size("grid")
    members = lax.axis_size("atom")
    lines, cores = 4, 2
    planes = groups // lines
    spans = members // cores
    stack, sheet = planes * cores, lines * spans
    shares = 4 * lines
    owned = owner_slot.shape[0] // members
    scale = 1.0 / math.sqrt(points * groups // owned)
    iters = slot_index.shape[0]
    cfg = (iters, hist_len, harmonics, batches, points // batches, owned, planes, lines, spans, cores, scale)
    tiles = points // LANES
    flat = (tiles, LANES)
    kinds = 3 * iters + 5 + (iters - 1)
    any_space = pl.BlockSpec(memory_space=pl.ANY)
    smem = pl.BlockSpec(memory_space=pltpu.SMEM)
    vmem = pl.BlockSpec(memory_space=pltpu.VMEM)
    density, moments = pl.pallas_call(
        functools.partial(kernel, cfg),
        out_shape=(jax.ShapeDtypeStruct(flat, F32), jax.ShapeDtypeStruct((harmonics, owned), F32)),
        in_specs=[smem] * 3 + [any_space] * 6,
        out_specs=(vmem, vmem),
        scratch_shapes=[
            pltpu.VMEM(flat, F32),
            pltpu.VMEM(flat, F32),
            pltpu.VMEM(flat, F32),
            pltpu.VMEM((harmonics, points), F32),
            pltpu.VMEM((hist_len, points), F32),
            pltpu.VMEM((hist_len, points), F32),
            pltpu.VMEM(flat, F32),
            pltpu.VMEM(flat, F32),
            pltpu.VMEM((iters, stack, 1, LANES), F32),
            pltpu.VMEM((iters, sheet, 1, LANES), F32),
            pltpu.VMEM((sheet, 1, LANES), F32),
            pltpu.VMEM((stack, hist_len // 2, harmonics, LANES), F32),
            pltpu.VMEM((iters - 1, stack, 2 * SUBS, LANES), F32),
            pltpu.VMEM((iters, sheet, 2 * SUBS, LANES), F32),
            pltpu.VMEM((iters, sheet, 2 * SUBS, LANES), F32),
            pltpu.VMEM((sheet, SUBS, LANES), F32),
            pltpu.VMEM((sheet, SUBS, LANES), F32),
            pltpu.VMEM((shares, SUBS, LANES), F32),
            pltpu.VMEM((stack * batches, LANES), F32),
            pltpu.VMEM((stack * batches, sheet * (batches + owned // shares)), jnp.bfloat16),
            pltpu.VMEM((batches // 4 * hist_len, LANES), F32),
            pltpu.VMEM(flat, F32),
            pltpu.VMEM(flat, F32),
            pltpu.SemaphoreType.DMA((6,)),
            pltpu.SemaphoreType.DMA((kinds,)),
            pltpu.SemaphoreType.DMA((kinds,)),
            pltpu.SemaphoreType.DMA((planes - 1,)),
        ],
        compiler_params=pltpu.CompilerParams(
            collective_id=0, has_side_effects=True, vmem_limit_bytes=67043328
        ),
    )(
        batch_atom,
        owner_slot,
        slot_index,
        weights.reshape(flat),
        target.reshape(flat),
        coupling.reshape(flat),
        multipole_basis,
        rho_hist,
        res_hist,
    )
    density, moments = pl.pallas_call(
        finish,
        out_shape=(jax.ShapeDtypeStruct(flat, F32), jax.ShapeDtypeStruct((harmonics, owned), F32)),
        in_specs=[vmem] * 2,
        out_specs=(vmem, vmem),
    )(density, moments)
    return density.reshape(points), moments


def solution(mesh):
    both = ("grid", "atom")
    placed = (P(both), P(both), P(both), P(None, both), P(None, both), P(None, both), P(both), P(), P())
    return jax.shard_map(
        local,
        mesh=mesh,
        in_specs=placed,
        out_specs=(P(both), P(None, "atom")),
        check_vma=False,
    )
```

```python
import functools
import math

import jax
import jax.numpy as jnp
from jax import lax
from jax.experimental import pallas as pl
from jax.experimental.pallas import tpu as pltpu
from jax.sharding import PartitionSpec as P

MESH = pl.DeviceIdType.MESH
LANES = 128
SUBS = 8
mixing_beta = 0.5
ridge_share = 0.1
F32 = jnp.float32


def solve_coeffs(entry, hist_len):
    trace = entry[0][0]
    for i in range(1, hist_len):
        trace = trace + entry[i][i]
    ridge = (ridge_share / hist_len) * trace
    low = [[entry[i][j] for j in range(i + 1)] for i in range(hist_len)]
    for i in range(hist_len):
        low[i][i] = low[i][i] + ridge
    inverse = [None] * hist_len
    factor = [[None] * hist_len for _ in range(hist_len)]
    forward = [jnp.ones_like(trace) for _ in range(hist_len)]
    for j in range(hist_len):
        inverse[j] = 1.0 / low[j][j]
        for i in range(j + 1, hist_len):
            factor[i][j] = low[i][j] * inverse[j]
        for i in range(j + 1, hist_len):
            forward[i] = forward[i] - factor[i][j] * forward[j]
            for k in range(j + 1, i + 1):
                low[i][k] = low[i][k] - factor[i][j] * low[k][j]
    backward = [forward[i] * inverse[i] for i in range(hist_len)]
    for j in reversed(range(hist_len)):
        for i in range(j):
            backward[i] = backward[i] - factor[j][i] * backward[j]
    total = backward[0]
    for i in range(1, hist_len):
        total = total + backward[i]
    return [backward[i] / total for i in range(hist_len)]


def split(x):
    pieces = []
    for _ in range(3):
        piece = x.astype(jnp.bfloat16).astype(F32)
        pieces.append(piece)
        x = x - piece
    return pieces


def kernel(
    cfg,
    batch_atom_hbm,
    owner_slot_hbm,
    slot_index_hbm,
    w_hbm,
    target_hbm,
    coupling_hbm,
    basis_hbm,
    rho_hbm,
    res_hbm,
    density_out,
    moments_out,
    w,
    target,
    coupling,
    basis,
    rho,
    res,
    fresh,
    fresh_w,
    stack_rows,
    sheet_rows,
    id_rows,
    hist_all,
    fresh_all,
    part_send,
    part_recv,
    own_send,
    own_recv,
    chunks,
    source_cols,
    mask,
    hist_moments,
    base_rows,
    correct,
    batch_atom,
    owner_slot,
    slot_index,
    load_sem,
    send_sem,
    recv_sem,
    pass_sem,
):
    iters, hist_len, harmonics, batches, width, owned, planes, lines, spans, cores, scale = cfg
    tiles = w.shape[0]
    per_batch = width // LANES
    half = LANES // 2
    rows = batches // 4
    stack = planes * cores
    sheet = lines * spans
    near_lanes = sheet * batches
    shares = chunks.shape[0]
    depth = shares // lines
    share = owned // shares
    my_group = lax.axis_index("grid")
    my_member = lax.axis_index("atom")
    my_plane = lax.div(my_group, lines)
    my_line = lax.rem(my_group, lines)
    my_span = lax.div(my_member, cores)
    my_core = lax.rem(my_member, cores)
    in_stack = my_plane * cores + my_core
    in_sheet = my_line * spans + my_span
    my_share = my_line * depth + lax.rem(my_plane, depth)

    def ring(step, count):
        return min(step, count - step)

    def stack_peer(step):
        plane, core = lax.rem(my_plane + step[0], planes), lax.rem(my_core + step[1], cores)
        return plane * cores + core, (plane * lines + my_line, my_span * cores + core)

    def sheet_peer(step):
        line, span = lax.rem(my_line + step[0], lines), lax.rem(my_span + step[1], spans)
        return line * spans + span, (my_plane * lines + line, span * cores + my_core)

    def share_peer(step):
        line, plane = lax.rem(my_line + step[0], lines), lax.rem(my_plane + step[1], depth)
        device = (lax.div(my_plane, depth) * depth + plane) * lines + line, my_member
        return line * depth + plane, device

    def far_first(across, along):
        steps = [(a, b) for a in range(across) for b in range(along) if a or b]
        return sorted(steps, key=lambda step: -ring(step[0], across) - ring(step[1], along))

    stack_group = (stack, in_stack, stack_peer, far_first(planes, cores))
    sheet_group = (sheet, in_sheet, sheet_peer, far_first(lines, spans))
    share_group = (shares, my_share, share_peer, far_first(lines, depth))
    groups = (stack_group, sheet_group, share_group)
    first_half = pl.ds(0, tiles * LANES // 2)
    second_half = pl.ds(tiles * LANES // 2, tiles * LANES // 2)
    loads = [
        pltpu.make_async_copy(src, dst, load_sem.at[k])
        for k, (src, dst) in enumerate(
            (
                (w_hbm, w),
                (res_hbm.at[:, first_half], res.at[:, first_half]),
                (res_hbm.at[:, second_half], res.at[:, second_half]),
                (batch_atom_hbm, batch_atom),
                (owner_slot_hbm, owner_slot),
                (basis_hbm, basis),
                (slot_index_hbm, slot_index),
                (rho_hbm, rho),
                (target_hbm, target),
                (coupling_hbm, coupling),
            )
        )
    ]
    for load in loads:
        load.start()

    barrier = pltpu.get_barrier_semaphore()
    for _, _, peer, steps in groups:
        for step in steps:
            pl.semaphore_signal(barrier, inc=1, device_id=peer(step)[1], device_id_type=MESH)

    lane = lax.broadcasted_iota(jnp.int32, (SUBS, LANES), 1)
    sub = lax.broadcasted_iota(jnp.int32, (SUBS, LANES), 0)
    quarter = lane // 32
    lane_row = lax.broadcasted_iota(jnp.int32, (1, LANES), 1)
    low_row = lane_row < half
    low = lax.broadcasted_iota(jnp.int32, (2 * SUBS, LANES), 1) < half
    low_wide = lax.broadcasted_iota(jnp.int32, (32, LANES), 1) < half

    def lane_tile(t):
        return pl.ds(pl.multiple_of(t * LANES, LANES), LANES)

    kinds = []
    sends = []

    def channel():
        kinds.append(len(kinds))
        return kinds[-1]

    def copy_to(src, dst, which, device, arrival=None):
        return pltpu.make_async_remote_copy(
            src_ref=src,
            dst_ref=dst,
            send_sem=send_sem.at[which],
            recv_sem=recv_sem.at[which] if arrival is None else arrival,
            device_id=device,
            device_id_type=MESH,
        )

    def drained(src, which):
        sends.append((src, send_sem.at[which]))

    def waiter(src, dst, which, count):
        drained(src.at[pl.ds(0, count)], which)

        def wait():
            arrived = dst.at[pl.ds(0, count)]
            pltpu.make_async_copy(arrived, arrived, recv_sem.at[which]).wait()

        return wait

    def exchange(buf, group):
        count, mine, peer, steps = group
        which = channel()
        for step in steps:
            copy_to(buf.at[mine], buf.at[mine], which, peer(step)[1]).start()
        return waiter(buf, buf, which, count - 1)

    def scatter(src, dst, group):
        count, mine, peer, steps = group
        which = channel()

        def send(step):
            at, device = peer(step)
            copy_to(src.at[at], dst.at[mine], which, device).start()

        return send, waiter(src, dst, which, count - 1)

    def tree(parts):
        parts = list(parts)
        while len(parts) > 1:
            parts = [parts[k] + parts[k + 1] if k + 1 < len(parts) else parts[k] for k in range(0, len(parts), 2)]
        return parts[0]

    def total(buf, count):
        return tree(buf[k] for k in range(count))

    def splat(row, k):
        return jnp.broadcast_to(row[:, k : k + 1], (1, LANES))

    def weigh():
        @pl.loop(0, rows // 4)
        def _(step):
            for u in range(4):
                r = step * 4 + u
                xs, ys = [], []
                for q in range(4):
                    b = q * rows + r
                    at = pl.ds(pl.multiple_of(b * width, width), width)
                    gain = jnp.concatenate([w[pl.ds(b * per_batch + v, 1), :] for v in range(per_batch)], axis=1)
                    xs.extend(split(res[:, at] * gain))
                    ys.append(
                        jnp.concatenate([basis[0:24, at], jnp.broadcast_to(basis[24:25, at], (SUBS, width))], axis=0)
                    )
                x = jnp.concatenate(xs, axis=0).astype(jnp.bfloat16)
                out = None
                for y in split(jnp.concatenate(ys, axis=0)):
                    part = lax.dot_general(
                        x, y.astype(jnp.bfloat16), (((1,), (1,)), ((), ())), preferred_element_type=F32
                    )
                    out = part if out is None else out + part
                tile = jnp.zeros((SUBS, LANES), F32)
                for q in range(4):
                    block = out[24 * q : 24 * q + 8] + out[24 * q + 8 : 24 * q + 16] + out[24 * q + 16 : 24 * q + 24]
                    tile = jnp.where(quarter == q, block, tile)
                hist_moments[pl.ds(r, hist_len, stride=rows), :] = tile

    def turn(block, by):
        return pltpu.roll(block, by % LANES, 1) if by % LANES else block

    shifts = hist_len // 2 + 1
    entry = None
    for iteration in range(iters):
        stack_row = stack_rows.at[iteration]
        sheet_row = sheet_rows.at[iteration]
        sent = part_send.at[iteration]
        received = part_recv.at[iteration]
        last = iteration == iters - 1

        if iteration == 0:
            loads[0].wait()
            loads[1].wait()

            def gram(step, acc):
                acc = list(acc)
                for u in range(8):
                    t = step * 8 + u
                    x = res[:, lane_tile(t)]
                    y = x * w[pl.ds(t, 1), :]
                    for r in range(shifts):
                        acc[r] = acc[r] + y * (pltpu.roll(x, r, 0) if r else x)
                return tuple(acc)

            acc = tuple(jnp.zeros((SUBS, LANES), F32) for _ in range(shifts))
            acc = lax.fori_loop(0, tiles // 16, gram, acc)
            loads[2].wait()
            acc = lax.fori_loop(tiles // 16, tiles // 8, gram, acc)
            loads[3].wait()
            loads[4].wait()
            slot_row = jnp.zeros((1, LANES), F32)
            for b in range(batches):
                slot_row = jnp.where(lane_row == half + b, owner_slot[batch_atom[b]].astype(F32), slot_row)
            id_rows[pl.ds(in_sheet, 1)] = slot_row[None]
            packed = jnp.zeros((SUBS, LANES), F32)
            for r in range(shifts):
                packed = jnp.where(lane == hist_len * r + sub, jnp.sum(acc[r], axis=1, keepdims=True), packed)
            stack_row[pl.ds(in_stack, 1)] = (jnp.sum(packed, axis=0, keepdims=True) + slot_row)[None]
            pl.semaphore_wait(barrier, sum(group[0] - 1 for group in groups))
        else:
            slot = slot_index[iteration - 1]
            replaced = sub == slot

            def refresh(step, acc):
                for u in range(8):
                    t = step * 8 + u
                    new_res = jnp.where(replaced, fresh[pl.ds(t, 1), :], res[:, lane_tile(t)])
                    new_rho = jnp.where(replaced, density_out[pl.ds(t, 1), :], rho[:, lane_tile(t)])
                    res[:, lane_tile(t)] = new_res
                    rho[:, lane_tile(t)] = new_rho
                    acc = acc + fresh_w[pl.ds(t, 1), :] * new_res
                return acc

            acc = lax.fori_loop(0, tiles // 8, refresh, jnp.zeros((SUBS, LANES), F32))
            packed = jnp.where(lane == sub, jnp.sum(acc, axis=1, keepdims=True), 0.0)
            stack_row[pl.ds(in_stack, 1)] = jnp.sum(packed, axis=0, keepdims=True)[None]
        wait = exchange(stack_row, stack_group)
        if iteration == 0:
            wait_ids = exchange(id_rows, sheet_group)

        if iteration == 0:
            loads[5].wait()
        weigh()
        if iteration == 0:
            mine = hist_all.at[in_stack]
            for pair in range(hist_len // 2):
                turned = jnp.concatenate(
                    [
                        turn(hist_moments[(2 * pair + h) * rows : (2 * pair + h + 1) * rows], -32 * q)
                        for h in range(2)
                        for q in range(4)
                    ],
                    axis=0,
                )
                mine[pair] = jnp.transpose(turned)[0:harmonics]
            passed, across = channel(), channel()
            sibling = stack_peer((0, 1))[1]
            far = planes // 2
            near_steps = [(sign * hop) % planes for hop in (far // 2, 1) for sign in (1, -1)]

            def block_of(step):
                return hist_all.at[stack_peer((-step % planes, 0))[0]]

            def move(block, step, arrival):
                copy_to(block, block, across, stack_peer((step % planes, 0))[1], pass_sem.at[arrival]).start()

            def landed(block, arrival):
                pltpu.make_async_copy(block, block, pass_sem.at[arrival]).wait()

            def pass_on(block):
                copy_to(block, block, passed, sibling).start()

            for step in near_steps:
                move(mine, step, step)
            pass_on(mine)
            drained(hist_all.at[pl.ds(0, planes - 1)], across)
            wait_passed = waiter(hist_all, hist_all, passed, planes)
        else:
            fresh_rows = hist_moments[0:rows]
            slot_vec = jnp.zeros((rows, LANES), jnp.int32) + slot
            for i in range(1, hist_len):
                fresh_rows = jnp.where(slot_vec == i, hist_moments[i * rows : (i + 1) * rows], fresh_rows)
            turned = jnp.concatenate([turn(fresh_rows, -32 * q - 16 * h) for h in range(2) for q in range(4)], axis=0)
            new_moment = fresh_all.at[iteration - 1]
            new_moment[pl.ds(in_stack, 1)] = jnp.transpose(turned)[0 : 2 * SUBS][None]
            wait_fresh = exchange(new_moment, stack_group)

        wait()
        sheet_row[pl.ds(in_sheet, 1)] = total(stack_row, stack)[None]
        wait = exchange(sheet_row, sheet_group)

        if iteration == 0:
            ids = jnp.concatenate([stack_row[k] for k in range(stack)] * (LANES // stack), axis=0)
            ids = jnp.transpose(ids)
            for k in range(stack):
                source_cols[k * batches : (k + 1) * batches] = jnp.broadcast_to(
                    ids[half : half + batches, k : k + 1], (batches, LANES)
                )
            wait_ids()

            def fill(lanes, wanted):
                for k in range(mask.shape[0] // (2 * SUBS)):
                    at = slice(2 * SUBS * k, 2 * SUBS * (k + 1))
                    mask[at, lanes] = jnp.where(source_cols[at] == wanted, 1.0, 0.0).astype(jnp.bfloat16)

            @pl.loop(0, near_lanes // LANES)
            def _(t):
                pair = jnp.where(low_row, pltpu.roll(id_rows[2 * t], half, 1), id_rows[2 * t + 1])
                fill(lane_tile(t), pair)

            @pl.loop(0, sheet * share // LANES)
            def _(t):
                at = t * (LANES // share) + lane_row // share
                member = (at % spans) * cores + my_core
                held = member * owned + ((at // spans) * depth + lax.rem(my_plane, depth)) * share
                fill(lane_tile(t + near_lanes // LANES), (held + lane_row % share).astype(F32))

            for load in loads[6:]:
                load.wait()

        if iteration == 0:
            hops = far // 2
            for sign in (1, -1):
                block = block_of(sign * hops)
                landed(block, sign * hops % planes)
                part = pl.ds(0 if sign > 0 else hist_len // 4, hist_len // 4)
                move(block.at[part], sign * hops, far)
                move(block, sign * (far - 1 - hops), sign * (far - 1) % planes)
                pass_on(block)

        wait()
        row = total(sheet_row, sheet)
        if iteration == 0:
            entry = [[None] * (i + 1) for i in range(hist_len)]
            for i in range(hist_len):
                for j in range(i + 1):
                    r = i - j
                    at = hist_len * r + i if r < shifts else hist_len * (hist_len - r) + j
                    entry[i][j] = splat(row, at)
        else:
            news = [splat(row, k) for k in range(hist_len)]
            slot_vec = jnp.zeros((1, LANES), jnp.int32) + slot
            entry = [
                [
                    jnp.where(slot_vec == i, news[j], jnp.where(slot_vec == j, news[i], entry[i][j]))
                    for j in range(i + 1)
                ]
                for i in range(hist_len)
            ]
        coeffs = solve_coeffs(entry, hist_len)
        coeff_col = jnp.zeros((SUBS, LANES), F32)
        for i in range(hist_len):
            coeff_col = jnp.where(sub == i, coeffs[i], coeff_col)

        if iteration == 0:
            for step in (1, planes - 1, far - 1, planes - far + 1, far):
                block = block_of(step)
                landed(block, step)
                pass_on(block)
            wait_passed()
            old = coeffs
        else:
            wait_fresh()
            old = [jnp.where(slot_vec == i, 0.0, coeffs[i]) for i in range(hist_len)]
            new = coeffs[0]
            for i in range(1, hist_len):
                new = jnp.where(slot_vec == i, coeffs[i], new)

        gains = [jnp.where(low_row, old[2 * pair], old[2 * pair + 1]) for pair in range(hist_len // 2)]

        def mixed(at):
            top = tree(gains[pair] * hist_all[at, pair, 0:24] for pair in range(hist_len // 2))
            end = tree(gains[pair] * hist_all[at, pair, 24:25] for pair in range(hist_len // 2))
            return jnp.concatenate([top, jnp.broadcast_to(end, (SUBS, LANES))], axis=0)

        blocks = []
        for k in range(0, stack, 2):
            one, two = mixed(k), mixed(k + 1)
            block = jnp.where(low_wide, one, two) + pltpu.roll(jnp.where(low_wide, two, one), half, 1)
            if iteration:
                one, two = new_moment[k], new_moment[k + 1]
                upper = jnp.where(low, one, pltpu.roll(two, half, 1))
                lower = jnp.where(low, pltpu.roll(one, half, 1), two)
                block = block + new * jnp.concatenate([upper, lower], axis=0)
            blocks.append(block)
        everywhere = jnp.concatenate(blocks, axis=1)
        pieces = jnp.concatenate(split(everywhere), axis=0).astype(jnp.bfloat16)

        def gathered(first, count):
            out = jnp.dot(
                pieces, mask[:, pl.ds(pl.multiple_of(first, count), count)], preferred_element_type=F32
            )
            return out[0:32] + out[32:64] + out[64:96]

        if last:
            many = 2 * LANES // share
            each = LANES // share
            send, wait_own = scatter(own_send, own_recv, sheet_group)
            for first in range(0, sheet, many):
                out = gathered(near_lanes + first * share, many * share)
                for k in range(many):
                    tile = out[:, k // each * LANES : (k // each + 1) * LANES]
                    kept = jnp.zeros((SUBS, LANES), F32)
                    for g in range(4):
                        piece = tile[g * SUBS : (g + 1) * SUBS]
                        kept = jnp.where(quarter == g, turn(piece, (g - k % each) * 32), kept)
                    own_send[first + k] = kept
            own_recv[pl.ds(in_sheet, 1)] = own_send[pl.ds(in_sheet, 1)]
            for step in sheet_group[3]:
                send(step)

        send, wait = scatter(sent, received, sheet_group)
        for line_step in sorted(range(lines), key=lambda step: -ring(step, lines)):
            first = lax.rem(my_line + line_step, lines) * spans
            out = gathered(first * batches, spans * batches)
            for k in range(0, spans, 2):
                upper = out[0:16, k * batches : (k + 2) * batches]
                lower = out[16:32, k * batches : (k + 2) * batches]
                sent[first + k] = jnp.where(low, upper, pltpu.roll(lower, half, 1))
                sent[first + k + 1] = jnp.where(low, pltpu.roll(upper, half, 1), lower)
            for step in sheet_group[3]:
                if step[0] == line_step:
                    send(step)
        received[pl.ds(in_sheet, 1)] = sent[pl.ds(in_sheet, 1)]

        def base_step(step, carry):
            for u in range(8):
                t = step * 8 + u
                part = coeff_col * (rho[:, lane_tile(t)] + mixing_beta * res[:, lane_tile(t)])
                base_rows[pl.ds(t, 1), :] = jnp.sum(part, axis=0, keepdims=True)
            return carry

        lax.fori_loop(0, tiles // 8, base_step, 0)

        if last:
            wait_own()
            chunks[pl.ds(my_share, 1)] = (total(own_recv, sheet) * scale)[None]
            wait_chunks = exchange(chunks, share_group)

        wait()
        summed = total(received, sheet)
        at_batch = jnp.concatenate([summed, pltpu.roll(summed, half, 1)], axis=0) * scale
        comp = lax.broadcasted_iota(jnp.int32, (32, LANES), 0)
        degree = sum((comp >= (l + 1) * (l + 1)).astype(F32) for l in range(4))
        damped = jnp.where(comp < harmonics, at_batch * (mixing_beta / (1.0 + degree)), 0.0)

        def density_step(step, ahead):
            for u in range(16):
                b = step * 16 + u
                col = jnp.broadcast_to(ahead[:, u : u + 1], (32, LANES))
                for v in range(per_batch):
                    t = b * per_batch + v
                    part = col[24:32] * basis[24:25, lane_tile(t)]
                    for g in range(3):
                        part = part + col[g * SUBS : (g + 1) * SUBS] * basis[g * SUBS : (g + 1) * SUBS, lane_tile(t)]
                    correct[pl.ds(t, 1), :] = jnp.sum(part, axis=0, keepdims=True)
            return pltpu.roll(ahead, LANES - 16, 1)

        lax.fori_loop(0, batches // 16, density_step, damped)
        density = base_rows[...] - correct[...]
        density_out[...] = density
        if last:
            wait_chunks()
            each = LANES // share
            for t in range(owned // LANES):
                held = [chunks[t * each + k] for k in range(each)]
                for g in range(4):
                    tile = jnp.zeros((SUBS, LANES), F32)
                    for k in range(each):
                        tile = jnp.where(quarter == k, turn(held[k], (k - g) * 32), tile)
                    top = min(SUBS, harmonics - g * SUBS)
                    moments_out[g * SUBS : g * SUBS + top, t * LANES : (t + 1) * LANES] = tile[0:top]
        else:
            new = target[...] + coupling[...] * jnp.tanh(density) - density
            fresh[...] = new
            fresh_w[...] = new * w[...]
    for src, sem in sends:
        pltpu.make_async_copy(src, src, sem).wait()


def finish(density, moments, density_out, moments_out):
    density_out[...] = density[...]
    moments_out[...] = moments[...]


def local(weights, target, coupling, multipole_basis, rho_hist, res_hist, batch_atom, owner_slot, slot_index):
    harmonics, points = multipole_basis.shape
    hist_len = res_hist.shape[0]
    batches = batch_atom.shape[0]
    groups = lax.axis_size("grid")
    members = lax.axis_size("atom")
    lines, cores = 4, 2
    planes = groups // lines
    spans = members // cores
    stack, sheet = planes * cores, lines * spans
    shares = 4 * lines
    owned = owner_slot.shape[0] // members
    scale = 1.0 / math.sqrt(points * groups // owned)
    iters = slot_index.shape[0]
    cfg = (iters, hist_len, harmonics, batches, points // batches, owned, planes, lines, spans, cores, scale)
    tiles = points // LANES
    flat = (tiles, LANES)
    kinds = 3 * iters + 5 + (iters - 1)
    any_space = pl.BlockSpec(memory_space=pltpu.HBM)
    vmem = pl.BlockSpec(memory_space=pltpu.VMEM)
    density, moments = pl.pallas_call(
        functools.partial(kernel, cfg),
        out_shape=(jax.ShapeDtypeStruct(flat, F32), jax.ShapeDtypeStruct((harmonics, owned), F32)),
        in_specs=[any_space] * 9,
        out_specs=(vmem, vmem),
        scratch_shapes=[
            pltpu.VMEM(flat, F32),
            pltpu.VMEM(flat, F32),
            pltpu.VMEM(flat, F32),
            pltpu.VMEM((harmonics, points), F32),
            pltpu.VMEM((hist_len, points), F32),
            pltpu.VMEM((hist_len, points), F32),
            pltpu.VMEM(flat, F32),
            pltpu.VMEM(flat, F32),
            pltpu.VMEM((iters, stack, 1, LANES), F32),
            pltpu.VMEM((iters, sheet, 1, LANES), F32),
            pltpu.VMEM((sheet, 1, LANES), F32),
            pltpu.VMEM((stack, hist_len // 2, harmonics, LANES), F32),
            pltpu.VMEM((iters - 1, stack, 2 * SUBS, LANES), F32),
            pltpu.VMEM((iters, sheet, 2 * SUBS, LANES), F32),
            pltpu.VMEM((iters, sheet, 2 * SUBS, LANES), F32),
            pltpu.VMEM((sheet, SUBS, LANES), F32),
            pltpu.VMEM((sheet, SUBS, LANES), F32),
            pltpu.VMEM((shares, SUBS, LANES), F32),
            pltpu.VMEM((stack * batches, LANES), F32),
            pltpu.VMEM((stack * batches, sheet * (batches + owned // shares)), jnp.bfloat16),
            pltpu.VMEM((batches // 4 * hist_len, LANES), F32),
            pltpu.VMEM(flat, F32),
            pltpu.VMEM(flat, F32),
            pltpu.SMEM(batch_atom.shape, jnp.int32),
            pltpu.SMEM(owner_slot.shape, jnp.int32),
            pltpu.SMEM(slot_index.shape, jnp.int32),
            pltpu.SemaphoreType.DMA((10,)),
            pltpu.SemaphoreType.DMA((kinds,)),
            pltpu.SemaphoreType.DMA((kinds,)),
            pltpu.SemaphoreType.DMA((planes,)),
        ],
        compiler_params=pltpu.CompilerParams(
            collective_id=0, has_side_effects=True, vmem_limit_bytes=16777216
        ),
    )(
        *(
            pltpu.with_memory_space_constraint(array, pltpu.HBM)
            for array in (
                batch_atom,
                owner_slot,
                slot_index,
                weights.reshape(flat),
                target.reshape(flat),
                coupling.reshape(flat),
                multipole_basis,
                rho_hist,
                res_hist,
            )
        )
    )
    density, moments = pl.pallas_call(
        finish,
        out_shape=(jax.ShapeDtypeStruct(flat, F32), jax.ShapeDtypeStruct((harmonics, owned), F32)),
        in_specs=[vmem] * 2,
        out_specs=(vmem, vmem),
        compiler_params=pltpu.CompilerParams(vmem_limit_bytes=1048576),
    )(density, moments)
    return density.reshape(points), moments


def solution(mesh):
    both = ("grid", "atom")
    placed = (P(both), P(both), P(both), P(None, both), P(None, both), P(None, both), P(both), P(), P())
    return jax.shard_map(
        local,
        mesh=mesh,
        in_specs=placed,
        out_specs=(P(both), P(None, "atom")),
        check_vma=False,
    )
```

```python
import functools
import math

import jax
import jax.numpy as jnp
from jax import lax
from jax.experimental import pallas as pl
from jax.experimental.pallas import tpu as pltpu
from jax.sharding import PartitionSpec as P

MESH = pl.DeviceIdType.MESH
LANES = 128
SUBS = 8
mixing_beta = 0.5
ridge_share = 0.1
F32 = jnp.float32


def solve_coeffs(entry, hist_len):
    trace = entry[0][0]
    for i in range(1, hist_len):
        trace = trace + entry[i][i]
    ridge = (ridge_share / hist_len) * trace
    low = [[entry[i][j] for j in range(i + 1)] for i in range(hist_len)]
    for i in range(hist_len):
        low[i][i] = low[i][i] + ridge
    inverse = [None] * hist_len
    factor = [[None] * hist_len for _ in range(hist_len)]
    forward = [jnp.ones_like(trace) for _ in range(hist_len)]
    for j in range(hist_len):
        inverse[j] = 1.0 / low[j][j]
        for i in range(j + 1, hist_len):
            factor[i][j] = low[i][j] * inverse[j]
        for i in range(j + 1, hist_len):
            forward[i] = forward[i] - factor[i][j] * forward[j]
            for k in range(j + 1, i + 1):
                low[i][k] = low[i][k] - factor[i][j] * low[k][j]
    backward = [forward[i] * inverse[i] for i in range(hist_len)]
    for j in reversed(range(hist_len)):
        for i in range(j):
            backward[i] = backward[i] - factor[j][i] * backward[j]
    total = backward[0]
    for i in range(1, hist_len):
        total = total + backward[i]
    return [backward[i] / total for i in range(hist_len)]


def split(x):
    pieces = []
    for _ in range(3):
        piece = x.astype(jnp.bfloat16).astype(F32)
        pieces.append(piece)
        x = x - piece
    return pieces


def kernel(
    cfg,
    batch_atom_hbm,
    owner_slot_hbm,
    slot_index_hbm,
    w_hbm,
    target_hbm,
    coupling_hbm,
    basis_hbm,
    rho_hbm,
    res_hbm,
    density_out,
    moments_out,
    w,
    target,
    coupling,
    basis,
    rho,
    res,
    fresh,
    fresh_w,
    stack_rows,
    sheet_rows,
    id_rows,
    hist_all,
    fresh_all,
    part_send,
    part_recv,
    own_send,
    own_recv,
    chunks,
    source_cols,
    mask,
    hist_moments,
    base_rows,
    correct,
    batch_atom,
    owner_slot,
    slot_index,
    load_sem,
    send_sem,
    recv_sem,
    pass_sem,
):
    iters, hist_len, harmonics, batches, width, owned, planes, lines, spans, cores, scale = cfg
    tiles = w.shape[0]
    per_batch = width // LANES
    half = LANES // 2
    rows = batches // 4
    stack = planes * cores
    sheet = lines * spans
    near_lanes = sheet * batches
    shares = chunks.shape[0]
    depth = shares // lines
    share = owned // shares
    my_group = lax.axis_index("grid")
    my_member = lax.axis_index("atom")
    my_plane = lax.div(my_group, lines)
    my_line = lax.rem(my_group, lines)
    my_span = lax.div(my_member, cores)
    my_core = lax.rem(my_member, cores)
    in_stack = my_plane * cores + my_core
    in_sheet = my_line * spans + my_span
    my_share = my_line * depth + lax.rem(my_plane, depth)

    def ring(step, count):
        return min(step, count - step)

    def stack_peer(step):
        plane, core = lax.rem(my_plane + step[0], planes), lax.rem(my_core + step[1], cores)
        return plane * cores + core, (plane * lines + my_line, my_span * cores + core)

    def sheet_peer(step):
        line, span = lax.rem(my_line + step[0], lines), lax.rem(my_span + step[1], spans)
        return line * spans + span, (my_plane * lines + line, span * cores + my_core)

    def share_peer(step):
        line, plane = lax.rem(my_line + step[0], lines), lax.rem(my_plane + step[1], depth)
        device = (lax.div(my_plane, depth) * depth + plane) * lines + line, my_member
        return line * depth + plane, device

    def far_first(across, along):
        steps = [(a, b) for a in range(across) for b in range(along) if a or b]
        return sorted(steps, key=lambda step: -ring(step[0], across) - ring(step[1], along))

    stack_group = (stack, in_stack, stack_peer, far_first(planes, cores))
    sheet_group = (sheet, in_sheet, sheet_peer, far_first(lines, spans))
    share_group = (shares, my_share, share_peer, far_first(lines, depth))
    groups = (stack_group, sheet_group)
    barrier = pltpu.get_barrier_semaphore()
    for _, _, peer, steps in groups:
        for step in steps:
            pl.semaphore_signal(barrier, inc=1, device_id=peer(step)[1], device_id_type=MESH)

    first_half = pl.ds(0, tiles * LANES // 2)
    second_half = pl.ds(tiles * LANES // 2, tiles * LANES // 2)
    loads = [
        pltpu.make_async_copy(src, dst, load_sem.at[k])
        for k, (src, dst) in enumerate(
            (
                (w_hbm, w),
                (res_hbm.at[:, first_half], res.at[:, first_half]),
                (res_hbm.at[:, second_half], res.at[:, second_half]),
                (batch_atom_hbm, batch_atom),
                (owner_slot_hbm, owner_slot),
                (basis_hbm, basis),
                (slot_index_hbm, slot_index),
                (rho_hbm, rho),
                (target_hbm, target),
                (coupling_hbm, coupling),
            )
        )
    ]
    for load in loads:
        load.start()

    lane = lax.broadcasted_iota(jnp.int32, (SUBS, LANES), 1)
    sub = lax.broadcasted_iota(jnp.int32, (SUBS, LANES), 0)
    quarter = lane // 32
    lane_row = lax.broadcasted_iota(jnp.int32, (1, LANES), 1)
    low_row = lane_row < half
    low = lax.broadcasted_iota(jnp.int32, (2 * SUBS, LANES), 1) < half
    low_wide = lax.broadcasted_iota(jnp.int32, (32, LANES), 1) < half

    def lane_tile(t):
        return pl.ds(pl.multiple_of(t * LANES, LANES), LANES)

    kinds = []
    sends = []

    def channel():
        kinds.append(len(kinds))
        return kinds[-1]

    def copy_to(src, dst, which, device, arrival=None):
        return pltpu.make_async_remote_copy(
            src_ref=src,
            dst_ref=dst,
            send_sem=send_sem.at[which],
            recv_sem=recv_sem.at[which] if arrival is None else arrival,
            device_id=device,
            device_id_type=MESH,
        )

    def drained(src, which):
        sends.append((src, send_sem.at[which]))

    def waiter(src, dst, which, count):
        drained(src.at[pl.ds(0, count)], which)

        def wait():
            arrived = dst.at[pl.ds(0, count)]
            pltpu.make_async_copy(arrived, arrived, recv_sem.at[which]).wait()

        return wait

    def exchange(buf, group):
        count, mine, peer, steps = group
        which = channel()
        for step in steps:
            copy_to(buf.at[mine], buf.at[mine], which, peer(step)[1]).start()
        return waiter(buf, buf, which, count - 1)

    def scatter(src, dst, group):
        count, mine, peer, steps = group
        which = channel()

        def send(step):
            at, device = peer(step)
            copy_to(src.at[at], dst.at[mine], which, device).start()

        return send, waiter(src, dst, which, count - 1)

    def tree(parts):
        parts = list(parts)
        while len(parts) > 1:
            parts = [parts[k] + parts[k + 1] if k + 1 < len(parts) else parts[k] for k in range(0, len(parts), 2)]
        return parts[0]

    def total(buf, count):
        return tree(buf[k] for k in range(count))

    def splat(row, k):
        return jnp.broadcast_to(row[:, k : k + 1], (1, LANES))

    def weigh():
        @pl.loop(0, rows // 4)
        def _(step):
            for u in range(4):
                r = step * 4 + u
                xs, ys = [], []
                for q in range(4):
                    b = q * rows + r
                    at = pl.ds(pl.multiple_of(b * width, width), width)
                    gain = jnp.concatenate([w[pl.ds(b * per_batch + v, 1), :] for v in range(per_batch)], axis=1)
                    xs.extend(split(res[:, at] * gain))
                    ys.append(
                        jnp.concatenate([basis[0:24, at], jnp.broadcast_to(basis[24:25, at], (SUBS, width))], axis=0)
                    )
                x = jnp.concatenate(xs, axis=0).astype(jnp.bfloat16)
                out = None
                for y in split(jnp.concatenate(ys, axis=0)):
                    part = lax.dot_general(
                        x, y.astype(jnp.bfloat16), (((1,), (1,)), ((), ())), preferred_element_type=F32
                    )
                    out = part if out is None else out + part
                tile = jnp.zeros((SUBS, LANES), F32)
                for q in range(4):
                    block = out[24 * q : 24 * q + 8] + out[24 * q + 8 : 24 * q + 16] + out[24 * q + 16 : 24 * q + 24]
                    tile = jnp.where(quarter == q, block, tile)
                hist_moments[pl.ds(r, hist_len, stride=rows), :] = tile

    def turn(block, by):
        return pltpu.roll(block, by % LANES, 1) if by % LANES else block

    shifts = hist_len // 2 + 1
    entry = None
    for iteration in range(iters):
        stack_row = stack_rows.at[iteration]
        sheet_row = sheet_rows.at[iteration]
        sent = part_send.at[iteration]
        received = part_recv.at[iteration]
        last = iteration == iters - 1

        if iteration == 0:
            loads[0].wait()
            loads[1].wait()

            def gram(step, acc):
                acc = list(acc)
                for u in range(8):
                    t = step * 8 + u
                    x = res[:, lane_tile(t)]
                    y = x * w[pl.ds(t, 1), :]
                    for r in range(shifts):
                        acc[r] = acc[r] + y * (pltpu.roll(x, r, 0) if r else x)
                return tuple(acc)

            acc = tuple(jnp.zeros((SUBS, LANES), F32) for _ in range(shifts))
            acc = lax.fori_loop(0, tiles // 16, gram, acc)
            loads[2].wait()
            acc = lax.fori_loop(tiles // 16, tiles // 8, gram, acc)
            loads[3].wait()
            loads[4].wait()
            slot_row = jnp.zeros((1, LANES), F32)
            for b in range(batches):
                slot_row = jnp.where(lane_row == half + b, owner_slot[batch_atom[b]].astype(F32), slot_row)
            id_rows[pl.ds(in_sheet, 1)] = slot_row[None]
            packed = jnp.zeros((SUBS, LANES), F32)
            for r in range(shifts):
                packed = jnp.where(lane == hist_len * r + sub, jnp.sum(acc[r], axis=1, keepdims=True), packed)
            stack_row[pl.ds(in_stack, 1)] = (jnp.sum(packed, axis=0, keepdims=True) + slot_row)[None]
            loads[5].wait()
            weigh()
            mine = hist_all.at[in_stack]
            for pair in range(hist_len // 2):
                turned = jnp.concatenate(
                    [
                        turn(hist_moments[(2 * pair + h) * rows : (2 * pair + h + 1) * rows], -32 * q)
                        for h in range(2)
                        for q in range(4)
                    ],
                    axis=0,
                )
                mine[pair] = jnp.transpose(turned)[0:harmonics]
            pl.semaphore_wait(barrier, sum(group[0] - 1 for group in groups))
        else:
            slot = slot_index[iteration - 1]
            replaced = sub == slot

            def refresh(step, acc):
                for u in range(8):
                    t = step * 8 + u
                    new_res = jnp.where(replaced, fresh[pl.ds(t, 1), :], res[:, lane_tile(t)])
                    new_rho = jnp.where(replaced, density_out[pl.ds(t, 1), :], rho[:, lane_tile(t)])
                    res[:, lane_tile(t)] = new_res
                    rho[:, lane_tile(t)] = new_rho
                    acc = acc + fresh_w[pl.ds(t, 1), :] * new_res
                return acc

            acc = lax.fori_loop(0, tiles // 8, refresh, jnp.zeros((SUBS, LANES), F32))
            packed = jnp.where(lane == sub, jnp.sum(acc, axis=1, keepdims=True), 0.0)
            stack_row[pl.ds(in_stack, 1)] = jnp.sum(packed, axis=0, keepdims=True)[None]
        wait = exchange(stack_row, stack_group)
        if iteration == 0:
            wait_ids = exchange(id_rows, sheet_group)

        if iteration == 0:
            passed, across = channel(), channel()
            sibling = stack_peer((0, 1))[1]
            far = planes // 2
            near_steps = [(sign * hop) % planes for hop in (far // 2, 1) for sign in (1, -1)]

            def block_of(step):
                return hist_all.at[stack_peer((-step % planes, 0))[0]]

            def move(block, step, arrival):
                copy_to(block, block, across, stack_peer((step % planes, 0))[1], pass_sem.at[arrival]).start()

            def landed(block, arrival):
                pltpu.make_async_copy(block, block, pass_sem.at[arrival]).wait()

            def pass_on(block):
                copy_to(block, block, passed, sibling).start()

            for step in near_steps:
                move(mine, step, step)
            pass_on(mine)
            drained(hist_all.at[pl.ds(0, planes - 1)], across)
            wait_passed = waiter(hist_all, hist_all, passed, planes)
        else:
            weigh()
            fresh_rows = hist_moments[0:rows]
            slot_vec = jnp.zeros((rows, LANES), jnp.int32) + slot
            for i in range(1, hist_len):
                fresh_rows = jnp.where(slot_vec == i, hist_moments[i * rows : (i + 1) * rows], fresh_rows)
            turned = jnp.concatenate([turn(fresh_rows, -32 * q - 16 * h) for h in range(2) for q in range(4)], axis=0)
            new_moment = fresh_all.at[iteration - 1]
            new_moment[pl.ds(in_stack, 1)] = jnp.transpose(turned)[0 : 2 * SUBS][None]
            wait_fresh = exchange(new_moment, stack_group)

        wait()
        sheet_row[pl.ds(in_sheet, 1)] = total(stack_row, stack)[None]
        wait = exchange(sheet_row, sheet_group)

        if iteration == 0:
            hops = far // 2
            for sign in (1, -1):
                block = block_of(sign * hops)
                landed(block, sign * hops % planes)
                part = pl.ds(0 if sign > 0 else hist_len // 4, hist_len // 4)
                move(block.at[part], sign * hops, far)
                move(block, sign * (far - 1 - hops), sign * (far - 1) % planes)
                pass_on(block)

            ids = jnp.concatenate([stack_row[k] for k in range(stack)] * (LANES // stack), axis=0)
            ids = jnp.transpose(ids)
            for k in range(stack):
                source_cols[k * batches : (k + 1) * batches] = jnp.broadcast_to(
                    ids[half : half + batches, k : k + 1], (batches, LANES)
                )
            wait_ids()

            def fill(lanes, wanted):
                for k in range(mask.shape[0] // (2 * SUBS)):
                    at = slice(2 * SUBS * k, 2 * SUBS * (k + 1))
                    mask[at, lanes] = jnp.where(source_cols[at] == wanted, 1.0, 0.0).astype(jnp.bfloat16)

            @pl.loop(0, near_lanes // LANES)
            def _(t):
                pair = jnp.where(low_row, pltpu.roll(id_rows[2 * t], half, 1), id_rows[2 * t + 1])
                fill(lane_tile(t), pair)

            @pl.loop(0, sheet * share // LANES)
            def _(t):
                at = t * (LANES // share) + lane_row // share
                member = (at % spans) * cores + my_core
                held = member * owned + ((at // spans) * depth + lax.rem(my_plane, depth)) * share
                fill(lane_tile(t + near_lanes // LANES), (held + lane_row % share).astype(F32))

            for load in loads[6:]:
                load.wait()

        wait()
        row = total(sheet_row, sheet)
        if iteration == 0:
            entry = [[None] * (i + 1) for i in range(hist_len)]
            for i in range(hist_len):
                for j in range(i + 1):
                    r = i - j
                    at = hist_len * r + i if r < shifts else hist_len * (hist_len - r) + j
                    entry[i][j] = splat(row, at)
        else:
            news = [splat(row, k) for k in range(hist_len)]
            slot_vec = jnp.zeros((1, LANES), jnp.int32) + slot
            entry = [
                [
                    jnp.where(slot_vec == i, news[j], jnp.where(slot_vec == j, news[i], entry[i][j]))
                    for j in range(i + 1)
                ]
                for i in range(hist_len)
            ]
        coeffs = solve_coeffs(entry, hist_len)
        coeff_col = jnp.zeros((SUBS, LANES), F32)
        for i in range(hist_len):
            coeff_col = jnp.where(sub == i, coeffs[i], coeff_col)

        if iteration == 0:
            for step in (1, planes - 1, far - 1, planes - far + 1, far):
                block = block_of(step)
                landed(block, step)
                pass_on(block)
            wait_passed()
            old = coeffs
        else:
            wait_fresh()
            old = [jnp.where(slot_vec == i, 0.0, coeffs[i]) for i in range(hist_len)]
            new = coeffs[0]
            for i in range(1, hist_len):
                new = jnp.where(slot_vec == i, coeffs[i], new)

        gains = [jnp.where(low_row, old[2 * pair], old[2 * pair + 1]) for pair in range(hist_len // 2)]

        def mixed(at):
            top = tree(gains[pair] * hist_all[at, pair, 0:24] for pair in range(hist_len // 2))
            end = tree(gains[pair] * hist_all[at, pair, 24:25] for pair in range(hist_len // 2))
            return jnp.concatenate([top, jnp.broadcast_to(end, (SUBS, LANES))], axis=0)

        blocks = []
        for k in range(0, stack, 2):
            one, two = mixed(k), mixed(k + 1)
            block = jnp.where(low_wide, one, two) + pltpu.roll(jnp.where(low_wide, two, one), half, 1)
            if iteration:
                one, two = new_moment[k], new_moment[k + 1]
                upper = jnp.where(low, one, pltpu.roll(two, half, 1))
                lower = jnp.where(low, pltpu.roll(one, half, 1), two)
                block = block + new * jnp.concatenate([upper, lower], axis=0)
            blocks.append(block)
        everywhere = jnp.concatenate(blocks, axis=1)
        pieces = jnp.concatenate(split(everywhere), axis=0).astype(jnp.bfloat16)

        def gathered(first, count):
            out = jnp.dot(
                pieces, mask[:, pl.ds(pl.multiple_of(first, count), count)], preferred_element_type=F32
            )
            return out[0:32] + out[32:64] + out[64:96]

        if last:
            many = 2 * LANES // share
            each = LANES // share
            send, wait_own = scatter(own_send, own_recv, sheet_group)
            for first in range(0, sheet, many):
                out = gathered(near_lanes + first * share, many * share)
                for k in range(many):
                    tile = out[:, k // each * LANES : (k // each + 1) * LANES]
                    kept = jnp.zeros((SUBS, LANES), F32)
                    for g in range(4):
                        piece = tile[g * SUBS : (g + 1) * SUBS]
                        kept = jnp.where(quarter == g, turn(piece, (g - k % each) * 32), kept)
                    own_send[first + k] = kept
            own_recv[pl.ds(in_sheet, 1)] = own_send[pl.ds(in_sheet, 1)]
            for step in sheet_group[3]:
                send(step)

        send, wait = scatter(sent, received, sheet_group)
        for line_step in sorted(range(lines), key=lambda step: -ring(step, lines)):
            first = lax.rem(my_line + line_step, lines) * spans
            out = gathered(first * batches, spans * batches)
            for k in range(0, spans, 2):
                upper = out[0:16, k * batches : (k + 2) * batches]
                lower = out[16:32, k * batches : (k + 2) * batches]
                sent[first + k] = jnp.where(low, upper, pltpu.roll(lower, half, 1))
                sent[first + k + 1] = jnp.where(low, pltpu.roll(upper, half, 1), lower)
            for step in sheet_group[3]:
                if step[0] == line_step:
                    send(step)
        received[pl.ds(in_sheet, 1)] = sent[pl.ds(in_sheet, 1)]

        def base_step(step, carry):
            for u in range(8):
                t = step * 8 + u
                part = coeff_col * (rho[:, lane_tile(t)] + mixing_beta * res[:, lane_tile(t)])
                base_rows[pl.ds(t, 1), :] = jnp.sum(part, axis=0, keepdims=True)
            return carry

        lax.fori_loop(0, tiles // 8, base_step, 0)

        if last:
            wait_own()
            chunks[pl.ds(my_share, 1)] = (total(own_recv, sheet) * scale)[None]
            wait_chunks = exchange(chunks, share_group)

        wait()
        summed = total(received, sheet)
        at_batch = jnp.concatenate([summed, pltpu.roll(summed, half, 1)], axis=0) * scale
        comp = lax.broadcasted_iota(jnp.int32, (32, LANES), 0)
        degree = sum((comp >= (l + 1) * (l + 1)).astype(F32) for l in range(4))
        damped = jnp.where(comp < harmonics, at_batch * (mixing_beta / (1.0 + degree)), 0.0)

        def density_step(step, ahead):
            for u in range(16):
                b = step * 16 + u
                col = jnp.broadcast_to(ahead[:, u : u + 1], (32, LANES))
                for v in range(per_batch):
                    t = b * per_batch + v
                    part = col[24:32] * basis[24:25, lane_tile(t)]
                    for g in range(3):
                        part = part + col[g * SUBS : (g + 1) * SUBS] * basis[g * SUBS : (g + 1) * SUBS, lane_tile(t)]
                    correct[pl.ds(t, 1), :] = jnp.sum(part, axis=0, keepdims=True)
            return pltpu.roll(ahead, LANES - 16, 1)

        lax.fori_loop(0, batches // 16, density_step, damped)
        density = base_rows[...] - correct[...]
        density_out[...] = density
        if last:
            wait_chunks()
            each = LANES // share
            for t in range(owned // LANES):
                held = [chunks[t * each + k] for k in range(each)]
                for g in range(4):
                    tile = jnp.zeros((SUBS, LANES), F32)
                    for k in range(each):
                        tile = jnp.where(quarter == k, turn(held[k], (k - g) * 32), tile)
                    top = min(SUBS, harmonics - g * SUBS)
                    moments_out[g * SUBS : g * SUBS + top, t * LANES : (t + 1) * LANES] = tile[0:top]
        else:
            new = target[...] + coupling[...] * jnp.tanh(density) - density
            fresh[...] = new
            fresh_w[...] = new * w[...]
    for src, sem in sends:
        pltpu.make_async_copy(src, src, sem).wait()


def finish(density, moments, density_out, moments_out):
    density_out[...] = density[...]
    moments_out[...] = moments[...]


def local(weights, target, coupling, multipole_basis, rho_hist, res_hist, batch_atom, owner_slot, slot_index):
    harmonics, points = multipole_basis.shape
    hist_len = res_hist.shape[0]
    batches = batch_atom.shape[0]
    groups = lax.axis_size("grid")
    members = lax.axis_size("atom")
    lines, cores = 4, 2
    planes = groups // lines
    spans = members // cores
    stack, sheet = planes * cores, lines * spans
    shares = 4 * lines
    owned = owner_slot.shape[0] // members
    scale = 1.0 / math.sqrt(points * groups // owned)
    iters = slot_index.shape[0]
    cfg = (iters, hist_len, harmonics, batches, points // batches, owned, planes, lines, spans, cores, scale)
    tiles = points // LANES
    flat = (tiles, LANES)
    kinds = 3 * iters + 5 + (iters - 1)
    any_space = pl.BlockSpec(memory_space=pltpu.HBM)
    vmem = pl.BlockSpec(memory_space=pltpu.VMEM)
    density, moments = pl.pallas_call(
        functools.partial(kernel, cfg),
        out_shape=(jax.ShapeDtypeStruct(flat, F32), jax.ShapeDtypeStruct((harmonics, owned), F32)),
        in_specs=[any_space] * 9,
        out_specs=(vmem, vmem),
        scratch_shapes=[
            pltpu.VMEM(flat, F32),
            pltpu.VMEM(flat, F32),
            pltpu.VMEM(flat, F32),
            pltpu.VMEM((harmonics, points), F32),
            pltpu.VMEM((hist_len, points), F32),
            pltpu.VMEM((hist_len, points), F32),
            pltpu.VMEM(flat, F32),
            pltpu.VMEM(flat, F32),
            pltpu.VMEM((iters, stack, 1, LANES), F32),
            pltpu.VMEM((iters, sheet, 1, LANES), F32),
            pltpu.VMEM((sheet, 1, LANES), F32),
            pltpu.VMEM((stack, hist_len // 2, harmonics, LANES), F32),
            pltpu.VMEM((iters - 1, stack, 2 * SUBS, LANES), F32),
            pltpu.VMEM((iters, sheet, 2 * SUBS, LANES), F32),
            pltpu.VMEM((iters, sheet, 2 * SUBS, LANES), F32),
            pltpu.VMEM((sheet, SUBS, LANES), F32),
            pltpu.VMEM((sheet, SUBS, LANES), F32),
            pltpu.VMEM((shares, SUBS, LANES), F32),
            pltpu.VMEM((stack * batches, LANES), F32),
            pltpu.VMEM((stack * batches, sheet * (batches + owned // shares)), jnp.bfloat16),
            pltpu.VMEM((batches // 4 * hist_len, LANES), F32),
            pltpu.VMEM(flat, F32),
            pltpu.VMEM(flat, F32),
            pltpu.SMEM(batch_atom.shape, jnp.int32),
            pltpu.SMEM(owner_slot.shape, jnp.int32),
            pltpu.SMEM(slot_index.shape, jnp.int32),
            pltpu.SemaphoreType.DMA((10,)),
            pltpu.SemaphoreType.DMA((kinds,)),
            pltpu.SemaphoreType.DMA((kinds,)),
            pltpu.SemaphoreType.DMA((planes,)),
        ],
        compiler_params=pltpu.CompilerParams(
            collective_id=0, has_side_effects=True, vmem_limit_bytes=16777216
        ),
    )(
        *(
            pltpu.with_memory_space_constraint(array, pltpu.HBM)
            for array in (
                batch_atom,
                owner_slot,
                slot_index,
                weights.reshape(flat),
                target.reshape(flat),
                coupling.reshape(flat),
                multipole_basis,
                rho_hist,
                res_hist,
            )
        )
    )
    density, moments = pl.pallas_call(
        finish,
        out_shape=(jax.ShapeDtypeStruct(flat, F32), jax.ShapeDtypeStruct((harmonics, owned), F32)),
        in_specs=[vmem] * 2,
        out_specs=(vmem, vmem),
        compiler_params=pltpu.CompilerParams(vmem_limit_bytes=1048576),
    )(density, moments)
    return density.reshape(points), moments


def solution(mesh):
    both = ("grid", "atom")
    placed = (P(both), P(both), P(both), P(None, both), P(None, both), P(None, both), P(both), P(), P())
    return jax.shard_map(
        local,
        mesh=mesh,
        in_specs=placed,
        out_specs=(P(both), P(None, "atom")),
        check_vma=False,
    )
```

```python
import functools
import math

import jax
import jax.numpy as jnp
from jax import lax
from jax.experimental import pallas as pl
from jax.experimental.pallas import tpu as pltpu
from jax.sharding import PartitionSpec as P

MESH = pl.DeviceIdType.MESH
LANES = 128
SUBS = 8
mixing_beta = 0.5
ridge_share = 0.1
F32 = jnp.float32


def solve_coeffs(entry, hist_len):
    trace = entry[0][0]
    for i in range(1, hist_len):
        trace = trace + entry[i][i]
    ridge = (ridge_share / hist_len) * trace
    low = [[entry[i][j] for j in range(i + 1)] for i in range(hist_len)]
    for i in range(hist_len):
        low[i][i] = low[i][i] + ridge
    inverse = [None] * hist_len
    factor = [[None] * hist_len for _ in range(hist_len)]
    forward = [jnp.ones_like(trace) for _ in range(hist_len)]
    for j in range(hist_len):
        inverse[j] = 1.0 / low[j][j]
        for i in range(j + 1, hist_len):
            factor[i][j] = low[i][j] * inverse[j]
        for i in range(j + 1, hist_len):
            forward[i] = forward[i] - factor[i][j] * forward[j]
            for k in range(j + 1, i + 1):
                low[i][k] = low[i][k] - factor[i][j] * low[k][j]
    backward = [forward[i] * inverse[i] for i in range(hist_len)]
    for j in reversed(range(hist_len)):
        for i in range(j):
            backward[i] = backward[i] - factor[j][i] * backward[j]
    total = backward[0]
    for i in range(1, hist_len):
        total = total + backward[i]
    return [backward[i] / total for i in range(hist_len)]


def split(x, count=3):
    pieces = []
    for _ in range(count):
        piece = x.astype(jnp.bfloat16).astype(F32)
        pieces.append(piece)
        x = x - piece
    return pieces


def kernel(
    cfg,
    batch_atom_hbm,
    owner_slot_hbm,
    slot_index_hbm,
    w_hbm,
    target_hbm,
    coupling_hbm,
    basis_hbm,
    rho_hbm,
    res_hbm,
    density_out,
    moments_out,
    w,
    target,
    coupling,
    basis,
    rho,
    res,
    fresh,
    fresh_w,
    stack_rows,
    sheet_rows,
    id_rows,
    hist_all,
    fresh_all,
    part_send,
    part_recv,
    own_send,
    own_recv,
    chunks,
    source_cols,
    mask,
    hist_moments,
    base_rows,
    correct,
    batch_atom,
    owner_slot,
    slot_index,
    load_sem,
    send_sem,
    recv_sem,
    pass_sem,
):
    iters, hist_len, harmonics, batches, width, owned, planes, lines, spans, cores, scale = cfg
    tiles = w.shape[0]
    per_batch = width // LANES
    half = LANES // 2
    rows = batches // 4
    stack = planes * cores
    sheet = lines * spans
    near_lanes = sheet * batches
    shares = chunks.shape[0]
    depth = shares // lines
    share = owned // shares
    my_group = lax.axis_index("grid")
    my_member = lax.axis_index("atom")
    my_plane = lax.div(my_group, lines)
    my_line = lax.rem(my_group, lines)
    my_span = lax.div(my_member, cores)
    my_core = lax.rem(my_member, cores)
    in_stack = my_plane * cores + my_core
    in_sheet = my_line * spans + my_span
    my_share = my_line * depth + lax.rem(my_plane, depth)

    def ring(step, count):
        return min(step, count - step)

    def stack_peer(step):
        plane, core = lax.rem(my_plane + step[0], planes), lax.rem(my_core + step[1], cores)
        return plane * cores + core, (plane * lines + my_line, my_span * cores + core)

    def sheet_peer(step):
        line, span = lax.rem(my_line + step[0], lines), lax.rem(my_span + step[1], spans)
        return line * spans + span, (my_plane * lines + line, span * cores + my_core)

    def share_peer(step):
        line, plane = lax.rem(my_line + step[0], lines), lax.rem(my_plane + step[1], depth)
        device = (lax.div(my_plane, depth) * depth + plane) * lines + line, my_member
        return line * depth + plane, device

    def far_first(across, along):
        steps = [(a, b) for a in range(across) for b in range(along) if a or b]
        return sorted(steps, key=lambda step: -ring(step[0], across) - ring(step[1], along))

    stack_group = (stack, in_stack, stack_peer, far_first(planes, cores))
    sheet_group = (sheet, in_sheet, sheet_peer, far_first(lines, spans))
    share_group = (shares, my_share, share_peer, far_first(lines, depth))
    groups = (stack_group, sheet_group)
    barrier = pltpu.get_barrier_semaphore()
    for _, _, peer, steps in groups:
        for step in steps:
            pl.semaphore_signal(barrier, inc=1, device_id=peer(step)[1], device_id_type=MESH)

    quarters = [pl.ds(k * tiles * LANES // 4, tiles * LANES // 4) for k in range(4)]
    first_half = pl.ds(0, tiles * LANES // 2)
    second_half = pl.ds(tiles * LANES // 2, tiles * LANES // 2)
    loads = [
        pltpu.make_async_copy(src, dst, load_sem.at[k])
        for k, (src, dst) in enumerate(
            (
                (w_hbm, w),
                (res_hbm.at[:, first_half], res.at[:, first_half]),
                (res_hbm.at[:, second_half], res.at[:, second_half]),
                (batch_atom_hbm, batch_atom),
                (owner_slot_hbm, owner_slot),
                *((basis_hbm.at[:, part], basis.at[:, part]) for part in quarters),
                (slot_index_hbm, slot_index),
                (rho_hbm, rho),
                (target_hbm, target),
                (coupling_hbm, coupling),
            )
        )
    ]
    for load in loads:
        load.start()

    lane = lax.broadcasted_iota(jnp.int32, (SUBS, LANES), 1)
    sub = lax.broadcasted_iota(jnp.int32, (SUBS, LANES), 0)
    quarter = lane // 32
    lane_row = lax.broadcasted_iota(jnp.int32, (1, LANES), 1)
    low_row = lane_row < half
    low = lax.broadcasted_iota(jnp.int32, (2 * SUBS, LANES), 1) < half
    low_wide = lax.broadcasted_iota(jnp.int32, (32, LANES), 1) < half

    def lane_tile(t):
        return pl.ds(pl.multiple_of(t * LANES, LANES), LANES)

    kinds = []
    sends = []

    def channel():
        kinds.append(len(kinds))
        return kinds[-1]

    def copy_to(src, dst, which, device, arrival=None):
        return pltpu.make_async_remote_copy(
            src_ref=src,
            dst_ref=dst,
            send_sem=send_sem.at[which],
            recv_sem=recv_sem.at[which] if arrival is None else arrival,
            device_id=device,
            device_id_type=MESH,
        )

    def drained(src, which):
        sends.append((src, send_sem.at[which]))

    def waiter(src, dst, which, count):
        drained(src.at[pl.ds(0, count)], which)

        def wait():
            arrived = dst.at[pl.ds(0, count)]
            pltpu.make_async_copy(arrived, arrived, recv_sem.at[which]).wait()

        return wait

    def exchange(buf, group):
        count, mine, peer, steps = group
        which = channel()
        for step in steps:
            copy_to(buf.at[mine], buf.at[mine], which, peer(step)[1]).start()
        return waiter(buf, buf, which, count - 1)

    def scatter(src, dst, group):
        count, mine, peer, steps = group
        which = channel()

        def send(step):
            at, device = peer(step)
            copy_to(src.at[at], dst.at[mine], which, device).start()

        return send, waiter(src, dst, which, count - 1)

    def tree(parts):
        parts = list(parts)
        while len(parts) > 1:
            parts = [parts[k] + parts[k + 1] if k + 1 < len(parts) else parts[k] for k in range(0, len(parts), 2)]
        return parts[0]

    def total(buf, count):
        return tree(buf[k] for k in range(count))

    def splat(row, k):
        return jnp.broadcast_to(row[:, k : k + 1], (1, LANES))

    def weigh(weighted):
        @pl.loop(0, rows // 4)
        def _(step):
            for u in range(4):
                r = step * 4 + u
                xs, ys = [], []
                for q in range(4):
                    b = q * rows + r
                    at = pl.ds(pl.multiple_of(b * width, width), width)
                    xs.extend(split(weighted(b, at)))
                    ys.append(
                        jnp.concatenate([basis[0:24, at], jnp.broadcast_to(basis[24:25, at], (SUBS, width))], axis=0)
                    )
                x = jnp.concatenate(xs, axis=0).astype(jnp.bfloat16)
                out = None
                for y in split(jnp.concatenate(ys, axis=0), 2):
                    part = lax.dot_general(
                        x, y.astype(jnp.bfloat16), (((1,), (1,)), ((), ())), preferred_element_type=F32
                    )
                    out = part if out is None else out + part
                tile = jnp.zeros((SUBS, LANES), F32)
                for q in range(4):
                    block = out[24 * q : 24 * q + 8] + out[24 * q + 8 : 24 * q + 16] + out[24 * q + 16 : 24 * q + 24]
                    tile = jnp.where(quarter == q, block, tile)
                hist_moments[pl.ds(r, hist_len, stride=rows), :] = tile

    def batch_row(ref, b):
        return jnp.concatenate([ref[pl.ds(b * per_batch + v, 1), :] for v in range(per_batch)], axis=1)

    def weighted_hist(b, at):
        return res[:, at] * batch_row(w, b)

    def weighted_fresh(b, at):
        return jnp.broadcast_to(batch_row(fresh_w, b), (SUBS, width))

    def turn(block, by):
        return pltpu.roll(block, by % LANES, 1) if by % LANES else block

    shifts = hist_len // 2 + 1
    entry = None
    for iteration in range(iters):
        stack_row = stack_rows.at[iteration]
        sheet_row = sheet_rows.at[iteration]
        sent = part_send.at[iteration]
        received = part_recv.at[iteration]
        last = iteration == iters - 1

        if iteration == 0:
            loads[0].wait()
            loads[1].wait()

            def gram(step, acc):
                acc = list(acc)
                for u in range(8):
                    t = step * 8 + u
                    x = res[:, lane_tile(t)]
                    y = x * w[pl.ds(t, 1), :]
                    for r in range(shifts):
                        acc[r] = acc[r] + y * (pltpu.roll(x, r, 0) if r else x)
                return tuple(acc)

            acc = tuple(jnp.zeros((SUBS, LANES), F32) for _ in range(shifts))
            acc = lax.fori_loop(0, tiles // 16, gram, acc)
            loads[2].wait()
            acc = lax.fori_loop(tiles // 16, tiles // 8, gram, acc)
            loads[3].wait()
            loads[4].wait()
            id_row = jnp.zeros((1, LANES), F32)
            for b in range(batches):
                id_row = jnp.where(lane_row == half + b, owner_slot[batch_atom[b]].astype(F32), id_row)
            id_rows[pl.ds(in_sheet, 1)] = id_row[None]
            packed = jnp.zeros((SUBS, LANES), F32)
            for r in range(shifts):
                packed = jnp.where(lane == hist_len * r + sub, jnp.sum(acc[r], axis=1, keepdims=True), packed)
            stack_row[pl.ds(in_stack, 1)] = (jnp.sum(packed, axis=0, keepdims=True) + id_row)[None]
            for load in loads[5:9]:
                load.wait()
            weigh(weighted_hist)
            mine = hist_all.at[in_stack]
            for pair in range(hist_len // 2):
                turned = jnp.concatenate(
                    [
                        turn(hist_moments[(2 * pair + h) * rows : (2 * pair + h + 1) * rows], -32 * q)
                        for h in range(2)
                        for q in range(4)
                    ],
                    axis=0,
                )
                mine[pair] = jnp.transpose(turned)[0:harmonics]
            pl.semaphore_wait(barrier, sum(group[0] - 1 for group in groups))
        else:
            slot = slot_index[iteration - 1]
            slot_row = jnp.zeros((1, LANES), jnp.int32) + slot

            def refresh(step, acc):
                acc, own = acc
                for u in range(8):
                    t = step * 8 + u
                    acc = acc + fresh_w[pl.ds(t, 1), :] * res[:, lane_tile(t)]
                rows_at = pl.ds(pl.multiple_of(step * 8, 8), 8)
                return acc, own + fresh_w[rows_at, :] * fresh[rows_at, :]

            zero = jnp.zeros((SUBS, LANES), F32)
            acc, own = lax.fori_loop(0, tiles // 8, refresh, (zero, zero))
            acc = jnp.where(sub == slot, jnp.sum(own, axis=0, keepdims=True), acc)
            packed = jnp.where(lane == sub, jnp.sum(acc, axis=1, keepdims=True), 0.0)
            stack_row[pl.ds(in_stack, 1)] = jnp.sum(packed, axis=0, keepdims=True)[None]
        wait = exchange(stack_row, stack_group)
        if iteration == 0:
            wait_ids = exchange(id_rows, sheet_group)

        if iteration == 0:
            passed, across = channel(), channel()
            sibling = stack_peer((0, 1))[1]
            far = planes // 2

            def block_of(step):
                return hist_all.at[stack_peer((-step % planes, 0))[0]]

            def move(block, step, arrival):
                copy_to(block, block, across, stack_peer((step % planes, 0))[1], pass_sem.at[arrival]).start()

            def landed(block, arrival):
                pltpu.make_async_copy(block, block, pass_sem.at[arrival]).wait()

            def relay(k):
                for sign in (1, -1):
                    block = block_of(sign * hops).at[parts[k]]
                    landed(block, sign * hops % planes if k else planes + (sign < 0))
                    if (sign < 0) == bool(k):
                        move(block, sign * hops, far)
                    move(block, sign * (far - 1 - hops), sign * (far - 1) % planes)
                    pass_on(block)

            def pass_on(block):
                copy_to(block, block, passed, sibling).start()

            parts = [pl.ds(k * hist_len // 4, hist_len // 4) for k in range(2)]
            hops = far // 2
            for k in range(2):
                for sign in (1, -1):
                    move(mine.at[parts[k]], sign * hops, sign * hops % planes if k else planes + (sign < 0))
            for sign in (1, -1):
                move(mine, sign, sign % planes)
            pass_on(mine)
            drained(hist_all.at[pl.ds(0, planes - 1)], across)
            wait_passed = waiter(hist_all, hist_all, passed, planes)
        else:
            weigh(weighted_fresh)
            fresh_rows = hist_moments[0:rows]
            turned = jnp.concatenate([turn(fresh_rows, -32 * q - 16 * h) for h in range(2) for q in range(4)], axis=0)
            new_moment = fresh_all.at[iteration - 1]
            new_moment[pl.ds(in_stack, 1)] = jnp.transpose(turned)[0 : 2 * SUBS][None]
            wait_fresh = exchange(new_moment, stack_group)

        if iteration == 0:
            relay(0)
        wait()
        sheet_row[pl.ds(in_sheet, 1)] = total(stack_row, stack)[None]
        wait = exchange(sheet_row, sheet_group)

        if iteration == 0:
            relay(1)

            ids = jnp.concatenate([stack_row[k] for k in range(stack)] * (LANES // stack), axis=0)
            ids = jnp.transpose(ids)
            for k in range(stack):
                source_cols[k * batches : (k + 1) * batches] = jnp.broadcast_to(
                    ids[half : half + batches, k : k + 1], (batches, LANES)
                )
            wait_ids()

            def fill(lanes, wanted):
                for k in range(mask.shape[0] // (2 * SUBS)):
                    at = slice(2 * SUBS * k, 2 * SUBS * (k + 1))
                    mask[at, lanes] = jnp.where(source_cols[at] == wanted, 1.0, 0.0).astype(jnp.bfloat16)

            @pl.loop(0, near_lanes // LANES)
            def _(t):
                pair = jnp.where(low_row, pltpu.roll(id_rows[2 * t], half, 1), id_rows[2 * t + 1])
                fill(lane_tile(t), pair)

            @pl.loop(0, sheet * share // LANES)
            def _(t):
                at = t * (LANES // share) + lane_row // share
                member = (at % spans) * cores + my_core
                held = member * owned + ((at // spans) * depth + lax.rem(my_plane, depth)) * share
                fill(lane_tile(t + near_lanes // LANES), (held + lane_row % share).astype(F32))

            for load in loads[9:]:
                load.wait()

        wait()
        row = total(sheet_row, sheet)
        if iteration == 0:
            entry = [[None] * (i + 1) for i in range(hist_len)]
            for i in range(hist_len):
                for j in range(i + 1):
                    r = i - j
                    at = hist_len * r + i if r < shifts else hist_len * (hist_len - r) + j
                    entry[i][j] = splat(row, at)
        else:
            news = [splat(row, k) for k in range(hist_len)]
            entry = [
                [
                    jnp.where(slot_row == i, news[j], jnp.where(slot_row == j, news[i], entry[i][j]))
                    for j in range(i + 1)
                ]
                for i in range(hist_len)
            ]
        coeffs = solve_coeffs(entry, hist_len)

        if iteration == 0:
            for step in (1, planes - 1, far - 1, planes - far + 1, far):
                block = block_of(step)
                landed(block, step)
                pass_on(block)
            wait_passed()
            old = coeffs
        else:
            wait_fresh()
            old = [jnp.where(slot_row == i, 0.0, coeffs[i]) for i in range(hist_len)]
            new = coeffs[0]
            for i in range(1, hist_len):
                new = jnp.where(slot_row == i, coeffs[i], new)

        coeff_col = jnp.zeros((SUBS, LANES), F32)
        for i in range(hist_len):
            coeff_col = jnp.where(sub == i, old[i], coeff_col)

        gains = [jnp.where(low_row, old[2 * pair], old[2 * pair + 1]) for pair in range(hist_len // 2)]

        def mixed(at):
            top = tree(gains[pair] * hist_all[at, pair, 0:24] for pair in range(hist_len // 2))
            end = tree(gains[pair] * hist_all[at, pair, 24:25] for pair in range(hist_len // 2))
            return jnp.concatenate([top, jnp.broadcast_to(end, (SUBS, LANES))], axis=0)

        blocks = []
        for k in range(0, stack, 2):
            one, two = mixed(k), mixed(k + 1)
            block = jnp.where(low_wide, one, two) + pltpu.roll(jnp.where(low_wide, two, one), half, 1)
            if iteration:
                one, two = new_moment[k], new_moment[k + 1]
                upper = jnp.where(low, one, pltpu.roll(two, half, 1))
                lower = jnp.where(low, pltpu.roll(one, half, 1), two)
                block = block + new * jnp.concatenate([upper, lower], axis=0)
            blocks.append(block)
        everywhere = jnp.concatenate(blocks, axis=1)
        pieces = jnp.concatenate(split(everywhere), axis=0).astype(jnp.bfloat16)

        def gathered(first, count):
            out = jnp.dot(
                pieces, mask[:, pl.ds(pl.multiple_of(first, count), count)], preferred_element_type=F32
            )
            return out[0:32] + out[32:64] + out[64:96]

        if last:
            many = 2 * LANES // share
            each = LANES // share
            send, wait_own = scatter(own_send, own_recv, sheet_group)
            for first in range(0, sheet, many):
                out = gathered(near_lanes + first * share, many * share)
                for k in range(many):
                    tile = out[:, k // each * LANES : (k // each + 1) * LANES]
                    kept = jnp.zeros((SUBS, LANES), F32)
                    for g in range(4):
                        piece = tile[g * SUBS : (g + 1) * SUBS]
                        kept = jnp.where(quarter == g, turn(piece, (g - k % each) * 32), kept)
                    own_send[first + k] = kept
            own_recv[pl.ds(in_sheet, 1)] = own_send[pl.ds(in_sheet, 1)]
            for step in sheet_group[3]:
                send(step)

        send, wait = scatter(sent, received, sheet_group)
        for line_step in sorted(range(lines), key=lambda step: -ring(step, lines)):
            first = lax.rem(my_line + line_step, lines) * spans
            out = gathered(first * batches, spans * batches)
            for k in range(0, spans, 2):
                upper = out[0:16, k * batches : (k + 2) * batches]
                lower = out[16:32, k * batches : (k + 2) * batches]
                sent[first + k] = jnp.where(low, upper, pltpu.roll(lower, half, 1))
                sent[first + k + 1] = jnp.where(low, pltpu.roll(upper, half, 1), lower)
            for step in sheet_group[3]:
                if step[0] == line_step:
                    send(step)
        received[pl.ds(in_sheet, 1)] = sent[pl.ds(in_sheet, 1)]

        def base_step(step, carry):
            for u in range(8):
                t = step * 8 + u
                part = coeff_col * (rho[:, lane_tile(t)] + mixing_beta * res[:, lane_tile(t)])
                base_rows[pl.ds(t, 1), :] = jnp.sum(part, axis=0, keepdims=True)
            return carry

        lax.fori_loop(0, tiles // 8, base_step, 0)

        if last:
            wait_own()
            chunks[pl.ds(my_share, 1)] = (total(own_recv, sheet) * scale)[None]
            wait_chunks = exchange(chunks, share_group)

        wait()
        summed = total(received, sheet)
        at_batch = jnp.concatenate([summed, pltpu.roll(summed, half, 1)], axis=0) * scale
        comp = lax.broadcasted_iota(jnp.int32, (32, LANES), 0)
        degree = sum((comp >= (l + 1) * (l + 1)).astype(F32) for l in range(4))
        damped = jnp.where(comp < harmonics, at_batch * (mixing_beta / (1.0 + degree)), 0.0)

        def density_step(step, ahead):
            for u in range(16):
                b = step * 16 + u
                col = jnp.broadcast_to(ahead[:, u : u + 1], (32, LANES))
                for v in range(per_batch):
                    t = b * per_batch + v
                    part = col[24:32] * basis[24:25, lane_tile(t)]
                    for g in range(3):
                        part = part + col[g * SUBS : (g + 1) * SUBS] * basis[g * SUBS : (g + 1) * SUBS, lane_tile(t)]
                    correct[pl.ds(t, 1), :] = jnp.sum(part, axis=0, keepdims=True)
            return pltpu.roll(ahead, LANES - 16, 1)

        lax.fori_loop(0, batches // 16, density_step, damped)
        density = base_rows[...] - correct[...]
        if iteration:
            density = density + new * (density_out[...] + mixing_beta * fresh[...])
        density_out[...] = density
        if last:
            wait_chunks()
            each = LANES // share
            for t in range(owned // LANES):
                held = [chunks[t * each + k] for k in range(each)]
                for g in range(4):
                    tile = jnp.zeros((SUBS, LANES), F32)
                    for k in range(each):
                        tile = jnp.where(quarter == k, turn(held[k], (k - g) * 32), tile)
                    top = min(SUBS, harmonics - g * SUBS)
                    moments_out[g * SUBS : g * SUBS + top, t * LANES : (t + 1) * LANES] = tile[0:top]
        else:
            made = target[...] + coupling[...] * jnp.tanh(density) - density
            fresh[...] = made
            fresh_w[...] = made * w[...]
    for src, sem in sends:
        pltpu.make_async_copy(src, src, sem).wait()


def finish(density, moments, density_out, moments_out):
    density_out[...] = density[...]
    moments_out[...] = moments[...]


def local(weights, target, coupling, multipole_basis, rho_hist, res_hist, batch_atom, owner_slot, slot_index):
    harmonics, points = multipole_basis.shape
    hist_len = res_hist.shape[0]
    batches = batch_atom.shape[0]
    groups = lax.axis_size("grid")
    members = lax.axis_size("atom")
    lines, cores = 4, 2
    planes = groups // lines
    spans = members // cores
    stack, sheet = planes * cores, lines * spans
    shares = 4 * lines
    owned = owner_slot.shape[0] // members
    scale = 1.0 / math.sqrt(points * groups // owned)
    iters = slot_index.shape[0]
    cfg = (iters, hist_len, harmonics, batches, points // batches, owned, planes, lines, spans, cores, scale)
    tiles = points // LANES
    flat = (tiles, LANES)
    kinds = 3 * iters + 5 + (iters - 1)
    any_space = pl.BlockSpec(memory_space=pltpu.HBM)
    vmem = pl.BlockSpec(memory_space=pltpu.VMEM)
    density, moments = pl.pallas_call(
        functools.partial(kernel, cfg),
        out_shape=(jax.ShapeDtypeStruct(flat, F32), jax.ShapeDtypeStruct((harmonics, owned), F32)),
        in_specs=[any_space] * 9,
        out_specs=(vmem, vmem),
        scratch_shapes=[
            pltpu.VMEM(flat, F32),
            pltpu.VMEM(flat, F32),
            pltpu.VMEM(flat, F32),
            pltpu.VMEM((harmonics, points), F32),
            pltpu.VMEM((hist_len, points), F32),
            pltpu.VMEM((hist_len, points), F32),
            pltpu.VMEM(flat, F32),
            pltpu.VMEM(flat, F32),
            pltpu.VMEM((iters, stack, 1, LANES), F32),
            pltpu.VMEM((iters, sheet, 1, LANES), F32),
            pltpu.VMEM((sheet, 1, LANES), F32),
            pltpu.VMEM((stack, hist_len // 2, harmonics, LANES), F32),
            pltpu.VMEM((iters - 1, stack, 2 * SUBS, LANES), F32),
            pltpu.VMEM((iters, sheet, 2 * SUBS, LANES), F32),
            pltpu.VMEM((iters, sheet, 2 * SUBS, LANES), F32),
            pltpu.VMEM((sheet, SUBS, LANES), F32),
            pltpu.VMEM((sheet, SUBS, LANES), F32),
            pltpu.VMEM((shares, SUBS, LANES), F32),
            pltpu.VMEM((stack * batches, LANES), F32),
            pltpu.VMEM((stack * batches, sheet * (batches + owned // shares)), jnp.bfloat16),
            pltpu.VMEM((batches // 4 * hist_len, LANES), F32),
            pltpu.VMEM(flat, F32),
            pltpu.VMEM(flat, F32),
            pltpu.SMEM(batch_atom.shape, jnp.int32),
            pltpu.SMEM(owner_slot.shape, jnp.int32),
            pltpu.SMEM(slot_index.shape, jnp.int32),
            pltpu.SemaphoreType.DMA((13,)),
            pltpu.SemaphoreType.DMA((kinds,)),
            pltpu.SemaphoreType.DMA((kinds,)),
            pltpu.SemaphoreType.DMA((planes + 2,)),
        ],
        compiler_params=pltpu.CompilerParams(
            collective_id=0, has_side_effects=True, vmem_limit_bytes=16777216
        ),
    )(
        *(
            pltpu.with_memory_space_constraint(array, pltpu.HBM)
            for array in (
                batch_atom,
                owner_slot,
                slot_index,
                weights.reshape(flat),
                target.reshape(flat),
                coupling.reshape(flat),
                multipole_basis,
                rho_hist,
                res_hist,
            )
        )
    )
    density, moments = pl.pallas_call(
        finish,
        out_shape=(jax.ShapeDtypeStruct(flat, F32), jax.ShapeDtypeStruct((harmonics, owned), F32)),
        in_specs=[vmem] * 2,
        out_specs=(vmem, vmem),
        compiler_params=pltpu.CompilerParams(vmem_limit_bytes=1048576),
    )(density, moments)
    return density.reshape(points), moments


def solution(mesh):
    both = ("grid", "atom")
    placed = (P(both), P(both), P(both), P(None, both), P(None, both), P(None, both), P(both), P(), P())
    return jax.shard_map(
        local,
        mesh=mesh,
        in_specs=placed,
        out_specs=(P(both), P(None, "atom")),
        check_vma=False,
    )
```

```python
import functools
import math

import jax
import jax.numpy as jnp
from jax import lax
from jax.experimental import pallas as pl
from jax.experimental.pallas import tpu as pltpu
from jax.sharding import PartitionSpec as P

MESH = pl.DeviceIdType.MESH
LANES = 128
SUBS = 8
mixing_beta = 0.5
ridge_share = 0.1
F32 = jnp.float32


def solve_coeffs(entry, hist_len):
    trace = entry[0][0]
    for i in range(1, hist_len):
        trace = trace + entry[i][i]
    ridge = (ridge_share / hist_len) * trace
    low = [[entry[i][j] for j in range(i + 1)] for i in range(hist_len)]
    for i in range(hist_len):
        low[i][i] = low[i][i] + ridge
    inverse = [None] * hist_len
    factor = [[None] * hist_len for _ in range(hist_len)]
    forward = [jnp.ones_like(trace) for _ in range(hist_len)]
    for j in range(hist_len):
        inverse[j] = 1.0 / low[j][j]
        for i in range(j + 1, hist_len):
            factor[i][j] = low[i][j] * inverse[j]
        for i in range(j + 1, hist_len):
            forward[i] = forward[i] - factor[i][j] * forward[j]
            for k in range(j + 1, i + 1):
                low[i][k] = low[i][k] - factor[i][j] * low[k][j]
    backward = [forward[i] * inverse[i] for i in range(hist_len)]
    for j in reversed(range(hist_len)):
        for i in range(j):
            backward[i] = backward[i] - factor[j][i] * backward[j]
    total = backward[0]
    for i in range(1, hist_len):
        total = total + backward[i]
    return [backward[i] / total for i in range(hist_len)]


def split(x, count=3):
    pieces = []
    for _ in range(count):
        piece = x.astype(jnp.bfloat16).astype(F32)
        pieces.append(piece)
        x = x - piece
    return pieces


def kernel(
    cfg,
    batch_atom_hbm,
    owner_slot_hbm,
    slot_index_hbm,
    w_hbm,
    target_hbm,
    coupling_hbm,
    basis_hbm,
    rho_hbm,
    res_hbm,
    density_out,
    moments_out,
    w,
    target,
    coupling,
    basis,
    rho,
    res,
    fresh,
    fresh_w,
    stack_rows,
    sheet_rows,
    id_rows,
    hist_all,
    fresh_all,
    part_send,
    part_recv,
    own_send,
    own_recv,
    old_send,
    old_recv,
    old_pieces,
    chunks,
    source_cols,
    mask,
    hist_moments,
    base_rows,
    correct,
    batch_atom,
    owner_slot,
    slot_index,
    load_sem,
    send_sem,
    recv_sem,
    pass_sem,
):
    iters, hist_len, harmonics, batches, width, owned, planes, lines, spans, cores, scale = cfg
    tiles = w.shape[0]
    per_batch = width // LANES
    half = LANES // 2
    rows = batches // 4
    stack = planes * cores
    sheet = lines * spans
    near_lanes = sheet * batches
    shares = chunks.shape[0]
    depth = shares // lines
    share = owned // shares
    my_group = lax.axis_index("grid")
    my_member = lax.axis_index("atom")
    my_plane = lax.div(my_group, lines)
    my_line = lax.rem(my_group, lines)
    my_span = lax.div(my_member, cores)
    my_core = lax.rem(my_member, cores)
    in_stack = my_plane * cores + my_core
    in_sheet = my_line * spans + my_span
    my_share = my_line * depth + lax.rem(my_plane, depth)

    def ring(step, count):
        return min(step, count - step)

    def stack_peer(step):
        plane, core = lax.rem(my_plane + step[0], planes), lax.rem(my_core + step[1], cores)
        return plane * cores + core, (plane * lines + my_line, my_span * cores + core)

    def sheet_peer(step):
        line, span = lax.rem(my_line + step[0], lines), lax.rem(my_span + step[1], spans)
        return line * spans + span, (my_plane * lines + line, span * cores + my_core)

    def share_peer(step):
        line, plane = lax.rem(my_line + step[0], lines), lax.rem(my_plane + step[1], depth)
        device = (lax.div(my_plane, depth) * depth + plane) * lines + line, my_member
        return line * depth + plane, device

    def far_first(across, along):
        steps = [(a, b) for a in range(across) for b in range(along) if a or b]
        return sorted(steps, key=lambda step: -ring(step[0], across) - ring(step[1], along))

    stack_group = (stack, in_stack, stack_peer, far_first(planes, cores))
    sheet_group = (sheet, in_sheet, sheet_peer, far_first(lines, spans))
    share_group = (shares, my_share, share_peer, far_first(lines, depth))
    groups = (stack_group, sheet_group)
    barrier = pltpu.get_barrier_semaphore()
    for _, _, peer, steps in groups:
        for step in steps:
            pl.semaphore_signal(barrier, inc=1, device_id=peer(step)[1], device_id_type=MESH)

    quarters = [pl.ds(k * tiles * LANES // 4, tiles * LANES // 4) for k in range(4)]
    first_half = pl.ds(0, tiles * LANES // 2)
    second_half = pl.ds(tiles * LANES // 2, tiles * LANES // 2)
    loads = [
        pltpu.make_async_copy(src, dst, load_sem.at[k])
        for k, (src, dst) in enumerate(
            (
                (w_hbm, w),
                (res_hbm.at[:, first_half], res.at[:, first_half]),
                (res_hbm.at[:, second_half], res.at[:, second_half]),
                (batch_atom_hbm, batch_atom),
                (owner_slot_hbm, owner_slot),
                *((basis_hbm.at[:, part], basis.at[:, part]) for part in quarters),
                (slot_index_hbm, slot_index),
                (rho_hbm, rho),
                (target_hbm, target),
                (coupling_hbm, coupling),
            )
        )
    ]
    for load in loads:
        load.start()

    lane = lax.broadcasted_iota(jnp.int32, (SUBS, LANES), 1)
    sub = lax.broadcasted_iota(jnp.int32, (SUBS, LANES), 0)
    quarter = lane // 32
    lane_row = lax.broadcasted_iota(jnp.int32, (1, LANES), 1)
    low_row = lane_row < half
    low = lax.broadcasted_iota(jnp.int32, (2 * SUBS, LANES), 1) < half
    low_wide = lax.broadcasted_iota(jnp.int32, (32, LANES), 1) < half

    def lane_tile(t):
        return pl.ds(pl.multiple_of(t * LANES, LANES), LANES)

    kinds = []
    sends = []

    def channel():
        kinds.append(len(kinds))
        return kinds[-1]

    def copy_to(src, dst, which, device, arrival=None):
        return pltpu.make_async_remote_copy(
            src_ref=src,
            dst_ref=dst,
            send_sem=send_sem.at[which],
            recv_sem=recv_sem.at[which] if arrival is None else arrival,
            device_id=device,
            device_id_type=MESH,
        )

    def drained(src, which):
        sends.append((src, send_sem.at[which]))

    def waiter(src, dst, which, count):
        drained(src.at[pl.ds(0, count)], which)

        def wait():
            arrived = dst.at[pl.ds(0, count)]
            pltpu.make_async_copy(arrived, arrived, recv_sem.at[which]).wait()

        return wait

    def exchange(buf, group):
        count, mine, peer, steps = group
        which = channel()
        for step in steps:
            copy_to(buf.at[mine], buf.at[mine], which, peer(step)[1]).start()
        return waiter(buf, buf, which, count - 1)

    def scatter(src, dst, group):
        count, mine, peer, steps = group
        which = channel()

        def send(step):
            at, device = peer(step)
            copy_to(src.at[at], dst.at[mine], which, device).start()

        return send, waiter(src, dst, which, count - 1)

    def tree(parts):
        parts = list(parts)
        while len(parts) > 1:
            parts = [parts[k] + parts[k + 1] if k + 1 < len(parts) else parts[k] for k in range(0, len(parts), 2)]
        return parts[0]

    def total(buf, count):
        return tree(buf[k] for k in range(count))

    def splat(row, k):
        return jnp.broadcast_to(row[:, k : k + 1], (1, LANES))

    def weigh(weighted):
        @pl.loop(0, rows // 4)
        def _(step):
            for u in range(4):
                r = step * 4 + u
                xs, ys = [], []
                for q in range(4):
                    b = q * rows + r
                    at = pl.ds(pl.multiple_of(b * width, width), width)
                    xs.extend(split(weighted(b, at)))
                    ys.append(
                        jnp.concatenate([basis[0:24, at], jnp.broadcast_to(basis[24:25, at], (SUBS, width))], axis=0)
                    )
                x = jnp.concatenate(xs, axis=0).astype(jnp.bfloat16)
                out = None
                for y in split(jnp.concatenate(ys, axis=0), 2):
                    part = lax.dot_general(
                        x, y.astype(jnp.bfloat16), (((1,), (1,)), ((), ())), preferred_element_type=F32
                    )
                    out = part if out is None else out + part
                tile = jnp.zeros((SUBS, LANES), F32)
                for q in range(4):
                    block = out[24 * q : 24 * q + 8] + out[24 * q + 8 : 24 * q + 16] + out[24 * q + 16 : 24 * q + 24]
                    tile = jnp.where(quarter == q, block, tile)
                hist_moments[pl.ds(r, hist_len, stride=rows), :] = tile

    def batch_row(ref, b):
        return jnp.concatenate([ref[pl.ds(b * per_batch + v, 1), :] for v in range(per_batch)], axis=1)

    def weighted_hist(b, at):
        return res[:, at] * batch_row(w, b)

    def weighted_fresh(b, at):
        return jnp.broadcast_to(batch_row(fresh_w, b), (SUBS, width))

    def turn(block, by):
        return pltpu.roll(block, by % LANES, 1) if by % LANES else block

    def unfold(one, two):
        upper = jnp.where(low, one, pltpu.roll(two, half, 1))
        lower = jnp.where(low, pltpu.roll(one, half, 1), two)
        return jnp.concatenate([upper, lower], axis=0)

    def in_pieces(blocks):
        everywhere = jnp.concatenate(blocks, axis=1)
        return jnp.concatenate(split(everywhere), axis=0).astype(jnp.bfloat16)

    def gathered(pieces, first, count):
        return jnp.dot(pieces, mask[:, pl.ds(pl.multiple_of(first, count), count)], preferred_element_type=F32)

    def joined(out):
        return out[0:32] + out[32:64] + out[64:96]

    many = 2 * LANES // share
    each = LANES // share

    def kept(out, k):
        tile = out[:, k // each * LANES : (k // each + 1) * LANES]
        result = jnp.zeros((SUBS, LANES), F32)
        for g in range(4):
            piece = tile[g * SUBS : (g + 1) * SUBS]
            result = jnp.where(quarter == g, turn(piece, (g - k % each) * 32), result)
        return result

    shifts = hist_len // 2 + 1
    entry = None
    for iteration in range(iters):
        stack_row = stack_rows.at[iteration]
        sheet_row = sheet_rows.at[iteration]
        sent = part_send.at[iteration]
        received = part_recv.at[iteration]
        last = iteration == iters - 1

        if iteration == 0:
            loads[0].wait()
            loads[1].wait()

            def gram(step, acc):
                acc = list(acc)
                for u in range(8):
                    t = step * 8 + u
                    x = res[:, lane_tile(t)]
                    y = x * w[pl.ds(t, 1), :]
                    for r in range(shifts):
                        acc[r] = acc[r] + y * (pltpu.roll(x, r, 0) if r else x)
                return tuple(acc)

            acc = tuple(jnp.zeros((SUBS, LANES), F32) for _ in range(shifts))
            acc = lax.fori_loop(0, tiles // 16, gram, acc)
            loads[2].wait()
            acc = lax.fori_loop(tiles // 16, tiles // 8, gram, acc)
            loads[3].wait()
            loads[4].wait()
            id_row = jnp.zeros((1, LANES), F32)
            for b in range(batches):
                id_row = jnp.where(lane_row == half + b, owner_slot[batch_atom[b]].astype(F32), id_row)
            id_rows[pl.ds(in_sheet, 1)] = id_row[None]
            packed = jnp.zeros((SUBS, LANES), F32)
            for r in range(shifts):
                packed = jnp.where(lane == hist_len * r + sub, jnp.sum(acc[r], axis=1, keepdims=True), packed)
            stack_row[pl.ds(in_stack, 1)] = (jnp.sum(packed, axis=0, keepdims=True) + id_row)[None]
            for load in loads[5:9]:
                load.wait()
            weigh(weighted_hist)
            mine = hist_all.at[in_stack]
            for pair in range(hist_len // 2):
                turned = jnp.concatenate(
                    [
                        turn(hist_moments[(2 * pair + h) * rows : (2 * pair + h + 1) * rows], -32 * q)
                        for h in range(2)
                        for q in range(4)
                    ],
                    axis=0,
                )
                mine[pair] = jnp.transpose(turned)[0:harmonics]
            pl.semaphore_wait(barrier, sum(group[0] - 1 for group in groups))
        else:
            slot = slot_index[iteration - 1]
            slot_row = jnp.zeros((1, LANES), jnp.int32) + slot

            def refresh(step, acc):
                acc, own = acc
                for u in range(8):
                    t = step * 8 + u
                    acc = acc + fresh_w[pl.ds(t, 1), :] * res[:, lane_tile(t)]
                rows_at = pl.ds(pl.multiple_of(step * 8, 8), 8)
                return acc, own + fresh_w[rows_at, :] * fresh[rows_at, :]

            zero = jnp.zeros((SUBS, LANES), F32)
            acc, own = lax.fori_loop(0, tiles // 8, refresh, (zero, zero))
            acc = jnp.where(sub == slot, jnp.sum(own, axis=0, keepdims=True), acc)
            packed = jnp.where(lane == sub, jnp.sum(acc, axis=1, keepdims=True), 0.0)
            stack_row[pl.ds(in_stack, 1)] = jnp.sum(packed, axis=0, keepdims=True)[None]
        wait = exchange(stack_row, stack_group)
        if iteration == 0:
            wait_ids = exchange(id_rows, sheet_group)

        if iteration == 0:
            passed, across = channel(), channel()
            sibling = stack_peer((0, 1))[1]
            far = planes // 2

            def block_of(step):
                return hist_all.at[stack_peer((-step % planes, 0))[0]]

            def move(block, step, arrival):
                copy_to(block, block, across, stack_peer((step % planes, 0))[1], pass_sem.at[arrival]).start()

            def landed(block, arrival):
                pltpu.make_async_copy(block, block, pass_sem.at[arrival]).wait()

            def relay(k):
                for sign in (1, -1):
                    block = block_of(sign * hops).at[parts[k]]
                    landed(block, sign * hops % planes if k else planes + (sign < 0))
                    if (sign < 0) == bool(k):
                        move(block, sign * hops, far)
                    move(block, sign * (far - 1 - hops), sign * (far - 1) % planes)
                    pass_on(block)

            def pass_on(block):
                copy_to(block, block, passed, sibling).start()

            parts = [pl.ds(k * hist_len // 4, hist_len // 4) for k in range(2)]
            hops = far // 2
            for k in range(2):
                for sign in (1, -1):
                    move(mine.at[parts[k]], sign * hops, sign * hops % planes if k else planes + (sign < 0))
            for sign in (1, -1):
                move(mine, sign, sign % planes)
            pass_on(mine)
            drained(hist_all.at[pl.ds(0, planes - 1)], across)
            wait_passed = waiter(hist_all, hist_all, passed, planes)
        else:
            weigh(weighted_fresh)
            fresh_rows = hist_moments[0:rows]
            turned = jnp.concatenate([turn(fresh_rows, -32 * q - 16 * h) for h in range(2) for q in range(4)], axis=0)
            new_moment = fresh_all.at[iteration - 1]
            new_moment[pl.ds(in_stack, 1)] = jnp.transpose(turned)[0 : 2 * SUBS][None]
            wait_fresh = exchange(new_moment, stack_group)

        if iteration == 0:
            relay(0)
        wait()
        sheet_row[pl.ds(in_sheet, 1)] = total(stack_row, stack)[None]
        wait = exchange(sheet_row, sheet_group)

        if iteration == 0:
            relay(1)

            ids = jnp.concatenate([stack_row[k] for k in range(stack)] * (LANES // stack), axis=0)
            ids = jnp.transpose(ids)
            for k in range(stack):
                source_cols[k * batches : (k + 1) * batches] = jnp.broadcast_to(
                    ids[half : half + batches, k : k + 1], (batches, LANES)
                )
            wait_ids()

            def fill(lanes, wanted):
                for k in range(mask.shape[0] // (2 * SUBS)):
                    at = slice(2 * SUBS * k, 2 * SUBS * (k + 1))
                    mask[at, lanes] = jnp.where(source_cols[at] == wanted, 1.0, 0.0).astype(jnp.bfloat16)

            @pl.loop(0, near_lanes // LANES)
            def _(t):
                pair = jnp.where(low_row, pltpu.roll(id_rows[2 * t], half, 1), id_rows[2 * t + 1])
                fill(lane_tile(t), pair)

            @pl.loop(0, sheet * share // LANES)
            def _(t):
                at = t * (LANES // share) + lane_row // share
                member = (at % spans) * cores + my_core
                held = member * owned + ((at // spans) * depth + lax.rem(my_plane, depth)) * share
                fill(lane_tile(t + near_lanes // LANES), (held + lane_row % share).astype(F32))

            for load in loads[9:]:
                load.wait()

        if iteration:
            wait_fresh()
            fresh_blocks = [unfold(new_moment[k], new_moment[k + 1]) for k in range(0, stack, 2)]
            pieces = in_pieces(fresh_blocks)
            send, wait_own = scatter(own_send, own_recv, sheet_group)
            for first in range(0, sheet, many):
                out = joined(gathered(pieces, near_lanes + first * share, many * share))
                for k in range(many):
                    own_send[first + k] = kept(out, k)
            own_recv[pl.ds(in_sheet, 1)] = own_send[pl.ds(in_sheet, 1)]
            for step in sheet_group[3]:
                send(step)
            wait_old()
            held_old = [tree(old_recv[k, i] for k in range(sheet)) for i in range(hist_len)]

        wait()
        row = total(sheet_row, sheet)
        if iteration == 0:
            entry = [[None] * (i + 1) for i in range(hist_len)]
            for i in range(hist_len):
                for j in range(i + 1):
                    r = i - j
                    at = hist_len * r + i if r < shifts else hist_len * (hist_len - r) + j
                    entry[i][j] = splat(row, at)
        else:
            news = [splat(row, k) for k in range(hist_len)]
            entry = [
                [
                    jnp.where(slot_row == i, news[j], jnp.where(slot_row == j, news[i], entry[i][j]))
                    for j in range(i + 1)
                ]
                for i in range(hist_len)
            ]
        coeffs = solve_coeffs(entry, hist_len)

        if iteration == 0:
            for step in (1, planes - 1, far - 1, planes - far + 1, far):
                block = block_of(step)
                landed(block, step)
                pass_on(block)
            wait_passed()
            old = coeffs
        else:
            old = [jnp.where(slot_row == i, 0.0, coeffs[i]) for i in range(hist_len)]
            new = coeffs[0]
            for i in range(1, hist_len):
                new = jnp.where(slot_row == i, coeffs[i], new)

        coeff_col = jnp.zeros((SUBS, LANES), F32)
        for i in range(hist_len):
            coeff_col = jnp.where(sub == i, old[i], coeff_col)

        gains = [jnp.where(low_row, old[2 * pair], old[2 * pair + 1]) for pair in range(hist_len // 2)]

        def mixed(at):
            top = tree(gains[pair] * hist_all[at, pair, 0:24] for pair in range(hist_len // 2))
            end = tree(gains[pair] * hist_all[at, pair, 24:25] for pair in range(hist_len // 2))
            return jnp.concatenate([top, jnp.broadcast_to(end, (SUBS, LANES))], axis=0)

        blocks = []
        for k in range(0, stack, 2):
            one, two = mixed(k), mixed(k + 1)
            block = jnp.where(low_wide, one, two) + pltpu.roll(jnp.where(low_wide, two, one), half, 1)
            if iteration:
                one, two = new_moment[k], new_moment[k + 1]
                block = block + new * unfold(one, two)
            blocks.append(block)
        pieces = in_pieces(blocks)

        send, wait = scatter(sent, received, sheet_group)
        for line_step in sorted(range(lines), key=lambda step: -ring(step, lines)):
            first = lax.rem(my_line + line_step, lines) * spans
            out = joined(gathered(pieces, first * batches, spans * batches))
            for k in range(0, spans, 2):
                upper = out[0:16, k * batches : (k + 2) * batches]
                lower = out[16:32, k * batches : (k + 2) * batches]
                sent[first + k] = jnp.where(low, upper, pltpu.roll(lower, half, 1))
                sent[first + k + 1] = jnp.where(low, pltpu.roll(upper, half, 1), lower)
            for step in sheet_group[3]:
                if step[0] == line_step:
                    send(step)
        received[pl.ds(in_sheet, 1)] = sent[pl.ds(in_sheet, 1)]

        def base_step(step, carry):
            for u in range(8):
                t = step * 8 + u
                part = coeff_col * (rho[:, lane_tile(t)] + mixing_beta * res[:, lane_tile(t)])
                base_rows[pl.ds(t, 1), :] = jnp.sum(part, axis=0, keepdims=True)
            return carry

        lax.fori_loop(0, tiles // 8, base_step, 0)

        if iteration == 0:
            @pl.loop(0, hist_len // 2)
            def _(pair):
                ones = [hist_all[k, pair, 0:24] for k in range(stack)]
                ends = [jnp.broadcast_to(hist_all[k, pair, 24:25], (SUBS, LANES)) for k in range(stack)]
                rows_of = [jnp.concatenate([ones[k], ends[k]], axis=0) for k in range(stack)]
                firsts, seconds = [], []
                for k in range(0, stack, 2):
                    one, two = rows_of[k], rows_of[k + 1]
                    firsts.append(jnp.where(low_wide, one, pltpu.roll(two, half, 1)))
                    seconds.append(jnp.where(low_wide, pltpu.roll(one, half, 1), two))
                old_pieces[pl.ds(pl.multiple_of(pair * 192, 192), 96)] = in_pieces(firsts)
                old_pieces[pl.ds(pl.multiple_of(pair * 192 + 96, 96), 96)] = in_pieces(seconds)

            send, wait_old = scatter(old_send, old_recv, sheet_group)
            for first in range(0, sheet, many):
                out = gathered(old_pieces[...], near_lanes + first * share, many * share)
                for i in range(hist_len):
                    part = joined(out[i * 96 : (i + 1) * 96])
                    for k in range(many):
                        old_send[first + k, i] = kept(part, k)
            old_recv[pl.ds(in_sheet, 1)] = old_send[pl.ds(in_sheet, 1)]
            for step in sheet_group[3]:
                send(step)

        if last:
            wait_own()
            held = new * total(own_recv, sheet) + tree(old[i] * held_old[i] for i in range(hist_len))
            chunks[pl.ds(my_share, 1)] = (held * scale)[None]
            wait_chunks = exchange(chunks, share_group)

        wait()
        summed = total(received, sheet)
        at_batch = jnp.concatenate([summed, pltpu.roll(summed, half, 1)], axis=0) * scale
        comp = lax.broadcasted_iota(jnp.int32, (32, LANES), 0)
        degree = sum((comp >= (l + 1) * (l + 1)).astype(F32) for l in range(4))
        damped = jnp.where(comp < harmonics, at_batch * (mixing_beta / (1.0 + degree)), 0.0)

        def density_step(step, ahead):
            for u in range(16):
                b = step * 16 + u
                col = jnp.broadcast_to(ahead[:, u : u + 1], (32, LANES))
                for v in range(per_batch):
                    t = b * per_batch + v
                    part = col[24:32] * basis[24:25, lane_tile(t)]
                    for g in range(3):
                        part = part + col[g * SUBS : (g + 1) * SUBS] * basis[g * SUBS : (g + 1) * SUBS, lane_tile(t)]
                    correct[pl.ds(t, 1), :] = jnp.sum(part, axis=0, keepdims=True)
            return pltpu.roll(ahead, LANES - 16, 1)

        lax.fori_loop(0, batches // 16, density_step, damped)
        density = base_rows[...] - correct[...]
        if iteration:
            density = density + new * (density_out[...] + mixing_beta * fresh[...])
        density_out[...] = density
        if last:
            wait_chunks()
            for t in range(owned // LANES):
                held = [chunks[t * each + k] for k in range(each)]
                for g in range(4):
                    tile = jnp.zeros((SUBS, LANES), F32)
                    for k in range(each):
                        tile = jnp.where(quarter == k, turn(held[k], (k - g) * 32), tile)
                    top = min(SUBS, harmonics - g * SUBS)
                    moments_out[g * SUBS : g * SUBS + top, t * LANES : (t + 1) * LANES] = tile[0:top]
        else:
            made = target[...] + coupling[...] * jnp.tanh(density) - density
            fresh[...] = made
            fresh_w[...] = made * w[...]
    for src, sem in sends:
        pltpu.make_async_copy(src, src, sem).wait()


def finish(density, moments, density_out, moments_out):
    density_out[...] = density[...]
    moments_out[...] = moments[...]


def local(weights, target, coupling, multipole_basis, rho_hist, res_hist, batch_atom, owner_slot, slot_index):
    harmonics, points = multipole_basis.shape
    hist_len = res_hist.shape[0]
    batches = batch_atom.shape[0]
    groups = lax.axis_size("grid")
    members = lax.axis_size("atom")
    lines, cores = 4, 2
    planes = groups // lines
    spans = members // cores
    stack, sheet = planes * cores, lines * spans
    shares = 4 * lines
    owned = owner_slot.shape[0] // members
    scale = 1.0 / math.sqrt(points * groups // owned)
    iters = slot_index.shape[0]
    cfg = (iters, hist_len, harmonics, batches, points // batches, owned, planes, lines, spans, cores, scale)
    tiles = points // LANES
    flat = (tiles, LANES)
    kinds = 3 * iters + 6 + (iters - 1)
    any_space = pl.BlockSpec(memory_space=pltpu.HBM)
    vmem = pl.BlockSpec(memory_space=pltpu.VMEM)
    density, moments = pl.pallas_call(
        functools.partial(kernel, cfg),
        out_shape=(jax.ShapeDtypeStruct(flat, F32), jax.ShapeDtypeStruct((harmonics, owned), F32)),
        in_specs=[any_space] * 9,
        out_specs=(vmem, vmem),
        scratch_shapes=[
            pltpu.VMEM(flat, F32),
            pltpu.VMEM(flat, F32),
            pltpu.VMEM(flat, F32),
            pltpu.VMEM((harmonics, points), F32),
            pltpu.VMEM((hist_len, points), F32),
            pltpu.VMEM((hist_len, points), F32),
            pltpu.VMEM(flat, F32),
            pltpu.VMEM(flat, F32),
            pltpu.VMEM((iters, stack, 1, LANES), F32),
            pltpu.VMEM((iters, sheet, 1, LANES), F32),
            pltpu.VMEM((sheet, 1, LANES), F32),
            pltpu.VMEM((stack, hist_len // 2, harmonics, LANES), F32),
            pltpu.VMEM((iters - 1, stack, 2 * SUBS, LANES), F32),
            pltpu.VMEM((iters, sheet, 2 * SUBS, LANES), F32),
            pltpu.VMEM((iters, sheet, 2 * SUBS, LANES), F32),
            pltpu.VMEM((sheet, SUBS, LANES), F32),
            pltpu.VMEM((sheet, SUBS, LANES), F32),
            pltpu.VMEM((sheet, hist_len, SUBS, LANES), F32),
            pltpu.VMEM((sheet, hist_len, SUBS, LANES), F32),
            pltpu.VMEM((hist_len * 96, stack * batches), jnp.bfloat16),
            pltpu.VMEM((shares, SUBS, LANES), F32),
            pltpu.VMEM((stack * batches, LANES), F32),
            pltpu.VMEM((stack * batches, sheet * (batches + owned // shares)), jnp.bfloat16),
            pltpu.VMEM((batches // 4 * hist_len, LANES), F32),
            pltpu.VMEM(flat, F32),
            pltpu.VMEM(flat, F32),
            pltpu.SMEM(batch_atom.shape, jnp.int32),
            pltpu.SMEM(owner_slot.shape, jnp.int32),
            pltpu.SMEM(slot_index.shape, jnp.int32),
            pltpu.SemaphoreType.DMA((13,)),
            pltpu.SemaphoreType.DMA((kinds,)),
            pltpu.SemaphoreType.DMA((kinds,)),
            pltpu.SemaphoreType.DMA((planes + 2,)),
        ],
        compiler_params=pltpu.CompilerParams(
            collective_id=0, has_side_effects=True, vmem_limit_bytes=16777216
        ),
    )(
        *(
            pltpu.with_memory_space_constraint(array, pltpu.HBM)
            for array in (
                batch_atom,
                owner_slot,
                slot_index,
                weights.reshape(flat),
                target.reshape(flat),
                coupling.reshape(flat),
                multipole_basis,
                rho_hist,
                res_hist,
            )
        )
    )
    density, moments = pl.pallas_call(
        finish,
        out_shape=(jax.ShapeDtypeStruct(flat, F32), jax.ShapeDtypeStruct((harmonics, owned), F32)),
        in_specs=[vmem] * 2,
        out_specs=(vmem, vmem),
        compiler_params=pltpu.CompilerParams(vmem_limit_bytes=1048576),
    )(density, moments)
    return density.reshape(points), moments


def solution(mesh):
    both = ("grid", "atom")
    placed = (P(both), P(both), P(both), P(None, both), P(None, both), P(None, both), P(both), P(), P())
    return jax.shard_map(
        local,
        mesh=mesh,
        in_specs=placed,
        out_specs=(P(both), P(None, "atom")),
        check_vma=False,
    )
```

```python
import functools
import math

import jax
import jax.numpy as jnp
from jax import lax
from jax.experimental import pallas as pl
from jax.experimental.pallas import tpu as pltpu
from jax.sharding import PartitionSpec as P

MESH = pl.DeviceIdType.MESH
LANES = 128
SUBS = 8
mixing_beta = 0.5
ridge_share = 0.1
F32 = jnp.float32


def solve_coeffs(entry, hist_len):
    trace = entry[0][0]
    for i in range(1, hist_len):
        trace = trace + entry[i][i]
    ridge = (ridge_share / hist_len) * trace
    low = [[entry[i][j] for j in range(i + 1)] for i in range(hist_len)]
    for i in range(hist_len):
        low[i][i] = low[i][i] + ridge
    inverse = [None] * hist_len
    factor = [[None] * hist_len for _ in range(hist_len)]
    forward = [jnp.ones_like(trace) for _ in range(hist_len)]
    for j in range(hist_len):
        inverse[j] = 1.0 / low[j][j]
        for i in range(j + 1, hist_len):
            factor[i][j] = low[i][j] * inverse[j]
        for i in range(j + 1, hist_len):
            forward[i] = forward[i] - factor[i][j] * forward[j]
            for k in range(j + 1, i + 1):
                low[i][k] = low[i][k] - factor[i][j] * low[k][j]
    backward = [forward[i] * inverse[i] for i in range(hist_len)]
    for j in reversed(range(hist_len)):
        for i in range(j):
            backward[i] = backward[i] - factor[j][i] * backward[j]
    total = backward[0]
    for i in range(1, hist_len):
        total = total + backward[i]
    return [backward[i] / total for i in range(hist_len)]


def split(x, count=3):
    pieces = []
    for _ in range(count):
        piece = x.astype(jnp.bfloat16).astype(F32)
        pieces.append(piece)
        x = x - piece
    return pieces


def kernel(
    cfg,
    batch_atom_hbm,
    owner_slot_hbm,
    slot_index_hbm,
    w_hbm,
    target_hbm,
    coupling_hbm,
    basis_hbm,
    rho_hbm,
    res_hbm,
    density_out,
    moments_out,
    w,
    target,
    coupling,
    basis,
    rho,
    res,
    fresh,
    fresh_w,
    stack_rows,
    sheet_rows,
    id_rows,
    hist_all,
    fresh_all,
    part_send,
    part_recv,
    own_send,
    own_recv,
    old_send,
    old_recv,
    old_pieces,
    basis_pieces,
    early_sum,
    near_sum,
    chunks,
    source_cols,
    near_cols,
    mask,
    hist_moments,
    base_rows,
    correct,
    batch_atom,
    owner_slot,
    slot_index,
    load_sem,
    send_sem,
    recv_sem,
    pass_sem,
):
    iters, hist_len, harmonics, batches, width, owned, planes, lines, spans, cores, scale = cfg
    tiles = w.shape[0]
    per_batch = width // LANES
    half = LANES // 2
    rows = batches // 4
    stack = planes * cores
    sheet = lines * spans
    near_lanes = sheet * batches
    shares = chunks.shape[0]
    depth = shares // lines
    share = owned // shares
    my_group = lax.axis_index("grid")
    my_member = lax.axis_index("atom")
    my_plane = lax.div(my_group, lines)
    my_line = lax.rem(my_group, lines)
    my_span = lax.div(my_member, cores)
    my_core = lax.rem(my_member, cores)
    in_stack = my_plane * cores + my_core
    in_sheet = my_line * spans + my_span
    my_share = my_line * depth + lax.rem(my_plane, depth)

    def ring(step, count):
        return min(step, count - step)

    def stack_peer(step):
        plane, core = lax.rem(my_plane + step[0], planes), lax.rem(my_core + step[1], cores)
        return plane * cores + core, (plane * lines + my_line, my_span * cores + core)

    def sheet_peer(step):
        line, span = lax.rem(my_line + step[0], lines), lax.rem(my_span + step[1], spans)
        return line * spans + span, (my_plane * lines + line, span * cores + my_core)

    def share_peer(step):
        line, plane = lax.rem(my_line + step[0], lines), lax.rem(my_plane + step[1], depth)
        device = (lax.div(my_plane, depth) * depth + plane) * lines + line, my_member
        return line * depth + plane, device

    def far_first(across, along):
        steps = [(a, b) for a in range(across) for b in range(along) if a or b]
        return sorted(steps, key=lambda step: -ring(step[0], across) - ring(step[1], along))

    stack_group = (stack, in_stack, stack_peer, far_first(planes, cores))
    sheet_group = (sheet, in_sheet, sheet_peer, far_first(lines, spans))
    share_group = (shares, my_share, share_peer, far_first(lines, depth))
    groups = (stack_group, sheet_group)
    far = planes // 2
    arrivals = [0, 1, -1] + [sign * hop for hop in range(2, far) for sign in (1, -1)] + [far]
    sources = [stack_peer((offset % planes, core))[0] for offset in arrivals for core in range(cores)]
    early = (2 * far - 3) * cores
    barrier = pltpu.get_barrier_semaphore()
    for _, _, peer, steps in groups:
        for step in steps:
            pl.semaphore_signal(barrier, inc=1, device_id=peer(step)[1], device_id_type=MESH)

    quarters = [pl.ds(k * tiles * LANES // 4, tiles * LANES // 4) for k in range(4)]
    first_half = pl.ds(0, tiles * LANES // 2)
    second_half = pl.ds(tiles * LANES // 2, tiles * LANES // 2)
    loads = [
        pltpu.make_async_copy(src, dst, load_sem.at[k])
        for k, (src, dst) in enumerate(
            (
                (w_hbm, w),
                (res_hbm.at[:, first_half], res.at[:, first_half]),
                (res_hbm.at[:, second_half], res.at[:, second_half]),
                (batch_atom_hbm, batch_atom),
                (owner_slot_hbm, owner_slot),
                *((basis_hbm.at[:, part], basis.at[:, part]) for part in quarters),
                (slot_index_hbm, slot_index),
                (rho_hbm, rho),
                (target_hbm, target),
                (coupling_hbm, coupling),
            )
        )
    ]
    for load in loads:
        load.start()

    lane = lax.broadcasted_iota(jnp.int32, (SUBS, LANES), 1)
    sub = lax.broadcasted_iota(jnp.int32, (SUBS, LANES), 0)
    quarter = lane // 32
    lane_row = lax.broadcasted_iota(jnp.int32, (1, LANES), 1)
    low_row = lane_row < half
    low = lax.broadcasted_iota(jnp.int32, (2 * SUBS, LANES), 1) < half
    low_wide = lax.broadcasted_iota(jnp.int32, (32, LANES), 1) < half

    def lane_tile(t):
        return pl.ds(pl.multiple_of(t * LANES, LANES), LANES)

    kinds = []
    sends = []

    def channel():
        kinds.append(len(kinds))
        return kinds[-1]

    def copy_to(src, dst, which, device, arrival=None):
        return pltpu.make_async_remote_copy(
            src_ref=src,
            dst_ref=dst,
            send_sem=send_sem.at[which],
            recv_sem=recv_sem.at[which] if arrival is None else arrival,
            device_id=device,
            device_id_type=MESH,
        )

    def drained(src, which):
        sends.append((src, send_sem.at[which]))

    def waiter(src, dst, which, count):
        drained(src.at[pl.ds(0, count)], which)

        def wait():
            arrived = dst.at[pl.ds(0, count)]
            pltpu.make_async_copy(arrived, arrived, recv_sem.at[which]).wait()

        return wait

    def exchange(buf, group):
        count, mine, peer, steps = group
        which = channel()
        for step in steps:
            copy_to(buf.at[mine], buf.at[mine], which, peer(step)[1]).start()
        return waiter(buf, buf, which, count - 1)

    def scatter(src, dst, group):
        count, mine, peer, steps = group
        which = channel()

        def send(step):
            at, device = peer(step)
            copy_to(src.at[at], dst.at[mine], which, device).start()

        return send, waiter(src, dst, which, count - 1)

    def tree(parts):
        parts = list(parts)
        while len(parts) > 1:
            parts = [parts[k] + parts[k + 1] if k + 1 < len(parts) else parts[k] for k in range(0, len(parts), 2)]
        return parts[0]

    def total(buf, count):
        return tree(buf[k] for k in range(count))

    def splat(row, k):
        return jnp.broadcast_to(row[:, k : k + 1], (1, LANES))

    def weigh():
        @pl.loop(0, rows // 4)
        def _(step):
            for u in range(4):
                r = step * 4 + u
                xs, ys = [], []
                for q in range(4):
                    b = q * rows + r
                    at = pl.ds(pl.multiple_of(b * width, width), width)
                    xs.extend(split(res[:, at] * batch_row(w, b)))
                    end = jnp.broadcast_to(basis[24:25, at], (SUBS, width))
                    ys.append(jnp.concatenate([basis[0:24, at], end], axis=0))
                x = jnp.concatenate(xs, axis=0).astype(jnp.bfloat16)
                out = None
                for k, y in enumerate(split(jnp.concatenate(ys, axis=0), 2)):
                    y = y.astype(jnp.bfloat16)
                    basis_pieces[k, pl.ds(pl.multiple_of(r * LANES, LANES), LANES)] = y
                    part = lax.dot_general(x, y, (((1,), (1,)), ((), ())), preferred_element_type=F32)
                    out = part if out is None else out + part
                tile = jnp.zeros((SUBS, LANES), F32)
                for q in range(4):
                    block = out[24 * q : 24 * q + 8] + out[24 * q + 8 : 24 * q + 16] + out[24 * q + 16 : 24 * q + 24]
                    tile = jnp.where(quarter == q, block, tile)
                hist_moments[pl.ds(r, hist_len, stride=rows), :] = tile

    def weigh_fresh():
        x = jnp.concatenate([fresh_w[pl.ds(v, batches, stride=per_batch), :] for v in range(per_batch)], axis=1)
        x = jnp.concatenate(split(x), axis=0).astype(jnp.bfloat16)
        out = None
        for k in range(2):
            part = lax.dot_general(x, basis_pieces[k], (((1,), (1,)), ((), ())), preferred_element_type=F32)
            out = part if out is None else out + part
        made = []
        for first in range(0, rows, SUBS):
            block = jnp.zeros((SUBS, LANES), F32)
            for u in range(SUBS):
                tile = slice((first + u) * LANES, (first + u + 1) * LANES)
                for q in range(4):
                    at = [k * batches + q * rows + first for k in range(3)]
                    piece = tree(out[begin : begin + SUBS, tile] for begin in at)
                    block = jnp.where((sub == u) & (quarter == q), piece, block)
            made.append(block)
        return jnp.concatenate(made, axis=0)

    def batch_row(ref, b):
        return jnp.concatenate([ref[pl.ds(b * per_batch + v, 1), :] for v in range(per_batch)], axis=1)

    def turn(block, by):
        return pltpu.roll(block, by % LANES, 1) if by % LANES else block

    def unfold(one, two):
        upper = jnp.where(low, one, pltpu.roll(two, half, 1))
        lower = jnp.where(low, pltpu.roll(one, half, 1), two)
        return jnp.concatenate([upper, lower], axis=0)

    def in_pieces(blocks):
        everywhere = jnp.concatenate(blocks, axis=1)
        return jnp.concatenate(split(everywhere), axis=0).astype(jnp.bfloat16)

    def gathered(pieces, first, count):
        return jnp.dot(pieces, mask[:, pl.ds(pl.multiple_of(first, count), count)], preferred_element_type=F32)

    def joined(out):
        return out[0:32] + out[32:64] + out[64:96]

    many = 2 * LANES // share
    each = LANES // share

    def kept(out, k):
        tile = out[:, k // each * LANES : (k // each + 1) * LANES]
        result = jnp.zeros((SUBS, LANES), F32)
        for g in range(4):
            piece = tile[g * SUBS : (g + 1) * SUBS]
            result = jnp.where(quarter == g, turn(piece, (g - k % each) * 32), result)
        return result

    shifts = hist_len // 2 + 1
    entry = None
    for iteration in range(iters):
        stack_row = stack_rows.at[iteration]
        sheet_row = sheet_rows.at[iteration]
        sent = part_send.at[iteration]
        received = part_recv.at[iteration]
        last = iteration == iters - 1

        if iteration == 0:
            loads[0].wait()
            loads[1].wait()

            def gram(step, acc):
                acc = list(acc)
                for u in range(8):
                    t = step * 8 + u
                    x = res[:, lane_tile(t)]
                    y = x * w[pl.ds(t, 1), :]
                    for r in range(shifts):
                        acc[r] = acc[r] + y * (pltpu.roll(x, r, 0) if r else x)
                return tuple(acc)

            acc = tuple(jnp.zeros((SUBS, LANES), F32) for _ in range(shifts))
            acc = lax.fori_loop(0, tiles // 16, gram, acc)
            loads[2].wait()
            acc = lax.fori_loop(tiles // 16, tiles // 8, gram, acc)
            loads[3].wait()
            loads[4].wait()
            id_row = jnp.zeros((1, LANES), F32)
            for b in range(batches):
                id_row = jnp.where(lane_row == half + b, owner_slot[batch_atom[b]].astype(F32), id_row)
            id_rows[pl.ds(in_sheet, 1)] = id_row[None]
            packed = jnp.zeros((SUBS, LANES), F32)
            for r in range(shifts):
                packed = jnp.where(lane == hist_len * r + sub, jnp.sum(acc[r], axis=1, keepdims=True), packed)
            stack_row[pl.ds(in_stack, 1)] = (jnp.sum(packed, axis=0, keepdims=True) + id_row)[None]
            for load in loads[5:9]:
                load.wait()
            weigh()
            mine = hist_all.at[in_stack]
            for pair in range(hist_len // 2):
                turned = jnp.concatenate(
                    [
                        turn(hist_moments[(2 * pair + h) * rows : (2 * pair + h + 1) * rows], -32 * q)
                        for h in range(2)
                        for q in range(4)
                    ],
                    axis=0,
                )
                mine[pair] = jnp.transpose(turned)[0:harmonics]
            pl.semaphore_wait(barrier, sum(group[0] - 1 for group in groups))
        else:
            slot = slot_index[iteration - 1]
            slot_row = jnp.zeros((1, LANES), jnp.int32) + slot

            def refresh(step, acc):
                acc, own = acc
                for u in range(8):
                    t = step * 8 + u
                    acc = acc + fresh_w[pl.ds(t, 1), :] * res[:, lane_tile(t)]
                rows_at = pl.ds(pl.multiple_of(step * 8, 8), 8)
                return acc, own + fresh_w[rows_at, :] * fresh[rows_at, :]

            zero = jnp.zeros((SUBS, LANES), F32)
            acc, own = lax.fori_loop(0, tiles // 8, refresh, (zero, zero))
            acc = jnp.where(sub == slot, jnp.sum(own, axis=0, keepdims=True), acc)
            packed = jnp.where(lane == sub, jnp.sum(acc, axis=1, keepdims=True), 0.0)
            stack_row[pl.ds(in_stack, 1)] = jnp.sum(packed, axis=0, keepdims=True)[None]
        wait = exchange(stack_row, stack_group)
        if iteration == 0:
            wait_ids = exchange(id_rows, sheet_group)

        if iteration == 0:
            passed, passed_late, across = channel(), channel(), channel()
            sibling = stack_peer((0, 1))[1]

            def block_of(step):
                return hist_all.at[stack_peer((-step % planes, 0))[0]]

            def move(block, step, arrival):
                copy_to(block, block, across, stack_peer((step % planes, 0))[1], pass_sem.at[arrival]).start()

            def landed(block, arrival):
                pltpu.make_async_copy(block, block, pass_sem.at[arrival]).wait()

            def relay(k):
                for sign in (1, -1):
                    block = block_of(sign * hops).at[parts[k]]
                    landed(block, sign * hops % planes if k else planes + (sign < 0))
                    if (sign < 0) == bool(k):
                        move(block, sign * hops, far)
                    move(block, sign * (far - 1 - hops), sign * (far - 1) % planes)
                    pass_on(block)

            def pass_on(block, late=False):
                copy_to(block, block, passed_late if late else passed, sibling).start()

            parts = [pl.ds(k * hist_len // 4, hist_len // 4) for k in range(2)]
            hops = far // 2
            for k in range(2):
                for sign in (1, -1):
                    move(mine.at[parts[k]], sign * hops, sign * hops % planes if k else planes + (sign < 0))
            for sign in (1, -1):
                move(mine, sign, sign % planes)
            pass_on(mine)
            drained(hist_all.at[pl.ds(0, planes - 1)], across)
            wait_passed = waiter(hist_all, hist_all, passed, early // cores)
            wait_late = waiter(hist_all, hist_all, passed_late, planes - early // cores)
        else:
            fresh_rows = weigh_fresh()
            turned = jnp.concatenate([turn(fresh_rows, -32 * q - 16 * h) for h in range(2) for q in range(4)], axis=0)
            new_moment = fresh_all.at[iteration - 1]
            new_moment[pl.ds(in_stack, 1)] = jnp.transpose(turned)[0 : 2 * SUBS][None]
            wait_fresh = exchange(new_moment, stack_group)

        if iteration == 0:
            relay(0)
        wait()
        sheet_row[pl.ds(in_sheet, 1)] = total(stack_row, stack)[None]
        wait = exchange(sheet_row, sheet_group)

        if iteration == 0:
            relay(1)

            for cols, order in ((source_cols, range(stack)), (near_cols, sources)):
                ids = jnp.transpose(jnp.concatenate([stack_row[k] for k in order] * (LANES // stack), axis=0))
                for k in range(stack):
                    cols[k * batches : (k + 1) * batches] = jnp.broadcast_to(
                        ids[half : half + batches, k : k + 1], (batches, LANES)
                    )
            wait_ids()

            def fill(cols, lanes, wanted):
                for k in range(mask.shape[0] // (2 * SUBS)):
                    at = slice(2 * SUBS * k, 2 * SUBS * (k + 1))
                    mask[at, lanes] = jnp.where(cols[at] == wanted, 1.0, 0.0).astype(jnp.bfloat16)

            @pl.loop(0, near_lanes // LANES)
            def _(t):
                pair = jnp.where(low_row, pltpu.roll(id_rows[2 * t], half, 1), id_rows[2 * t + 1])
                fill(near_cols, lane_tile(t), pair)

            @pl.loop(0, sheet * share // LANES)
            def _(t):
                at = t * (LANES // share) + lane_row // share
                member = (at % spans) * cores + my_core
                held = member * owned + ((at // spans) * depth + lax.rem(my_plane, depth)) * share
                fill(source_cols, lane_tile(t + near_lanes // LANES), (held + lane_row % share).astype(F32))

            for load in loads[9:]:
                load.wait()

        if iteration:
            wait_fresh()
            fresh_blocks = [unfold(new_moment[k], new_moment[k + 1]) for k in range(0, stack, 2)]
            pieces = in_pieces(fresh_blocks)
            send, wait_own = scatter(own_send, own_recv, sheet_group)
            out = joined(gathered(pieces, near_lanes, sheet * share))
            for k in range(sheet):
                own_send[k] = kept(out, k)
            own_recv[pl.ds(in_sheet, 1)] = own_send[pl.ds(in_sheet, 1)]
            for step in sheet_group[3]:
                send(step)
            wait_old()
            held_old = [tree(old_recv[k, i] for k in range(sheet)) for i in range(hist_len)]

        if iteration == 0:
            for step in (1, planes - 1, far - 1, planes - far + 1, far):
                block = block_of(step)
                landed(block, step)
                pass_on(block, step not in (1, planes - 1))
        wait()
        row = total(sheet_row, sheet)
        if iteration == 0:
            entry = [[None] * (i + 1) for i in range(hist_len)]
            for i in range(hist_len):
                for j in range(i + 1):
                    r = i - j
                    at = hist_len * r + i if r < shifts else hist_len * (hist_len - r) + j
                    entry[i][j] = splat(row, at)
        else:
            news = [splat(row, k) for k in range(hist_len)]
            entry = [
                [
                    jnp.where(slot_row == i, news[j], jnp.where(slot_row == j, news[i], entry[i][j]))
                    for j in range(i + 1)
                ]
                for i in range(hist_len)
            ]
        coeffs = solve_coeffs(entry, hist_len)

        if iteration == 0:
            wait_passed()
            old = coeffs
        else:
            old = [jnp.where(slot_row == i, 0.0, coeffs[i]) for i in range(hist_len)]
            new = coeffs[0]
            for i in range(1, hist_len):
                new = jnp.where(slot_row == i, coeffs[i], new)

        coeff_col = jnp.zeros((SUBS, LANES), F32)
        for i in range(hist_len):
            coeff_col = jnp.where(sub == i, old[i], coeff_col)

        gains = [jnp.where(low_row, old[2 * pair], old[2 * pair + 1]) for pair in range(hist_len // 2)]

        def mixed(at):
            top = tree(gains[pair] * hist_all[at, pair, 0:24] for pair in range(hist_len // 2))
            end = tree(gains[pair] * hist_all[at, pair, 24:25] for pair in range(hist_len // 2))
            return jnp.concatenate([top, jnp.broadcast_to(end, (SUBS, LANES))], axis=0)

        def near_pieces(order):
            blocks = []
            for k in range(0, len(order), 2):
                one, two = mixed(order[k]), mixed(order[k + 1])
                block = jnp.where(low_wide, one, two) + pltpu.roll(jnp.where(low_wide, two, one), half, 1)
                if iteration:
                    block = block + new * unfold(new_moment[order[k]], new_moment[order[k + 1]])
                blocks.append(block)
            return in_pieces(blocks)

        split_at = 0 if iteration else early
        if split_at:
            early_sum[...] = jnp.dot(
                near_pieces(sources[:split_at]),
                mask[0 : split_at * batches, 0:near_lanes],
                preferred_element_type=F32,
            )
            wait_late()
        out = jnp.dot(
            near_pieces(sources[split_at:]),
            mask[split_at * batches :, 0:near_lanes],
            preferred_element_type=F32,
        )
        near_sum[...] = joined(out + early_sum[...] if split_at else out)

        send, wait = scatter(sent, received, sheet_group)
        for line_step in sorted(range(lines), key=lambda step: -ring(step, lines)):
            first = lax.rem(my_line + line_step, lines) * spans
            lanes = pl.ds(pl.multiple_of(first * batches, spans * batches), spans * batches)
            out = near_sum[:, lanes]
            for k in range(0, spans, 2):
                upper = out[0:16, k * batches : (k + 2) * batches]
                lower = out[16:32, k * batches : (k + 2) * batches]
                sent[first + k] = jnp.where(low, upper, pltpu.roll(lower, half, 1))
                sent[first + k + 1] = jnp.where(low, pltpu.roll(upper, half, 1), lower)
            for step in sheet_group[3]:
                if step[0] == line_step:
                    send(step)
        received[pl.ds(in_sheet, 1)] = sent[pl.ds(in_sheet, 1)]

        def base_step(step, carry):
            for u in range(8):
                t = step * 8 + u
                part = coeff_col * (rho[:, lane_tile(t)] + mixing_beta * res[:, lane_tile(t)])
                base_rows[pl.ds(t, 1), :] = jnp.sum(part, axis=0, keepdims=True)
            return carry

        lax.fori_loop(0, tiles // 8, base_step, 0)

        if iteration == 0:
            @pl.loop(0, hist_len // 2)
            def _(pair):
                ones = [hist_all[k, pair, 0:24] for k in range(stack)]
                ends = [jnp.broadcast_to(hist_all[k, pair, 24:25], (SUBS, LANES)) for k in range(stack)]
                rows_of = [jnp.concatenate([ones[k], ends[k]], axis=0) for k in range(stack)]
                firsts, seconds = [], []
                for k in range(0, stack, 2):
                    one, two = rows_of[k], rows_of[k + 1]
                    firsts.append(jnp.where(low_wide, one, pltpu.roll(two, half, 1)))
                    seconds.append(jnp.where(low_wide, pltpu.roll(one, half, 1), two))
                old_pieces[pl.ds(pl.multiple_of(pair * 192, 192), 96)] = in_pieces(firsts)
                old_pieces[pl.ds(pl.multiple_of(pair * 192 + 96, 96), 96)] = in_pieces(seconds)

            send, wait_old = scatter(old_send, old_recv, sheet_group)
            for first in range(0, sheet, many):
                out = gathered(old_pieces[...], near_lanes + first * share, many * share)
                for i in range(hist_len):
                    part = joined(out[i * 96 : (i + 1) * 96])
                    for k in range(many):
                        old_send[first + k, i] = kept(part, k)
            old_recv[pl.ds(in_sheet, 1)] = old_send[pl.ds(in_sheet, 1)]
            for step in sheet_group[3]:
                send(step)

        if last:
            wait_own()
            held = new * total(own_recv, sheet) + tree(old[i] * held_old[i] for i in range(hist_len))
            chunks[pl.ds(my_share, 1)] = (held * scale)[None]
            wait_chunks = exchange(chunks, share_group)

        wait()
        summed = total(received, sheet)
        at_batch = jnp.concatenate([summed, pltpu.roll(summed, half, 1)], axis=0) * scale
        comp = lax.broadcasted_iota(jnp.int32, (32, LANES), 0)
        degree = sum((comp >= (l + 1) * (l + 1)).astype(F32) for l in range(4))
        damped = jnp.where(comp < harmonics, at_batch * (mixing_beta / (1.0 + degree)), 0.0)

        def density_step(step, ahead):
            for u in range(16):
                b = step * 16 + u
                col = jnp.broadcast_to(ahead[:, u : u + 1], (32, LANES))
                for v in range(per_batch):
                    t = b * per_batch + v
                    part = col[24:32] * basis[24:25, lane_tile(t)]
                    for g in range(3):
                        part = part + col[g * SUBS : (g + 1) * SUBS] * basis[g * SUBS : (g + 1) * SUBS, lane_tile(t)]
                    correct[pl.ds(t, 1), :] = jnp.sum(part, axis=0, keepdims=True)
            return pltpu.roll(ahead, LANES - 16, 1)

        lax.fori_loop(0, batches // 16, density_step, damped)
        density = base_rows[...] - correct[...]
        if iteration:
            density = density + new * (density_out[...] + mixing_beta * fresh[...])
        density_out[...] = density
        if last:
            wait_chunks()
            for t in range(owned // LANES):
                held = [chunks[t * each + k] for k in range(each)]
                for g in range(4):
                    tile = jnp.zeros((SUBS, LANES), F32)
                    for k in range(each):
                        tile = jnp.where(quarter == k, turn(held[k], (k - g) * 32), tile)
                    top = min(SUBS, harmonics - g * SUBS)
                    moments_out[g * SUBS : g * SUBS + top, t * LANES : (t + 1) * LANES] = tile[0:top]
        else:
            made = target[...] + coupling[...] * jnp.tanh(density) - density
            fresh[...] = made
            fresh_w[...] = made * w[...]
    for src, sem in sends:
        pltpu.make_async_copy(src, src, sem).wait()


def finish(density, moments, density_out, moments_out):
    density_out[...] = density[...]
    moments_out[...] = moments[...]


def local(weights, target, coupling, multipole_basis, rho_hist, res_hist, batch_atom, owner_slot, slot_index):
    harmonics, points = multipole_basis.shape
    hist_len = res_hist.shape[0]
    batches = batch_atom.shape[0]
    groups = lax.axis_size("grid")
    members = lax.axis_size("atom")
    lines, cores = 4, 2
    planes = groups // lines
    spans = members // cores
    stack, sheet = planes * cores, lines * spans
    shares = 4 * lines
    owned = owner_slot.shape[0] // members
    scale = 1.0 / math.sqrt(points * groups // owned)
    iters = slot_index.shape[0]
    cfg = (iters, hist_len, harmonics, batches, points // batches, owned, planes, lines, spans, cores, scale)
    tiles = points // LANES
    flat = (tiles, LANES)
    kinds = 3 * iters + 7 + (iters - 1)
    any_space = pl.BlockSpec(memory_space=pltpu.HBM)
    vmem = pl.BlockSpec(memory_space=pltpu.VMEM)
    density, moments = pl.pallas_call(
        functools.partial(kernel, cfg),
        out_shape=(jax.ShapeDtypeStruct(flat, F32), jax.ShapeDtypeStruct((harmonics, owned), F32)),
        in_specs=[any_space] * 9,
        out_specs=(vmem, vmem),
        scratch_shapes=[
            pltpu.VMEM(flat, F32),
            pltpu.VMEM(flat, F32),
            pltpu.VMEM(flat, F32),
            pltpu.VMEM((harmonics, points), F32),
            pltpu.VMEM((hist_len, points), F32),
            pltpu.VMEM((hist_len, points), F32),
            pltpu.VMEM(flat, F32),
            pltpu.VMEM(flat, F32),
            pltpu.VMEM((iters, stack, 1, LANES), F32),
            pltpu.VMEM((iters, sheet, 1, LANES), F32),
            pltpu.VMEM((sheet, 1, LANES), F32),
            pltpu.VMEM((stack, hist_len // 2, harmonics, LANES), F32),
            pltpu.VMEM((iters - 1, stack, 2 * SUBS, LANES), F32),
            pltpu.VMEM((iters, sheet, 2 * SUBS, LANES), F32),
            pltpu.VMEM((iters, sheet, 2 * SUBS, LANES), F32),
            pltpu.VMEM((sheet, SUBS, LANES), F32),
            pltpu.VMEM((sheet, SUBS, LANES), F32),
            pltpu.VMEM((sheet, hist_len, SUBS, LANES), F32),
            pltpu.VMEM((sheet, hist_len, SUBS, LANES), F32),
            pltpu.VMEM((hist_len * 96, stack * batches), jnp.bfloat16),
            pltpu.VMEM((2, batches // 4 * LANES, points // batches), jnp.bfloat16),
            pltpu.VMEM((96, sheet * batches), F32),
            pltpu.VMEM((32, sheet * batches), F32),
            pltpu.VMEM((shares, SUBS, LANES), F32),
            pltpu.VMEM((stack * batches, LANES), F32),
            pltpu.VMEM((stack * batches, LANES), F32),
            pltpu.VMEM((stack * batches, sheet * (batches + owned // shares)), jnp.bfloat16),
            pltpu.VMEM((batches // 4 * hist_len, LANES), F32),
            pltpu.VMEM(flat, F32),
            pltpu.VMEM(flat, F32),
            pltpu.SMEM(batch_atom.shape, jnp.int32),
            pltpu.SMEM(owner_slot.shape, jnp.int32),
            pltpu.SMEM(slot_index.shape, jnp.int32),
            pltpu.SemaphoreType.DMA((13,)),
            pltpu.SemaphoreType.DMA((kinds,)),
            pltpu.SemaphoreType.DMA((kinds,)),
            pltpu.SemaphoreType.DMA((planes + 2,)),
        ],
        compiler_params=pltpu.CompilerParams(
            collective_id=0, has_side_effects=True, vmem_limit_bytes=16777216
        ),
    )(
        *(
            pltpu.with_memory_space_constraint(array, pltpu.HBM)
            for array in (
                batch_atom,
                owner_slot,
                slot_index,
                weights.reshape(flat),
                target.reshape(flat),
                coupling.reshape(flat),
                multipole_basis,
                rho_hist,
                res_hist,
            )
        )
    )
    density, moments = pl.pallas_call(
        finish,
        out_shape=(jax.ShapeDtypeStruct(flat, F32), jax.ShapeDtypeStruct((harmonics, owned), F32)),
        in_specs=[vmem] * 2,
        out_specs=(vmem, vmem),
        compiler_params=pltpu.CompilerParams(vmem_limit_bytes=1048576),
    )(density, moments)
    return density.reshape(points), moments


def solution(mesh):
    both = ("grid", "atom")
    placed = (P(both), P(both), P(both), P(None, both), P(None, both), P(None, both), P(both), P(), P())
    return jax.shard_map(
        local,
        mesh=mesh,
        in_specs=placed,
        out_specs=(P(both), P(None, "atom")),
        check_vma=False,
    )
```

```python
import functools
import math

import jax
import jax.numpy as jnp
from jax import lax
from jax.experimental import pallas as pl
from jax.experimental.pallas import tpu as pltpu
from jax.sharding import PartitionSpec as P

MESH = pl.DeviceIdType.MESH
LANES = 128
SUBS = 8
mixing_beta = 0.5
ridge_share = 0.1
F32 = jnp.float32


def solve_coeffs(entry, hist_len):
    trace = entry[0][0]
    for i in range(1, hist_len):
        trace = trace + entry[i][i]
    ridge = (ridge_share / hist_len) * trace
    low = [[entry[i][j] for j in range(i + 1)] for i in range(hist_len)]
    for i in range(hist_len):
        low[i][i] = low[i][i] + ridge
    inverse = [None] * hist_len
    factor = [[None] * hist_len for _ in range(hist_len)]
    forward = [jnp.ones_like(trace) for _ in range(hist_len)]
    for j in range(hist_len):
        inverse[j] = 1.0 / low[j][j]
        for i in range(j + 1, hist_len):
            factor[i][j] = low[i][j] * inverse[j]
        for i in range(j + 1, hist_len):
            forward[i] = forward[i] - factor[i][j] * forward[j]
            for k in range(j + 1, i + 1):
                low[i][k] = low[i][k] - factor[i][j] * low[k][j]
    backward = [forward[i] * inverse[i] for i in range(hist_len)]
    for j in reversed(range(hist_len)):
        for i in range(j):
            backward[i] = backward[i] - factor[j][i] * backward[j]
    total = backward[0]
    for i in range(1, hist_len):
        total = total + backward[i]
    return [backward[i] / total for i in range(hist_len)]


def split(x, count=3):
    pieces = []
    for _ in range(count):
        piece = x.astype(jnp.bfloat16).astype(F32)
        pieces.append(piece)
        x = x - piece
    return pieces


def kernel(
    cfg,
    batch_atom_hbm,
    owner_slot_hbm,
    slot_index_hbm,
    w_hbm,
    target_hbm,
    coupling_hbm,
    basis_hbm,
    rho_hbm,
    res_hbm,
    density_out,
    moments_out,
    w,
    target,
    coupling,
    basis,
    rho,
    res,
    fresh,
    fresh_w,
    stack_rows,
    sheet_rows,
    id_rows,
    hist_all,
    fresh_all,
    part_send,
    part_recv,
    own_send,
    own_recv,
    old_send,
    old_recv,
    old_pieces,
    basis_pieces,
    early_sum,
    near_sum,
    chunks,
    source_cols,
    near_cols,
    mask,
    hist_moments,
    base_rows,
    correct,
    batch_atom,
    owner_slot,
    slot_index,
    load_sem,
    basis_sem,
    send_sem,
    recv_sem,
    pass_sem,
):
    iters, hist_len, harmonics, batches, width, owned, planes, lines, spans, cores, scale = cfg
    tiles = w.shape[0]
    per_batch = width // LANES
    half = LANES // 2
    rows = batches // 4
    stack = planes * cores
    sheet = lines * spans
    near_lanes = sheet * batches
    shares = chunks.shape[0]
    depth = shares // lines
    share = owned // shares
    my_group = lax.axis_index("grid")
    my_member = lax.axis_index("atom")
    my_plane = lax.div(my_group, lines)
    my_line = lax.rem(my_group, lines)
    my_span = lax.div(my_member, cores)
    my_core = lax.rem(my_member, cores)
    in_stack = my_plane * cores + my_core
    in_sheet = my_line * spans + my_span
    my_share = my_line * depth + lax.rem(my_plane, depth)

    def ring(step, count):
        return min(step, count - step)

    def stack_peer(step):
        plane, core = lax.rem(my_plane + step[0], planes), lax.rem(my_core + step[1], cores)
        return plane * cores + core, (plane * lines + my_line, my_span * cores + core)

    def sheet_peer(step):
        line, span = lax.rem(my_line + step[0], lines), lax.rem(my_span + step[1], spans)
        return line * spans + span, (my_plane * lines + line, span * cores + my_core)

    def share_peer(step):
        line, plane = lax.rem(my_line + step[0], lines), lax.rem(my_plane + step[1], depth)
        device = (lax.div(my_plane, depth) * depth + plane) * lines + line, my_member
        return line * depth + plane, device

    def far_first(across, along):
        steps = [(a, b) for a in range(across) for b in range(along) if a or b]
        return sorted(steps, key=lambda step: -ring(step[0], across) - ring(step[1], along))

    stack_group = (stack, in_stack, stack_peer, far_first(planes, cores))
    sheet_group = (sheet, in_sheet, sheet_peer, far_first(lines, spans))
    share_group = (shares, my_share, share_peer, far_first(lines, depth))
    groups = (stack_group, sheet_group)
    far = planes // 2
    arrivals = [0, 1, -1] + [sign * hop for hop in range(2, far) for sign in (1, -1)] + [far]
    sources = [stack_peer((offset % planes, core))[0] for offset in arrivals for core in range(cores)]
    early = (2 * far - 3) * cores
    barrier = pltpu.get_barrier_semaphore()
    for _, _, peer, steps in groups:
        for step in steps:
            pl.semaphore_signal(barrier, inc=1, device_id=peer(step)[1], device_id_type=MESH)

    first_half = pl.ds(0, tiles * LANES // 2)
    second_half = pl.ds(tiles * LANES // 2, tiles * LANES // 2)
    loads = [
        pltpu.make_async_copy(src, dst, load_sem.at[k])
        for k, (src, dst) in enumerate(
            (
                (w_hbm, w),
                (res_hbm.at[:, first_half], res.at[:, first_half]),
                (res_hbm.at[:, second_half], res.at[:, second_half]),
                (batch_atom_hbm, batch_atom),
                (owner_slot_hbm, owner_slot),
                (slot_index_hbm, slot_index),
                (rho_hbm, rho),
                (target_hbm, target),
                (coupling_hbm, coupling),
            )
        )
    ]
    basis_parts = [pl.ds(k * tiles * LANES // 4, tiles * LANES // 4) for k in range(4)]
    for load in loads[:5]:
        load.start()
    for part in basis_parts:
        pltpu.make_async_copy(basis_hbm.at[:, part], basis.at[:, part], basis_sem).start()

    lane = lax.broadcasted_iota(jnp.int32, (SUBS, LANES), 1)
    sub = lax.broadcasted_iota(jnp.int32, (SUBS, LANES), 0)
    quarter = lane // 32
    lane_row = lax.broadcasted_iota(jnp.int32, (1, LANES), 1)
    low_row = lane_row < half
    low = lax.broadcasted_iota(jnp.int32, (2 * SUBS, LANES), 1) < half
    low_wide = lax.broadcasted_iota(jnp.int32, (32, LANES), 1) < half

    def lane_tile(t):
        return pl.ds(pl.multiple_of(t * LANES, LANES), LANES)

    kinds = []
    sends = []

    def channel():
        kinds.append(len(kinds))
        return kinds[-1]

    def copy_to(src, dst, which, device, arrival=None):
        return pltpu.make_async_remote_copy(
            src_ref=src,
            dst_ref=dst,
            send_sem=send_sem.at[which],
            recv_sem=recv_sem.at[which] if arrival is None else arrival,
            device_id=device,
            device_id_type=MESH,
        )

    def drained(src, which):
        sends.append((src, send_sem.at[which]))

    def waiter(src, dst, which, count):
        drained(src.at[pl.ds(0, count)], which)

        def wait():
            arrived = dst.at[pl.ds(0, count)]
            pltpu.make_async_copy(arrived, arrived, recv_sem.at[which]).wait()

        return wait

    def exchange(buf, group):
        count, mine, peer, steps = group
        which = channel()
        for step in steps:
            copy_to(buf.at[mine], buf.at[mine], which, peer(step)[1]).start()
        return waiter(buf, buf, which, count - 1)

    def scatter(src, dst, group):
        count, mine, peer, steps = group
        which = channel()

        def send(step):
            at, device = peer(step)
            copy_to(src.at[at], dst.at[mine], which, device).start()

        return send, waiter(src, dst, which, count - 1)

    def tree(parts):
        parts = list(parts)
        while len(parts) > 1:
            parts = [parts[k] + parts[k + 1] if k + 1 < len(parts) else parts[k] for k in range(0, len(parts), 2)]
        return parts[0]

    def column_sums(parts):
        parts, gap = list(parts), SUBS // 2
        while gap:
            keep = sub % (2 * gap) < gap
            merged = []
            for one, two in zip(parts[:gap], parts[gap:]):
                if 2 * gap == SUBS:
                    merged.append(jnp.where(keep, one, two) + pltpu.roll(jnp.where(keep, two, one), gap, 0))
                else:
                    up, down = pltpu.roll(one, SUBS - gap, 0), pltpu.roll(two, gap, 0)
                    merged.append(jnp.where(keep, one, down) + jnp.where(keep, up, two))
            parts, gap = merged, gap // 2
        return parts[0]

    def total(buf, count):
        return tree(buf[k] for k in range(count))

    def splat(row, k):
        return jnp.broadcast_to(row[:, k : k + 1], (1, LANES))

    def weigh():
        @pl.loop(0, rows // 4)
        def _(step):
            for u in range(4):
                r = step * 4 + u
                xs, ys = [], []
                for q in range(4):
                    b = q * rows + r
                    at = pl.ds(pl.multiple_of(b * width, width), width)
                    xs.extend(split(res[:, at] * batch_row(w, b)))
                    end = jnp.broadcast_to(basis[24:25, at], (SUBS, width))
                    ys.append(jnp.concatenate([basis[0:24, at], end], axis=0))
                x = jnp.concatenate(xs, axis=0).astype(jnp.bfloat16)
                out = None
                for k, y in enumerate(split(jnp.concatenate(ys, axis=0), 2)):
                    y = y.astype(jnp.bfloat16)
                    basis_pieces[k, pl.ds(pl.multiple_of(r * LANES, LANES), LANES)] = y
                    part = lax.dot_general(x, y, (((1,), (1,)), ((), ())), preferred_element_type=F32)
                    out = part if out is None else out + part
                tile = jnp.zeros((SUBS, LANES), F32)
                for q in range(4):
                    block = out[24 * q : 24 * q + 8] + out[24 * q + 8 : 24 * q + 16] + out[24 * q + 16 : 24 * q + 24]
                    tile = jnp.where(quarter == q, block, tile)
                hist_moments[pl.ds(r, hist_len, stride=rows), :] = tile

    def weigh_fresh():
        x = jnp.concatenate([fresh_w[pl.ds(v, batches, stride=per_batch), :] for v in range(per_batch)], axis=1)
        x = jnp.concatenate(split(x), axis=0).astype(jnp.bfloat16)
        out = None
        for k in range(2):
            part = lax.dot_general(x, basis_pieces[k], (((1,), (1,)), ((), ())), preferred_element_type=F32)
            out = part if out is None else out + part
        made = []
        for first in range(0, rows, SUBS):
            block = jnp.zeros((SUBS, LANES), F32)
            for u in range(SUBS):
                tile = slice((first + u) * LANES, (first + u + 1) * LANES)
                for q in range(4):
                    at = [k * batches + q * rows + first for k in range(3)]
                    piece = tree(out[begin : begin + SUBS, tile] for begin in at)
                    block = jnp.where((sub == u) & (quarter == q), piece, block)
            made.append(block)
        return jnp.concatenate(made, axis=0)

    def batch_row(ref, b):
        return jnp.concatenate([ref[pl.ds(b * per_batch + v, 1), :] for v in range(per_batch)], axis=1)

    def turn(block, by):
        return pltpu.roll(block, by % LANES, 1) if by % LANES else block

    def unfold(one, two):
        low_here = low[0 : one.shape[0]]
        left = jnp.where(low_here, one, pltpu.roll(two, half, 1))
        right = jnp.where(low_here, pltpu.roll(one, half, 1), two)
        end = jnp.broadcast_to(right[12:13], (SUBS, LANES))
        return jnp.concatenate([left[0:8], right[0:8], left[8:12], right[8:12], end], axis=0)

    def fold(block):
        left = jnp.concatenate([block[0:8], block[16:21]], axis=0)
        right = jnp.concatenate([block[8:16], block[20:25]], axis=0)
        low_here = low[0 : left.shape[0]]
        return (
            jnp.where(low_here, left, pltpu.roll(right, half, 1)),
            jnp.where(low_here, pltpu.roll(left, half, 1), right),
        )

    def in_pieces(blocks):
        everywhere = jnp.concatenate(blocks, axis=1)
        return jnp.concatenate(split(everywhere), axis=0).astype(jnp.bfloat16)

    def gathered(pieces, first, count):
        return jnp.dot(pieces, mask[:, pl.ds(pl.multiple_of(first, count), count)], preferred_element_type=F32)

    def joined(out):
        return out[0:32] + out[32:64] + out[64:96]

    many = 2 * LANES // share
    each = LANES // share

    def kept(out, k):
        tile = out[:, k // each * LANES : (k // each + 1) * LANES]
        result = jnp.zeros((SUBS, LANES), F32)
        for g in range(4):
            piece = tile[g * SUBS : (g + 1) * SUBS]
            result = jnp.where(quarter == g, turn(piece, (g - k % each) * 32), result)
        return result

    shifts = hist_len // 2 + 1
    entry = None
    for iteration in range(iters):
        stack_row = stack_rows.at[iteration]
        sheet_row = sheet_rows.at[iteration]
        sent = part_send.at[iteration]
        received = part_recv.at[iteration]
        last = iteration == iters - 1

        if iteration == 0:
            loads[0].wait()
            loads[1].wait()

            def gram(step, acc):
                acc = list(acc)
                for u in range(8):
                    t = step * 8 + u
                    x = res[:, lane_tile(t)]
                    y = x * w[pl.ds(t, 1), :]
                    for r in range(shifts):
                        acc[r] = acc[r] + y * (pltpu.roll(x, r, 0) if r else x)
                return tuple(acc)

            acc = tuple(jnp.zeros((SUBS, LANES), F32) for _ in range(shifts))
            acc = lax.fori_loop(0, tiles // 16, gram, acc)
            loads[2].wait()
            acc = lax.fori_loop(tiles // 16, tiles // 8, gram, acc)
            loads[3].wait()
            loads[4].wait()
            id_row = jnp.zeros((1, LANES), F32)
            for b in range(batches):
                id_row = jnp.where(lane_row == half + b, owner_slot[batch_atom[b]].astype(F32), id_row)
            id_rows[pl.ds(in_sheet, 1)] = id_row[None]
            packed = jnp.zeros((SUBS, LANES), F32)
            for r in range(shifts):
                packed = jnp.where(lane == hist_len * r + sub, jnp.sum(acc[r], axis=1, keepdims=True), packed)
            stack_row[pl.ds(in_stack, 1)] = (jnp.sum(packed, axis=0, keepdims=True) + id_row)[None]
            pltpu.make_async_copy(basis_hbm, basis, basis_sem).wait()
            weigh()
            for load in loads[5:]:
                load.start()
            mine = hist_all.at[in_stack]
            for pair in range(hist_len // 2):
                turned = jnp.concatenate(
                    [
                        turn(hist_moments[(2 * pair + h) * rows : (2 * pair + h + 1) * rows], -32 * q)
                        for h in range(2)
                        for q in range(4)
                    ],
                    axis=0,
                )
                mine[pair] = jnp.transpose(turned)[0:harmonics]
            pl.semaphore_wait(barrier, sum(group[0] - 1 for group in groups))
        else:
            slot = slot_index[iteration - 1]
            slot_row = jnp.zeros((1, LANES), jnp.int32) + slot

            def refresh(step, acc):
                acc, own = acc
                sums = [acc] + [jnp.zeros((SUBS, LANES), F32) for _ in range(3)]
                for u in range(32):
                    t = step * 32 + u
                    sums[u % 4] = sums[u % 4] + fresh_w[pl.ds(t, 1), :] * res[:, lane_tile(t)]
                for u in range(0, 32, SUBS):
                    at = pl.ds(pl.multiple_of(step * 32 + u, SUBS), SUBS)
                    own = own + fresh_w[at, :] * fresh[at, :]
                return tree(sums), own

            zero = jnp.zeros((SUBS, LANES), F32)
            acc, own = lax.fori_loop(0, tiles // 32, refresh, (zero, zero))
            acc = jnp.where(sub == slot, jnp.sum(own, axis=0, keepdims=True), acc)
            packed = jnp.where(lane == sub, jnp.sum(acc, axis=1, keepdims=True), 0.0)
            stack_row[pl.ds(in_stack, 1)] = jnp.sum(packed, axis=0, keepdims=True)[None]
        wait = exchange(stack_row, stack_group)
        if iteration == 0:
            wait_ids = exchange(id_rows, sheet_group)

        if iteration == 0:
            passed, passed_late, across = channel(), channel(), channel()
            sibling = stack_peer((0, 1))[1]

            def block_of(step):
                return hist_all.at[stack_peer((-step % planes, 0))[0]]

            def move(block, step, arrival):
                copy_to(block, block, across, stack_peer((step % planes, 0))[1], pass_sem.at[arrival]).start()

            def landed(block, arrival):
                pltpu.make_async_copy(block, block, pass_sem.at[arrival]).wait()

            def relay(k):
                for sign in (1, -1):
                    block = block_of(sign * hops).at[parts[k]]
                    landed(block, sign * hops % planes if k else planes + (sign < 0))
                    if (sign < 0) == bool(k):
                        move(block, sign * hops, far)
                    move(block, sign * (far - 1 - hops), sign * (far - 1) % planes)
                    pass_on(block)

            def pass_on(block, late=False):
                copy_to(block, block, passed_late if late else passed, sibling).start()

            parts = [pl.ds(k * hist_len // 4, hist_len // 4) for k in range(2)]
            hops = far // 2
            for k in range(2):
                for sign in (1, -1):
                    move(mine.at[parts[k]], sign * hops, sign * hops % planes if k else planes + (sign < 0))
            for sign in (1, -1):
                move(mine, sign, sign % planes)
            pass_on(mine)
            drained(hist_all.at[pl.ds(0, planes - 1)], across)
            wait_passed = waiter(hist_all, hist_all, passed, early // cores)
            wait_late = waiter(hist_all, hist_all, passed_late, planes - early // cores)
        else:
            fresh_rows = weigh_fresh()
            first_lanes = lax.broadcasted_iota(jnp.int32, (rows, LANES), 1) < SUBS
            turned = [
                jnp.where(first_lanes, turn(fresh_rows, -32 * q - 8 * h), turn(fresh_rows, -32 * q - 8 - 4 * h))
                for h in range(2)
                for q in range(4)
            ]
            new_moment = fresh_all.at[iteration - 1]
            new_moment[pl.ds(in_stack, 1)] = jnp.transpose(jnp.concatenate(turned, axis=0))[0:13][None]
            wait_fresh = exchange(new_moment, stack_group)

        if iteration == 0:
            relay(0)
        wait()
        sheet_row[pl.ds(in_sheet, 1)] = total(stack_row, stack)[None]
        wait = exchange(sheet_row, sheet_group)

        if iteration == 0:
            relay(1)

            for cols, order in ((source_cols, range(stack)), (near_cols, sources)):
                ids = jnp.transpose(jnp.concatenate([stack_row[k] for k in order] * (LANES // stack), axis=0))
                for k in range(stack):
                    cols[k * batches : (k + 1) * batches] = jnp.broadcast_to(
                        ids[half : half + batches, k : k + 1], (batches, LANES)
                    )
            wait_ids()

            def fill(cols, lanes, wanted):
                for k in range(mask.shape[0] // (2 * SUBS)):
                    at = slice(2 * SUBS * k, 2 * SUBS * (k + 1))
                    mask[at, lanes] = jnp.where(cols[at] == wanted, 1.0, 0.0).astype(jnp.bfloat16)

            @pl.loop(0, near_lanes // LANES)
            def _(t):
                pair = jnp.where(low_row, pltpu.roll(id_rows[2 * t], half, 1), id_rows[2 * t + 1])
                fill(near_cols, lane_tile(t), pair)

            @pl.loop(0, sheet * share // LANES)
            def _(t):
                at = t * (LANES // share) + lane_row // share
                member = (at % spans) * cores + my_core
                held = member * owned + ((at // spans) * depth + lax.rem(my_plane, depth)) * share
                fill(source_cols, lane_tile(t + near_lanes // LANES), (held + lane_row % share).astype(F32))

            for load in loads[5:]:
                load.wait()

        if iteration:
            wait_fresh()
            fresh_blocks = [unfold(new_moment[k], new_moment[k + 1]) for k in range(0, stack, 2)]
            pieces = in_pieces(fresh_blocks)
            send, wait_own = scatter(own_send, own_recv, sheet_group)
            out = joined(gathered(pieces, near_lanes, sheet * share))
            for k in range(sheet):
                own_send[k] = kept(out, k)
            own_recv[pl.ds(in_sheet, 1)] = own_send[pl.ds(in_sheet, 1)]
            for step in sheet_group[3]:
                send(step)
            wait_old()
            held_old = [tree(old_recv[k, i] for k in range(sheet)) for i in range(hist_len)]

        if iteration == 0:
            for step in (1, planes - 1, far - 1, planes - far + 1, far):
                block = block_of(step)
                landed(block, step)
                pass_on(block, step not in (1, planes - 1))
        wait()
        row = total(sheet_row, sheet)
        if iteration == 0:
            entry = [[None] * (i + 1) for i in range(hist_len)]
            for i in range(hist_len):
                for j in range(i + 1):
                    r = i - j
                    at = hist_len * r + i if r < shifts else hist_len * (hist_len - r) + j
                    entry[i][j] = splat(row, at)
        else:
            news = [splat(row, k) for k in range(hist_len)]
            entry = [
                [
                    jnp.where(slot_row == i, news[j], jnp.where(slot_row == j, news[i], entry[i][j]))
                    for j in range(i + 1)
                ]
                for i in range(hist_len)
            ]
        coeffs = solve_coeffs(entry, hist_len)

        if iteration == 0:
            wait_passed()
            old = coeffs
        else:
            old = [jnp.where(slot_row == i, 0.0, coeffs[i]) for i in range(hist_len)]
            new = coeffs[0]
            for i in range(1, hist_len):
                new = jnp.where(slot_row == i, coeffs[i], new)

        coeff_col = jnp.zeros((SUBS, LANES), F32)
        for i in range(hist_len):
            coeff_col = jnp.where(sub == i, old[i], coeff_col)

        gains = [jnp.where(low_row, old[2 * pair], old[2 * pair + 1]) for pair in range(hist_len // 2)]

        def mixed(at):
            top = tree(gains[pair] * hist_all[at, pair, 0:24] for pair in range(hist_len // 2))
            end = tree(gains[pair] * hist_all[at, pair, 24:25] for pair in range(hist_len // 2))
            return jnp.concatenate([top, jnp.broadcast_to(end, (SUBS, LANES))], axis=0)

        def near_pieces(order):
            blocks = []
            for k in range(0, len(order), 2):
                one, two = mixed(order[k]), mixed(order[k + 1])
                block = jnp.where(low_wide, one, two) + pltpu.roll(jnp.where(low_wide, two, one), half, 1)
                if iteration:
                    block = block + new * unfold(new_moment[order[k]], new_moment[order[k + 1]])
                blocks.append(block)
            return in_pieces(blocks)

        split_at = 0 if iteration else early
        if split_at:
            early_sum[...] = jnp.dot(
                near_pieces(sources[:split_at]),
                mask[0 : split_at * batches, 0:near_lanes],
                preferred_element_type=F32,
            )
            wait_late()
        out = jnp.dot(
            near_pieces(sources[split_at:]),
            mask[split_at * batches :, 0:near_lanes],
            preferred_element_type=F32,
        )
        near_sum[...] = joined(out + early_sum[...] if split_at else out)

        send, wait = scatter(sent, received, sheet_group)
        for line_step in sorted(range(lines), key=lambda step: -ring(step, lines)):
            first = lax.rem(my_line + line_step, lines) * spans
            lanes = pl.ds(pl.multiple_of(first * batches, spans * batches), spans * batches)
            out = near_sum[:, lanes]
            for k in range(0, spans, 2):
                pair = fold(out[:, k * batches : (k + 2) * batches])
                sent[first + k], sent[first + k + 1] = pair
            for step in sheet_group[3]:
                if step[0] == line_step:
                    send(step)
        received[pl.ds(in_sheet, 1)] = sent[pl.ds(in_sheet, 1)]

        def base_step(step, carry):
            spans_at = [lane_tile(step * SUBS + u) for u in range(SUBS)]
            parts = [coeff_col * (rho[:, at] + mixing_beta * res[:, at]) for at in spans_at]
            base_rows[pl.ds(pl.multiple_of(step * SUBS, SUBS), SUBS), :] = column_sums(parts)
            return carry

        lax.fori_loop(0, tiles // 8, base_step, 0)

        if iteration == 0:
            @pl.loop(0, hist_len // 2)
            def _(pair):
                ones = [hist_all[k, pair, 0:24] for k in range(stack)]
                ends = [jnp.broadcast_to(hist_all[k, pair, 24:25], (SUBS, LANES)) for k in range(stack)]
                rows_of = [jnp.concatenate([ones[k], ends[k]], axis=0) for k in range(stack)]
                firsts, seconds = [], []
                for k in range(0, stack, 2):
                    one, two = rows_of[k], rows_of[k + 1]
                    firsts.append(jnp.where(low_wide, one, pltpu.roll(two, half, 1)))
                    seconds.append(jnp.where(low_wide, pltpu.roll(one, half, 1), two))
                old_pieces[pl.ds(pl.multiple_of(pair * 192, 192), 96)] = in_pieces(firsts)
                old_pieces[pl.ds(pl.multiple_of(pair * 192 + 96, 96), 96)] = in_pieces(seconds)

            send, wait_old = scatter(old_send, old_recv, sheet_group)
            for first in range(0, sheet, many):
                out = gathered(old_pieces[...], near_lanes + first * share, many * share)
                for i in range(hist_len):
                    part = joined(out[i * 96 : (i + 1) * 96])
                    for k in range(many):
                        old_send[first + k, i] = kept(part, k)
            old_recv[pl.ds(in_sheet, 1)] = old_send[pl.ds(in_sheet, 1)]
            for step in sheet_group[3]:
                send(step)

        if last:
            wait_own()
            held = new * total(own_recv, sheet) + tree(old[i] * held_old[i] for i in range(hist_len))
            chunks[pl.ds(my_share, 1)] = (held * scale)[None]
            wait_chunks = exchange(chunks, share_group)

        wait()
        summed = total(received, sheet)
        at_batch = unfold(summed, summed) * scale
        comp = lax.broadcasted_iota(jnp.int32, (32, LANES), 0)
        degree = sum((comp >= (l + 1) * (l + 1)).astype(F32) for l in range(4))
        damped = jnp.where(comp < harmonics, at_batch * (mixing_beta / (1.0 + degree)), 0.0)

        parts = []
        for b in range(batches):
            col = jnp.broadcast_to(damped[:, b : b + 1], (32, LANES))
            for t in range(b * per_batch, (b + 1) * per_batch):
                at = slice(t * LANES, (t + 1) * LANES)
                part = col[24:32] * basis[24:25, at]
                for g in range(3):
                    part = part + col[g * SUBS : (g + 1) * SUBS] * basis[g * SUBS : (g + 1) * SUBS, at]
                parts.append(part)
                if len(parts) == SUBS:
                    correct[t + 1 - SUBS : t + 1] = column_sums(parts)
                    parts = []
        density = base_rows[...] - correct[...]
        if iteration:
            density = density + new * (density_out[...] + mixing_beta * fresh[...])
        density_out[...] = density
        if last:
            wait_chunks()
            for t in range(owned // LANES):
                held = [chunks[t * each + k] for k in range(each)]
                for g in range(4):
                    tile = jnp.zeros((SUBS, LANES), F32)
                    for k in range(each):
                        tile = jnp.where(quarter == k, turn(held[k], (k - g) * 32), tile)
                    top = min(SUBS, harmonics - g * SUBS)
                    moments_out[g * SUBS : g * SUBS + top, t * LANES : (t + 1) * LANES] = tile[0:top]
        else:
            made = target[...] + coupling[...] * jnp.tanh(density) - density
            fresh[...] = made
            fresh_w[...] = made * w[...]
    for src, sem in sends:
        pltpu.make_async_copy(src, src, sem).wait()


def finish(density, moments, density_out, moments_out):
    density_out[...] = density[...]
    moments_out[...] = moments[...]


def local(weights, target, coupling, multipole_basis, rho_hist, res_hist, batch_atom, owner_slot, slot_index):
    harmonics, points = multipole_basis.shape
    hist_len = res_hist.shape[0]
    batches = batch_atom.shape[0]
    groups = lax.axis_size("grid")
    members = lax.axis_size("atom")
    lines, cores = 4, 2
    planes = groups // lines
    spans = members // cores
    stack, sheet = planes * cores, lines * spans
    shares = 4 * lines
    owned = owner_slot.shape[0] // members
    scale = 1.0 / math.sqrt(points * groups // owned)
    iters = slot_index.shape[0]
    cfg = (iters, hist_len, harmonics, batches, points // batches, owned, planes, lines, spans, cores, scale)
    tiles = points // LANES
    flat = (tiles, LANES)
    kinds = 3 * iters + 7 + (iters - 1)
    any_space = pl.BlockSpec(memory_space=pltpu.HBM)
    vmem = pl.BlockSpec(memory_space=pltpu.VMEM)
    density, moments = pl.pallas_call(
        functools.partial(kernel, cfg),
        out_shape=(jax.ShapeDtypeStruct(flat, F32), jax.ShapeDtypeStruct((harmonics, owned), F32)),
        in_specs=[any_space] * 9,
        out_specs=(vmem, vmem),
        scratch_shapes=[
            pltpu.VMEM(flat, F32),
            pltpu.VMEM(flat, F32),
            pltpu.VMEM(flat, F32),
            pltpu.VMEM((harmonics, points), F32),
            pltpu.VMEM((hist_len, points), F32),
            pltpu.VMEM((hist_len, points), F32),
            pltpu.VMEM(flat, F32),
            pltpu.VMEM(flat, F32),
            pltpu.VMEM((iters, stack, 1, LANES), F32),
            pltpu.VMEM((iters, sheet, 1, LANES), F32),
            pltpu.VMEM((sheet, 1, LANES), F32),
            pltpu.VMEM((stack, hist_len // 2, harmonics, LANES), F32),
            pltpu.VMEM((iters - 1, stack, 13, LANES), F32),
            pltpu.VMEM((iters, sheet, 13, LANES), F32),
            pltpu.VMEM((iters, sheet, 13, LANES), F32),
            pltpu.VMEM((sheet, SUBS, LANES), F32),
            pltpu.VMEM((sheet, SUBS, LANES), F32),
            pltpu.VMEM((sheet, hist_len, SUBS, LANES), F32),
            pltpu.VMEM((sheet, hist_len, SUBS, LANES), F32),
            pltpu.VMEM((hist_len * 96, stack * batches), jnp.bfloat16),
            pltpu.VMEM((2, batches // 4 * LANES, points // batches), jnp.bfloat16),
            pltpu.VMEM((96, sheet * batches), F32),
            pltpu.VMEM((32, sheet * batches), F32),
            pltpu.VMEM((shares, SUBS, LANES), F32),
            pltpu.VMEM((stack * batches, LANES), F32),
            pltpu.VMEM((stack * batches, LANES), F32),
            pltpu.VMEM((stack * batches, sheet * (batches + owned // shares)), jnp.bfloat16),
            pltpu.VMEM((batches // 4 * hist_len, LANES), F32),
            pltpu.VMEM(flat, F32),
            pltpu.VMEM(flat, F32),
            pltpu.SMEM(batch_atom.shape, jnp.int32),
            pltpu.SMEM(owner_slot.shape, jnp.int32),
            pltpu.SMEM(slot_index.shape, jnp.int32),
            pltpu.SemaphoreType.DMA((9,)),
            pltpu.SemaphoreType.DMA,
            pltpu.SemaphoreType.DMA((kinds,)),
            pltpu.SemaphoreType.DMA((kinds,)),
            pltpu.SemaphoreType.DMA((planes + 2,)),
        ],
        compiler_params=pltpu.CompilerParams(
            collective_id=0, has_side_effects=True, vmem_limit_bytes=16777216
        ),
    )(
        *(
            pltpu.with_memory_space_constraint(array, pltpu.HBM)
            for array in (
                batch_atom,
                owner_slot,
                slot_index,
                weights.reshape(flat),
                target.reshape(flat),
                coupling.reshape(flat),
                multipole_basis,
                rho_hist,
                res_hist,
            )
        )
    )
    density, moments = pl.pallas_call(
        finish,
        out_shape=(jax.ShapeDtypeStruct(flat, F32), jax.ShapeDtypeStruct((harmonics, owned), F32)),
        in_specs=[vmem] * 2,
        out_specs=(vmem, vmem),
        compiler_params=pltpu.CompilerParams(vmem_limit_bytes=1048576),
    )(density, moments)
    return density.reshape(points), moments


def solution(mesh):
    both = ("grid", "atom")
    placed = (P(both), P(both), P(both), P(None, both), P(None, both), P(None, both), P(both), P(), P())
    return jax.shard_map(
        local,
        mesh=mesh,
        in_specs=placed,
        out_specs=(P(both), P(None, "atom")),
        check_vma=False,
    )
```

```python
import functools
import math

import jax
import jax.numpy as jnp
from jax import lax
from jax.experimental import pallas as pl
from jax.experimental.pallas import tpu as pltpu
from jax.sharding import PartitionSpec as P

MESH = pl.DeviceIdType.MESH
LANES = 128
SUBS = 8
mixing_beta = 0.5
ridge_share = 0.1
F32 = jnp.float32


def solve_coeffs(entry, hist_len):
    trace = entry[0][0]
    for i in range(1, hist_len):
        trace = trace + entry[i][i]
    ridge = (ridge_share / hist_len) * trace
    low = [[entry[i][j] for j in range(i + 1)] for i in range(hist_len)]
    for i in range(hist_len):
        low[i][i] = low[i][i] + ridge
    inverse = [None] * hist_len
    factor = [[None] * hist_len for _ in range(hist_len)]
    forward = [jnp.ones_like(trace) for _ in range(hist_len)]
    for j in range(hist_len):
        inverse[j] = 1.0 / low[j][j]
        for i in range(j + 1, hist_len):
            factor[i][j] = low[i][j] * inverse[j]
        for i in range(j + 1, hist_len):
            forward[i] = forward[i] - factor[i][j] * forward[j]
            for k in range(j + 1, i + 1):
                low[i][k] = low[i][k] - factor[i][j] * low[k][j]
    backward = [forward[i] * inverse[i] for i in range(hist_len)]
    for j in reversed(range(hist_len)):
        for i in range(j):
            backward[i] = backward[i] - factor[j][i] * backward[j]
    total = backward[0]
    for i in range(1, hist_len):
        total = total + backward[i]
    return [backward[i] / total for i in range(hist_len)]


def split(x, count=3):
    pieces = []
    for _ in range(count):
        piece = x.astype(jnp.bfloat16).astype(F32)
        pieces.append(piece)
        x = x - piece
    return pieces


def kernel(
    cfg,
    batch_atom_hbm,
    owner_slot_hbm,
    slot_index_hbm,
    w_hbm,
    target_hbm,
    coupling_hbm,
    basis_hbm,
    rho_hbm,
    res_hbm,
    density_out,
    moments_out,
    w,
    target,
    coupling,
    basis,
    rho,
    res,
    fresh,
    fresh_w,
    stack_rows,
    sheet_rows,
    id_rows,
    hist_all,
    fresh_all,
    part_send,
    part_recv,
    own_send,
    own_recv,
    old_send,
    old_recv,
    old_pieces,
    basis_pieces,
    early_sum,
    near_sum,
    chunks,
    source_cols,
    near_cols,
    mask,
    hist_moments,
    base_rows,
    correct,
    batch_atom,
    owner_slot,
    slot_index,
    load_sem,
    basis_sem,
    send_sem,
    recv_sem,
    pass_sem,
):
    iters, hist_len, harmonics, batches, width, owned, planes, lines, spans, cores, scale = cfg
    tiles = w.shape[0]
    per_batch = width // LANES
    half = LANES // 2
    rows = batches // 4
    stack = planes * cores
    sheet = lines * spans
    near_lanes = sheet * batches
    shares = chunks.shape[0]
    depth = shares // lines
    share = owned // shares
    my_group = lax.axis_index("grid")
    my_member = lax.axis_index("atom")
    my_plane = lax.div(my_group, lines)
    my_line = lax.rem(my_group, lines)
    my_span = lax.div(my_member, cores)
    my_core = lax.rem(my_member, cores)
    in_stack = my_plane * cores + my_core
    in_sheet = my_line * spans + my_span
    my_share = my_line * depth + lax.rem(my_plane, depth)

    def ring(step, count):
        return min(step, count - step)

    def stack_peer(step):
        plane, core = lax.rem(my_plane + step[0], planes), lax.rem(my_core + step[1], cores)
        return plane * cores + core, (plane * lines + my_line, my_span * cores + core)

    def sheet_peer(step):
        line, span = lax.rem(my_line + step[0], lines), lax.rem(my_span + step[1], spans)
        return line * spans + span, (my_plane * lines + line, span * cores + my_core)

    def share_peer(step):
        line, plane = lax.rem(my_line + step[0], lines), lax.rem(my_plane + step[1], depth)
        device = (lax.div(my_plane, depth) * depth + plane) * lines + line, my_member
        return line * depth + plane, device

    def far_first(across, along):
        steps = [(a, b) for a in range(across) for b in range(along) if a or b]
        return sorted(steps, key=lambda step: -ring(step[0], across) - ring(step[1], along))

    stack_group = (stack, in_stack, stack_peer, far_first(planes, cores))
    sheet_group = (sheet, in_sheet, sheet_peer, far_first(lines, spans))
    share_group = (shares, my_share, share_peer, far_first(lines, depth))
    groups = (stack_group, sheet_group)
    far = planes // 2
    arrivals = [0, 1, -1] + [sign * hop for hop in range(2, far) for sign in (1, -1)] + [far]
    sources = [stack_peer((offset % planes, core))[0] for offset in arrivals for core in range(cores)]
    early = (2 * far - 3) * cores
    first_half = pl.ds(0, tiles * LANES // 2)
    second_half = pl.ds(tiles * LANES // 2, tiles * LANES // 2)
    loads = [
        pltpu.make_async_copy(src, dst, load_sem.at[k])
        for k, (src, dst) in enumerate(
            (
                (w_hbm, w),
                (res_hbm.at[:, first_half], res.at[:, first_half]),
                (res_hbm.at[:, second_half], res.at[:, second_half]),
                (batch_atom_hbm, batch_atom),
                (owner_slot_hbm, owner_slot),
                (slot_index_hbm, slot_index),
                (rho_hbm, rho),
                (target_hbm, target),
                (coupling_hbm, coupling),
            )
        )
    ]
    basis_parts = [pl.ds(k * tiles * LANES // 4, tiles * LANES // 4) for k in range(4)]
    for load in loads[:3]:
        load.start()
    barrier = pltpu.get_barrier_semaphore()
    for _, _, peer, steps in groups:
        for step in steps:
            pl.semaphore_signal(barrier, inc=1, device_id=peer(step)[1], device_id_type=MESH)
    for load in loads[3:5]:
        load.start()
    for part in basis_parts:
        pltpu.make_async_copy(basis_hbm.at[:, part], basis.at[:, part], basis_sem).start()

    lane = lax.broadcasted_iota(jnp.int32, (SUBS, LANES), 1)
    sub = lax.broadcasted_iota(jnp.int32, (SUBS, LANES), 0)
    quarter = lane // 32
    lane_row = lax.broadcasted_iota(jnp.int32, (1, LANES), 1)
    low_row = lane_row < half
    low = lax.broadcasted_iota(jnp.int32, (2 * SUBS, LANES), 1) < half
    low_wide = lax.broadcasted_iota(jnp.int32, (32, LANES), 1) < half

    def lane_tile(t):
        return pl.ds(pl.multiple_of(t * LANES, LANES), LANES)

    kinds = []
    sends = []

    def channel():
        kinds.append(len(kinds))
        return kinds[-1]

    def copy_to(src, dst, which, device, arrival=None):
        return pltpu.make_async_remote_copy(
            src_ref=src,
            dst_ref=dst,
            send_sem=send_sem.at[which],
            recv_sem=recv_sem.at[which] if arrival is None else arrival,
            device_id=device,
            device_id_type=MESH,
        )

    def drained(src, which):
        sends.append((src, send_sem.at[which]))

    def waiter(src, dst, which, count):
        drained(src.at[pl.ds(0, count)], which)

        def wait():
            arrived = dst.at[pl.ds(0, count)]
            pltpu.make_async_copy(arrived, arrived, recv_sem.at[which]).wait()

        return wait

    def exchange(buf, group):
        count, mine, peer, steps = group
        which = channel()
        for step in steps:
            copy_to(buf.at[mine], buf.at[mine], which, peer(step)[1]).start()
        return waiter(buf, buf, which, count - 1)

    def scatter(src, dst, group):
        count, mine, peer, steps = group
        which = channel()

        def send(step):
            at, device = peer(step)
            copy_to(src.at[at], dst.at[mine], which, device).start()

        return send, waiter(src, dst, which, count - 1)

    def tree(parts):
        parts = list(parts)
        while len(parts) > 1:
            parts = [parts[k] + parts[k + 1] if k + 1 < len(parts) else parts[k] for k in range(0, len(parts), 2)]
        return parts[0]

    def column_sums(parts):
        parts, gap = list(parts), SUBS // 2
        while gap:
            keep = sub % (2 * gap) < gap
            merged = []
            for one, two in zip(parts[:gap], parts[gap:]):
                if 2 * gap == SUBS:
                    merged.append(jnp.where(keep, one, two) + pltpu.roll(jnp.where(keep, two, one), gap, 0))
                else:
                    up, down = pltpu.roll(one, SUBS - gap, 0), pltpu.roll(two, gap, 0)
                    merged.append(jnp.where(keep, one, down) + jnp.where(keep, up, two))
            parts, gap = merged, gap // 2
        return parts[0]

    def total(buf, count):
        return tree(buf[k] for k in range(count))

    def splat(row, k):
        return jnp.broadcast_to(row[:, k : k + 1], (1, LANES))

    def weigh():
        @pl.loop(0, rows // 4)
        def _(step):
            for u in range(4):
                r = step * 4 + u
                xs, ys = [], []
                for q in range(4):
                    b = q * rows + r
                    at = pl.ds(pl.multiple_of(b * width, width), width)
                    xs.extend(split(res[:, at] * batch_row(w, b)))
                    end = jnp.broadcast_to(basis[24:25, at], (SUBS, width))
                    ys.append(jnp.concatenate([basis[0:24, at], end], axis=0))
                x = jnp.concatenate(xs, axis=0).astype(jnp.bfloat16)
                out = None
                for k, y in enumerate(split(jnp.concatenate(ys, axis=0), 2)):
                    y = y.astype(jnp.bfloat16)
                    basis_pieces[k, pl.ds(pl.multiple_of(r * LANES, LANES), LANES)] = y
                    part = lax.dot_general(x, y, (((1,), (1,)), ((), ())), preferred_element_type=F32)
                    out = part if out is None else out + part
                tile = jnp.zeros((SUBS, LANES), F32)
                for q in range(4):
                    block = out[24 * q : 24 * q + 8] + out[24 * q + 8 : 24 * q + 16] + out[24 * q + 16 : 24 * q + 24]
                    tile = jnp.where(quarter == q, block, tile)
                hist_moments[pl.ds(r, hist_len, stride=rows), :] = tile

    def weigh_fresh():
        x = jnp.concatenate([fresh_w[pl.ds(v, batches, stride=per_batch), :] for v in range(per_batch)], axis=1)
        x = jnp.concatenate(split(x), axis=0).astype(jnp.bfloat16)
        out = None
        for k in range(2):
            part = lax.dot_general(x, basis_pieces[k], (((1,), (1,)), ((), ())), preferred_element_type=F32)
            out = part if out is None else out + part
        made = []
        for first in range(0, rows, SUBS):
            block = jnp.zeros((SUBS, LANES), F32)
            for u in range(SUBS):
                tile = slice((first + u) * LANES, (first + u + 1) * LANES)
                for q in range(4):
                    at = [k * batches + q * rows + first for k in range(3)]
                    piece = tree(out[begin : begin + SUBS, tile] for begin in at)
                    block = jnp.where((sub == u) & (quarter == q), piece, block)
            made.append(block)
        return jnp.concatenate(made, axis=0)

    def batch_row(ref, b):
        return jnp.concatenate([ref[pl.ds(b * per_batch + v, 1), :] for v in range(per_batch)], axis=1)

    def turn(block, by):
        return pltpu.roll(block, by % LANES, 1) if by % LANES else block

    def unfold(one, two):
        low_here = low[0 : one.shape[0]]
        left = jnp.where(low_here, one, pltpu.roll(two, half, 1))
        right = jnp.where(low_here, pltpu.roll(one, half, 1), two)
        end = jnp.broadcast_to(right[12:13], (SUBS, LANES))
        return jnp.concatenate([left[0:8], right[0:8], left[8:12], right[8:12], end], axis=0)

    def fold(block):
        left = jnp.concatenate([block[0:8], block[16:21]], axis=0)
        right = jnp.concatenate([block[8:16], block[20:25]], axis=0)
        low_here = low[0 : left.shape[0]]
        return (
            jnp.where(low_here, left, pltpu.roll(right, half, 1)),
            jnp.where(low_here, pltpu.roll(left, half, 1), right),
        )

    def in_pieces(blocks):
        everywhere = jnp.concatenate(blocks, axis=1)
        return jnp.concatenate(split(everywhere), axis=0).astype(jnp.bfloat16)

    def gathered(pieces, first, count):
        return jnp.dot(pieces, mask[:, pl.ds(pl.multiple_of(first, count), count)], preferred_element_type=F32)

    def joined(out):
        return out[0:32] + out[32:64] + out[64:96]

    many = 2 * LANES // share
    each = LANES // share

    def kept(out, k):
        tile = out[:, k // each * LANES : (k // each + 1) * LANES]
        result = jnp.zeros((SUBS, LANES), F32)
        for g in range(4):
            piece = tile[g * SUBS : (g + 1) * SUBS]
            result = jnp.where(quarter == g, turn(piece, (g - k % each) * 32), result)
        return result

    shifts = hist_len // 2 + 1
    entry = None
    for iteration in range(iters):
        stack_row = stack_rows.at[iteration]
        sheet_row = sheet_rows.at[iteration]
        sent = part_send.at[iteration]
        received = part_recv.at[iteration]
        last = iteration == iters - 1

        if iteration == 0:
            loads[0].wait()
            loads[1].wait()

            def gram(step, acc):
                acc = list(acc)
                for u in range(8):
                    t = step * 8 + u
                    x = res[:, lane_tile(t)]
                    y = x * w[pl.ds(t, 1), :]
                    for r in range(shifts):
                        acc[r] = acc[r] + y * (pltpu.roll(x, r, 0) if r else x)
                return tuple(acc)

            acc = tuple(jnp.zeros((SUBS, LANES), F32) for _ in range(shifts))
            acc = lax.fori_loop(0, tiles // 16, gram, acc)
            loads[2].wait()
            acc = lax.fori_loop(tiles // 16, tiles // 8, gram, acc)
            loads[3].wait()
            loads[4].wait()
            id_row = jnp.zeros((1, LANES), F32)
            for b in range(batches):
                id_row = jnp.where(lane_row == half + b, owner_slot[batch_atom[b]].astype(F32), id_row)
            id_rows[pl.ds(in_sheet, 1)] = id_row[None]
            packed = jnp.zeros((SUBS, LANES), F32)
            for r in range(shifts):
                packed = jnp.where(lane == hist_len * r + sub, jnp.sum(acc[r], axis=1, keepdims=True), packed)
            stack_row[pl.ds(in_stack, 1)] = (jnp.sum(packed, axis=0, keepdims=True) + id_row)[None]
            pltpu.make_async_copy(basis_hbm, basis, basis_sem).wait()
            weigh()
            for load in loads[5:]:
                load.start()
            pl.semaphore_wait(barrier, sum(group[0] - 1 for group in groups))
        else:
            slot = slot_index[iteration - 1]
            slot_row = jnp.zeros((1, LANES), jnp.int32) + slot

            def refresh(step, acc):
                acc, own = acc
                sums = [acc] + [jnp.zeros((SUBS, LANES), F32) for _ in range(3)]
                for u in range(32):
                    t = step * 32 + u
                    sums[u % 4] = sums[u % 4] + fresh_w[pl.ds(t, 1), :] * res[:, lane_tile(t)]
                for u in range(0, 32, SUBS):
                    at = pl.ds(pl.multiple_of(step * 32 + u, SUBS), SUBS)
                    own = own + fresh_w[at, :] * fresh[at, :]
                return tree(sums), own

            zero = jnp.zeros((SUBS, LANES), F32)
            acc, own = lax.fori_loop(0, tiles // 32, refresh, (zero, zero))
            acc = jnp.where(sub == slot, jnp.sum(own, axis=0, keepdims=True), acc)
            packed = jnp.where(lane == sub, jnp.sum(acc, axis=1, keepdims=True), 0.0)
            stack_row[pl.ds(in_stack, 1)] = jnp.sum(packed, axis=0, keepdims=True)[None]
        wait = exchange(stack_row, stack_group)
        if iteration == 0:
            wait_ids = exchange(id_rows, sheet_group)

        if iteration == 0:
            mine = hist_all.at[in_stack]
            for pair in range(hist_len // 2):
                turned = jnp.concatenate(
                    [
                        turn(hist_moments[(2 * pair + h) * rows : (2 * pair + h + 1) * rows], -32 * q)
                        for h in range(2)
                        for q in range(4)
                    ],
                    axis=0,
                )
                mine[pair] = jnp.transpose(turned)[0:harmonics]
            passed, passed_late, across = channel(), channel(), channel()
            sibling = stack_peer((0, 1))[1]

            def block_of(step):
                return hist_all.at[stack_peer((-step % planes, 0))[0]]

            def move(block, step, arrival):
                copy_to(block, block, across, stack_peer((step % planes, 0))[1], pass_sem.at[arrival]).start()

            def landed(block, arrival):
                pltpu.make_async_copy(block, block, pass_sem.at[arrival]).wait()

            def relay(k):
                for sign in (1, -1):
                    block = block_of(sign * hops).at[parts[k]]
                    landed(block, sign * hops % planes if k else planes + (sign < 0))
                    if (sign < 0) == bool(k):
                        move(block, sign * hops, far)
                    move(block, sign * (far - 1 - hops), sign * (far - 1) % planes)
                    pass_on(block)

            def pass_on(block, late=False):
                copy_to(block, block, passed_late if late else passed, sibling).start()

            parts = [pl.ds(k * hist_len // 4, hist_len // 4) for k in range(2)]
            hops = far // 2
            for k in range(2):
                for sign in (1, -1):
                    move(mine.at[parts[k]], sign * hops, sign * hops % planes if k else planes + (sign < 0))
            for sign in (1, -1):
                move(mine, sign, sign % planes)
            pass_on(mine)
            drained(hist_all.at[pl.ds(0, planes - 1)], across)
            wait_passed = waiter(hist_all, hist_all, passed, early // cores)
            wait_late = waiter(hist_all, hist_all, passed_late, planes - early // cores)
        else:
            fresh_rows = weigh_fresh()
            first_lanes = lax.broadcasted_iota(jnp.int32, (rows, LANES), 1) < SUBS
            turned = [
                jnp.where(first_lanes, turn(fresh_rows, -32 * q - 8 * h), turn(fresh_rows, -32 * q - 8 - 4 * h))
                for h in range(2)
                for q in range(4)
            ]
            new_moment = fresh_all.at[iteration - 1]
            new_moment[pl.ds(in_stack, 1)] = jnp.transpose(jnp.concatenate(turned, axis=0))[0:13][None]
            wait_fresh = exchange(new_moment, stack_group)

        if iteration == 0:
            relay(0)
        wait()
        sheet_row[pl.ds(in_sheet, 1)] = total(stack_row, stack)[None]
        wait = exchange(sheet_row, sheet_group)

        if iteration == 0:
            relay(1)

            for cols, order in ((source_cols, range(stack)), (near_cols, sources)):
                ids = jnp.transpose(jnp.concatenate([stack_row[k] for k in order] * (LANES // stack), axis=0))
                for k in range(stack):
                    cols[k * batches : (k + 1) * batches] = jnp.broadcast_to(
                        ids[half : half + batches, k : k + 1], (batches, LANES)
                    )
            wait_ids()

            def fill(cols, lanes, wanted):
                for k in range(mask.shape[0] // (2 * SUBS)):
                    at = slice(2 * SUBS * k, 2 * SUBS * (k + 1))
                    mask[at, lanes] = jnp.where(cols[at] == wanted, 1.0, 0.0).astype(jnp.bfloat16)

            @pl.loop(0, near_lanes // LANES)
            def _(t):
                pair = jnp.where(low_row, pltpu.roll(id_rows[2 * t], half, 1), id_rows[2 * t + 1])
                fill(near_cols, lane_tile(t), pair)

            @pl.loop(0, sheet * share // LANES)
            def _(t):
                at = t * (LANES // share) + lane_row // share
                member = (at % spans) * cores + my_core
                held = member * owned + ((at // spans) * depth + lax.rem(my_plane, depth)) * share
                fill(source_cols, lane_tile(t + near_lanes // LANES), (held + lane_row % share).astype(F32))

            for load in loads[5:]:
                load.wait()

        if iteration:
            wait_fresh()
            fresh_blocks = [unfold(new_moment[k], new_moment[k + 1]) for k in range(0, stack, 2)]
            pieces = in_pieces(fresh_blocks)
            send, wait_own = scatter(own_send, own_recv, sheet_group)
            out = joined(gathered(pieces, near_lanes, sheet * share))
            for k in range(sheet):
                own_send[k] = kept(out, k)
            own_recv[pl.ds(in_sheet, 1)] = own_send[pl.ds(in_sheet, 1)]
            for step in sheet_group[3]:
                send(step)
            wait_old()
            held_old = [tree(old_recv[k, i] for k in range(sheet)) for i in range(hist_len)]

        if iteration == 0:
            for step in (1, planes - 1, far - 1, planes - far + 1, far):
                block = block_of(step)
                landed(block, step)
                pass_on(block, step not in (1, planes - 1))
        wait()
        row = total(sheet_row, sheet)
        if iteration == 0:
            entry = [[None] * (i + 1) for i in range(hist_len)]
            for i in range(hist_len):
                for j in range(i + 1):
                    r = i - j
                    at = hist_len * r + i if r < shifts else hist_len * (hist_len - r) + j
                    entry[i][j] = splat(row, at)
        else:
            news = [splat(row, k) for k in range(hist_len)]
            entry = [
                [
                    jnp.where(slot_row == i, news[j], jnp.where(slot_row == j, news[i], entry[i][j]))
                    for j in range(i + 1)
                ]
                for i in range(hist_len)
            ]
        coeffs = solve_coeffs(entry, hist_len)

        if iteration == 0:
            wait_passed()
            old = coeffs
        else:
            old = [jnp.where(slot_row == i, 0.0, coeffs[i]) for i in range(hist_len)]
            new = coeffs[0]
            for i in range(1, hist_len):
                new = jnp.where(slot_row == i, coeffs[i], new)

        coeff_col = jnp.zeros((SUBS, LANES), F32)
        for i in range(hist_len):
            coeff_col = jnp.where(sub == i, old[i], coeff_col)

        gains = [jnp.where(low_row, old[2 * pair], old[2 * pair + 1]) for pair in range(hist_len // 2)]

        def mixed(at):
            top = tree(gains[pair] * hist_all[at, pair, 0:24] for pair in range(hist_len // 2))
            end = tree(gains[pair] * hist_all[at, pair, 24:25] for pair in range(hist_len // 2))
            return jnp.concatenate([top, jnp.broadcast_to(end, (SUBS, LANES))], axis=0)

        def near_pieces(order):
            blocks = []
            for k in range(0, len(order), 2):
                one, two = mixed(order[k]), mixed(order[k + 1])
                block = jnp.where(low_wide, one, two) + pltpu.roll(jnp.where(low_wide, two, one), half, 1)
                if iteration:
                    block = block + new * unfold(new_moment[order[k]], new_moment[order[k + 1]])
                blocks.append(block)
            return in_pieces(blocks)

        split_at = 0 if iteration else early
        if split_at:
            early_sum[...] = jnp.dot(
                near_pieces(sources[:split_at]),
                mask[0 : split_at * batches, 0:near_lanes],
                preferred_element_type=F32,
            )
            wait_late()
        out = jnp.dot(
            near_pieces(sources[split_at:]),
            mask[split_at * batches :, 0:near_lanes],
            preferred_element_type=F32,
        )
        near_sum[...] = joined(out + early_sum[...] if split_at else out)

        send, wait = scatter(sent, received, sheet_group)
        for line_step in sorted(range(lines), key=lambda step: -ring(step, lines)):
            first = lax.rem(my_line + line_step, lines) * spans
            lanes = pl.ds(pl.multiple_of(first * batches, spans * batches), spans * batches)
            out = near_sum[:, lanes]
            for k in range(0, spans, 2):
                pair = fold(out[:, k * batches : (k + 2) * batches])
                sent[first + k], sent[first + k + 1] = pair
            for step in sheet_group[3]:
                if step[0] == line_step:
                    send(step)
        received[pl.ds(in_sheet, 1)] = sent[pl.ds(in_sheet, 1)]

        def base_step(step, carry):
            spans_at = [lane_tile(step * SUBS + u) for u in range(SUBS)]
            parts = [coeff_col * (rho[:, at] + mixing_beta * res[:, at]) for at in spans_at]
            base_rows[pl.ds(pl.multiple_of(step * SUBS, SUBS), SUBS), :] = column_sums(parts)
            return carry

        lax.fori_loop(0, tiles // 8, base_step, 0)

        if iteration == 0:
            @pl.loop(0, hist_len // 2)
            def _(pair):
                ones = [hist_all[k, pair, 0:24] for k in range(stack)]
                ends = [jnp.broadcast_to(hist_all[k, pair, 24:25], (SUBS, LANES)) for k in range(stack)]
                rows_of = [jnp.concatenate([ones[k], ends[k]], axis=0) for k in range(stack)]
                firsts, seconds = [], []
                for k in range(0, stack, 2):
                    one, two = rows_of[k], rows_of[k + 1]
                    firsts.append(jnp.where(low_wide, one, pltpu.roll(two, half, 1)))
                    seconds.append(jnp.where(low_wide, pltpu.roll(one, half, 1), two))
                old_pieces[pl.ds(pl.multiple_of(pair * 192, 192), 96)] = in_pieces(firsts)
                old_pieces[pl.ds(pl.multiple_of(pair * 192 + 96, 96), 96)] = in_pieces(seconds)

            send, wait_old = scatter(old_send, old_recv, sheet_group)
            for first in range(0, sheet, many):
                out = gathered(old_pieces[...], near_lanes + first * share, many * share)
                for i in range(hist_len):
                    part = joined(out[i * 96 : (i + 1) * 96])
                    for k in range(many):
                        old_send[first + k, i] = kept(part, k)
            old_recv[pl.ds(in_sheet, 1)] = old_send[pl.ds(in_sheet, 1)]
            for step in sheet_group[3]:
                send(step)

        if last:
            wait_own()
            held = new * total(own_recv, sheet) + tree(old[i] * held_old[i] for i in range(hist_len))
            chunks[pl.ds(my_share, 1)] = (held * scale)[None]
            wait_chunks = exchange(chunks, share_group)

        wait()
        summed = total(received, sheet)
        at_batch = unfold(summed, summed) * scale
        comp = lax.broadcasted_iota(jnp.int32, (32, LANES), 0)
        degree = sum((comp >= (l + 1) * (l + 1)).astype(F32) for l in range(4))
        damped = jnp.where(comp < harmonics, at_batch * (mixing_beta / (1.0 + degree)), 0.0)

        parts = []
        for b in range(batches):
            col = jnp.broadcast_to(damped[:, b : b + 1], (32, LANES))
            for t in range(b * per_batch, (b + 1) * per_batch):
                at = slice(t * LANES, (t + 1) * LANES)
                part = col[24:32] * basis[24:25, at]
                for g in range(3):
                    part = part + col[g * SUBS : (g + 1) * SUBS] * basis[g * SUBS : (g + 1) * SUBS, at]
                parts.append(part)
                if len(parts) == SUBS:
                    correct[t + 1 - SUBS : t + 1] = column_sums(parts)
                    parts = []
        density = base_rows[...] - correct[...]
        if iteration:
            density = density + new * (density_out[...] + mixing_beta * fresh[...])
        density_out[...] = density
        if last:
            wait_chunks()
            for t in range(owned // LANES):
                held = [chunks[t * each + k] for k in range(each)]
                for g in range(4):
                    tile = jnp.zeros((SUBS, LANES), F32)
                    for k in range(each):
                        tile = jnp.where(quarter == k, turn(held[k], (k - g) * 32), tile)
                    top = min(SUBS, harmonics - g * SUBS)
                    moments_out[g * SUBS : g * SUBS + top, t * LANES : (t + 1) * LANES] = tile[0:top]
        else:
            made = target[...] + coupling[...] * jnp.tanh(density) - density
            fresh[...] = made
            fresh_w[...] = made * w[...]
    for src, sem in sends:
        pltpu.make_async_copy(src, src, sem).wait()


def finish(density, moments, density_out, moments_out):
    density_out[...] = density[...]
    moments_out[...] = moments[...]


def local(weights, target, coupling, multipole_basis, rho_hist, res_hist, batch_atom, owner_slot, slot_index):
    harmonics, points = multipole_basis.shape
    hist_len = res_hist.shape[0]
    batches = batch_atom.shape[0]
    groups = lax.axis_size("grid")
    members = lax.axis_size("atom")
    lines, cores = 4, 2
    planes = groups // lines
    spans = members // cores
    stack, sheet = planes * cores, lines * spans
    shares = 4 * lines
    owned = owner_slot.shape[0] // members
    scale = 1.0 / math.sqrt(points * groups // owned)
    iters = slot_index.shape[0]
    cfg = (iters, hist_len, harmonics, batches, points // batches, owned, planes, lines, spans, cores, scale)
    tiles = points // LANES
    flat = (tiles, LANES)
    kinds = 3 * iters + 7 + (iters - 1)
    any_space = pl.BlockSpec(memory_space=pltpu.HBM)
    vmem = pl.BlockSpec(memory_space=pltpu.VMEM)
    density, moments = pl.pallas_call(
        functools.partial(kernel, cfg),
        out_shape=(jax.ShapeDtypeStruct(flat, F32), jax.ShapeDtypeStruct((harmonics, owned), F32)),
        in_specs=[any_space] * 9,
        out_specs=(vmem, vmem),
        scratch_shapes=[
            pltpu.VMEM(flat, F32),
            pltpu.VMEM(flat, F32),
            pltpu.VMEM(flat, F32),
            pltpu.VMEM((harmonics, points), F32),
            pltpu.VMEM((hist_len, points), F32),
            pltpu.VMEM((hist_len, points), F32),
            pltpu.VMEM(flat, F32),
            pltpu.VMEM(flat, F32),
            pltpu.VMEM((iters, stack, 1, LANES), F32),
            pltpu.VMEM((iters, sheet, 1, LANES), F32),
            pltpu.VMEM((sheet, 1, LANES), F32),
            pltpu.VMEM((stack, hist_len // 2, harmonics, LANES), F32),
            pltpu.VMEM((iters - 1, stack, 13, LANES), F32),
            pltpu.VMEM((iters, sheet, 13, LANES), F32),
            pltpu.VMEM((iters, sheet, 13, LANES), F32),
            pltpu.VMEM((sheet, SUBS, LANES), F32),
            pltpu.VMEM((sheet, SUBS, LANES), F32),
            pltpu.VMEM((sheet, hist_len, SUBS, LANES), F32),
            pltpu.VMEM((sheet, hist_len, SUBS, LANES), F32),
            pltpu.VMEM((hist_len * 96, stack * batches), jnp.bfloat16),
            pltpu.VMEM((2, batches // 4 * LANES, points // batches), jnp.bfloat16),
            pltpu.VMEM((96, sheet * batches), F32),
            pltpu.VMEM((32, sheet * batches), F32),
            pltpu.VMEM((shares, SUBS, LANES), F32),
            pltpu.VMEM((stack * batches, LANES), F32),
            pltpu.VMEM((stack * batches, LANES), F32),
            pltpu.VMEM((stack * batches, sheet * (batches + owned // shares)), jnp.bfloat16),
            pltpu.VMEM((batches // 4 * hist_len, LANES), F32),
            pltpu.VMEM(flat, F32),
            pltpu.VMEM(flat, F32),
            pltpu.SMEM(batch_atom.shape, jnp.int32),
            pltpu.SMEM(owner_slot.shape, jnp.int32),
            pltpu.SMEM(slot_index.shape, jnp.int32),
            pltpu.SemaphoreType.DMA((9,)),
            pltpu.SemaphoreType.DMA,
            pltpu.SemaphoreType.DMA((kinds,)),
            pltpu.SemaphoreType.DMA((kinds,)),
            pltpu.SemaphoreType.DMA((planes + 2,)),
        ],
        compiler_params=pltpu.CompilerParams(
            collective_id=0, has_side_effects=True, vmem_limit_bytes=16777216
        ),
    )(
        *(
            pltpu.with_memory_space_constraint(array, pltpu.HBM)
            for array in (
                batch_atom,
                owner_slot,
                slot_index,
                weights.reshape(flat),
                target.reshape(flat),
                coupling.reshape(flat),
                multipole_basis,
                rho_hist,
                res_hist,
            )
        )
    )
    density, moments = pl.pallas_call(
        finish,
        out_shape=(jax.ShapeDtypeStruct(flat, F32), jax.ShapeDtypeStruct((harmonics, owned), F32)),
        in_specs=[vmem] * 2,
        out_specs=(vmem, vmem),
        compiler_params=pltpu.CompilerParams(vmem_limit_bytes=1048576),
    )(density, moments)
    return density.reshape(points), moments


def solution(mesh):
    both = ("grid", "atom")
    placed = (P(both), P(both), P(both), P(None, both), P(None, both), P(None, both), P(both), P(), P())
    return jax.shard_map(
        local,
        mesh=mesh,
        in_specs=placed,
        out_specs=(P(both), P(None, "atom")),
        check_vma=False,
    )
```

```python
import functools
import math

import jax
import jax.numpy as jnp
from jax import lax
from jax.experimental import pallas as pl
from jax.experimental.pallas import tpu as pltpu
from jax.sharding import PartitionSpec as P

MESH = pl.DeviceIdType.MESH
LANES = 128
SUBS = 8
mixing_beta = 0.5
ridge_share = 0.1
F32 = jnp.float32


def solve_coeffs(entry, hist_len):
    trace = entry[0][0]
    for i in range(1, hist_len):
        trace = trace + entry[i][i]
    ridge = (ridge_share / hist_len) * trace
    low = [[entry[i][j] for j in range(i + 1)] for i in range(hist_len)]
    for i in range(hist_len):
        low[i][i] = low[i][i] + ridge
    inverse = [None] * hist_len
    factor = [[None] * hist_len for _ in range(hist_len)]
    forward = [jnp.ones_like(trace) for _ in range(hist_len)]
    for j in range(hist_len):
        inverse[j] = 1.0 / low[j][j]
        for i in range(j + 1, hist_len):
            factor[i][j] = low[i][j] * inverse[j]
        for i in range(j + 1, hist_len):
            forward[i] = forward[i] - factor[i][j] * forward[j]
            for k in range(j + 1, i + 1):
                low[i][k] = low[i][k] - factor[i][j] * low[k][j]
    backward = [forward[i] * inverse[i] for i in range(hist_len)]
    for j in reversed(range(hist_len)):
        for i in range(j):
            backward[i] = backward[i] - factor[j][i] * backward[j]
    total = backward[0]
    for i in range(1, hist_len):
        total = total + backward[i]
    return [backward[i] / total for i in range(hist_len)]


def split(x, count=2):
    pieces = []
    for _ in range(count):
        piece = x.astype(jnp.bfloat16).astype(F32)
        pieces.append(piece)
        x = x - piece
    return pieces


def kernel(
    cfg,
    batch_atom_hbm,
    owner_slot_hbm,
    slot_index_hbm,
    w_hbm,
    target_hbm,
    coupling_hbm,
    basis_hbm,
    rho_hbm,
    res_hbm,
    density_out,
    moments_out,
    w,
    target,
    coupling,
    basis,
    rho,
    res,
    fresh,
    fresh_w,
    stack_rows,
    sheet_rows,
    id_rows,
    hist_all,
    fresh_all,
    part_send,
    part_recv,
    own_send,
    own_recv,
    old_send,
    old_recv,
    old_pieces,
    basis_pieces,
    early_sum,
    near_sum,
    chunks,
    source_cols,
    near_cols,
    mask,
    hist_moments,
    base_rows,
    correct,
    batch_atom,
    owner_slot,
    slot_index,
    load_sem,
    basis_sem,
    send_sem,
    recv_sem,
    pass_sem,
):
    iters, hist_len, harmonics, batches, width, owned, planes, lines, spans, cores, scale = cfg
    tiles = w.shape[0]
    per_batch = width // LANES
    half = LANES // 2
    rows = batches // 4
    stack = planes * cores
    sheet = lines * spans
    near_lanes = sheet * batches
    shares = chunks.shape[0]
    depth = shares // lines
    share = owned // shares
    my_group = lax.axis_index("grid")
    my_member = lax.axis_index("atom")
    my_plane = lax.div(my_group, lines)
    my_line = lax.rem(my_group, lines)
    my_span = lax.div(my_member, cores)
    my_core = lax.rem(my_member, cores)
    in_stack = my_plane * cores + my_core
    in_sheet = my_line * spans + my_span
    my_share = my_line * depth + lax.rem(my_plane, depth)

    def ring(step, count):
        return min(step, count - step)

    def stack_peer(step):
        plane, core = lax.rem(my_plane + step[0], planes), lax.rem(my_core + step[1], cores)
        return plane * cores + core, (plane * lines + my_line, my_span * cores + core)

    def sheet_peer(step):
        line, span = lax.rem(my_line + step[0], lines), lax.rem(my_span + step[1], spans)
        return line * spans + span, (my_plane * lines + line, span * cores + my_core)

    def share_peer(step):
        line, plane = lax.rem(my_line + step[0], lines), lax.rem(my_plane + step[1], depth)
        device = (lax.div(my_plane, depth) * depth + plane) * lines + line, my_member
        return line * depth + plane, device

    def far_first(across, along):
        steps = [(a, b) for a in range(across) for b in range(along) if a or b]
        return sorted(steps, key=lambda step: -ring(step[0], across) - ring(step[1], along))

    stack_group = (stack, in_stack, stack_peer, far_first(planes, cores))
    sheet_group = (sheet, in_sheet, sheet_peer, far_first(lines, spans))
    share_group = (shares, my_share, share_peer, far_first(lines, depth))
    groups = (stack_group, sheet_group)
    far = planes // 2
    arrivals = [0, 1, -1] + [sign * hop for hop in range(2, far) for sign in (1, -1)] + [far]
    sources = [stack_peer((offset % planes, core))[0] for offset in arrivals for core in range(cores)]
    early = (2 * far - 3) * cores
    first_half = pl.ds(0, tiles * LANES // 2)
    second_half = pl.ds(tiles * LANES // 2, tiles * LANES // 2)
    loads = [
        pltpu.make_async_copy(src, dst, load_sem.at[k])
        for k, (src, dst) in enumerate(
            (
                (w_hbm, w),
                (res_hbm.at[:, first_half], res.at[:, first_half]),
                (res_hbm.at[:, second_half], res.at[:, second_half]),
                (batch_atom_hbm, batch_atom),
                (owner_slot_hbm, owner_slot),
                (slot_index_hbm, slot_index),
                (rho_hbm, rho),
                (target_hbm, target),
                (coupling_hbm, coupling),
            )
        )
    ]
    basis_parts = [pl.ds(k * tiles * LANES // 4, tiles * LANES // 4) for k in range(4)]
    for load in loads[:3]:
        load.start()
    barrier = pltpu.get_barrier_semaphore()
    for _, _, peer, steps in groups:
        for step in steps:
            pl.semaphore_signal(barrier, inc=1, device_id=peer(step)[1], device_id_type=MESH)
    for load in loads[3:5]:
        load.start()
    for part in basis_parts:
        pltpu.make_async_copy(basis_hbm.at[:, part], basis.at[:, part], basis_sem).start()

    lane = lax.broadcasted_iota(jnp.int32, (SUBS, LANES), 1)
    sub = lax.broadcasted_iota(jnp.int32, (SUBS, LANES), 0)
    quarter = lane // 32
    lane_row = lax.broadcasted_iota(jnp.int32, (1, LANES), 1)
    low_row = lane_row < half
    low = lax.broadcasted_iota(jnp.int32, (2 * SUBS, LANES), 1) < half
    low_wide = lax.broadcasted_iota(jnp.int32, (32, LANES), 1) < half

    def lane_tile(t):
        return pl.ds(pl.multiple_of(t * LANES, LANES), LANES)

    kinds = []
    sends = []

    def channel():
        kinds.append(len(kinds))
        return kinds[-1]

    def copy_to(src, dst, which, device, arrival=None):
        return pltpu.make_async_remote_copy(
            src_ref=src,
            dst_ref=dst,
            send_sem=send_sem.at[which],
            recv_sem=recv_sem.at[which] if arrival is None else arrival,
            device_id=device,
            device_id_type=MESH,
        )

    def drained(src, which):
        sends.append((src, send_sem.at[which]))

    def waiter(src, dst, which, count):
        drained(src.at[pl.ds(0, count)], which)

        def wait():
            arrived = dst.at[pl.ds(0, count)]
            pltpu.make_async_copy(arrived, arrived, recv_sem.at[which]).wait()

        return wait

    def exchange(buf, group):
        count, mine, peer, steps = group
        which = channel()
        for step in steps:
            copy_to(buf.at[mine], buf.at[mine], which, peer(step)[1]).start()
        return waiter(buf, buf, which, count - 1)

    def scatter(src, dst, group):
        count, mine, peer, steps = group
        which = channel()

        def send(step):
            at, device = peer(step)
            copy_to(src.at[at], dst.at[mine], which, device).start()

        return send, waiter(src, dst, which, count - 1)

    def tree(parts):
        parts = list(parts)
        while len(parts) > 1:
            parts = [parts[k] + parts[k + 1] if k + 1 < len(parts) else parts[k] for k in range(0, len(parts), 2)]
        return parts[0]

    def column_sums(parts):
        parts, gap = list(parts), SUBS // 2
        while gap:
            keep = sub % (2 * gap) < gap
            merged = []
            for one, two in zip(parts[:gap], parts[gap:]):
                if 2 * gap == SUBS:
                    merged.append(jnp.where(keep, one, two) + pltpu.roll(jnp.where(keep, two, one), gap, 0))
                else:
                    up, down = pltpu.roll(one, SUBS - gap, 0), pltpu.roll(two, gap, 0)
                    merged.append(jnp.where(keep, one, down) + jnp.where(keep, up, two))
            parts, gap = merged, gap // 2
        return parts[0]

    def total(buf, count):
        return tree(buf[k] for k in range(count))

    def splat(row, k):
        return jnp.broadcast_to(row[:, k : k + 1], (1, LANES))

    def weigh():
        @pl.loop(0, rows // 4)
        def _(step):
            for u in range(4):
                r = step * 4 + u
                xs, ys = [], []
                for q in range(4):
                    b = q * rows + r
                    at = pl.ds(pl.multiple_of(b * width, width), width)
                    xs.extend(split(res[:, at] * batch_row(w, b)))
                    end = jnp.broadcast_to(basis[24:25, at], (SUBS, width))
                    ys.append(jnp.concatenate([basis[0:24, at], end], axis=0))
                x = jnp.concatenate(xs, axis=0).astype(jnp.bfloat16)
                out = None
                for k, y in enumerate(split(jnp.concatenate(ys, axis=0))):
                    y = y.astype(jnp.bfloat16)
                    basis_pieces[k, pl.ds(pl.multiple_of(r * LANES, LANES), LANES)] = y
                    part = lax.dot_general(x, y, (((1,), (1,)), ((), ())), preferred_element_type=F32)
                    out = part if out is None else out + part
                tile = jnp.zeros((SUBS, LANES), F32)
                for q in range(4):
                    block = out[16 * q : 16 * q + 8] + out[16 * q + 8 : 16 * q + 16]
                    tile = jnp.where(quarter == q, block, tile)
                hist_moments[pl.ds(r, hist_len, stride=rows), :] = tile

    def weigh_fresh():
        x = jnp.concatenate([fresh_w[pl.ds(v, batches, stride=per_batch), :] for v in range(per_batch)], axis=1)
        x = jnp.concatenate(split(x), axis=0).astype(jnp.bfloat16)
        out = None
        for k in range(2):
            part = lax.dot_general(x, basis_pieces[k], (((1,), (1,)), ((), ())), preferred_element_type=F32)
            out = part if out is None else out + part
        made = []
        for first in range(0, rows, SUBS):
            block = jnp.zeros((SUBS, LANES), F32)
            for u in range(SUBS):
                tile = slice((first + u) * LANES, (first + u + 1) * LANES)
                for q in range(4):
                    at = [k * batches + q * rows + first for k in range(2)]
                    piece = tree(out[begin : begin + SUBS, tile] for begin in at)
                    block = jnp.where((sub == u) & (quarter == q), piece, block)
            made.append(block)
        return jnp.concatenate(made, axis=0)

    def batch_row(ref, b):
        return jnp.concatenate([ref[pl.ds(b * per_batch + v, 1), :] for v in range(per_batch)], axis=1)

    def turn(block, by):
        return pltpu.roll(block, by % LANES, 1) if by % LANES else block

    def unfold(one, two):
        low_here = low[0 : one.shape[0]]
        left = jnp.where(low_here, one, pltpu.roll(two, half, 1))
        right = jnp.where(low_here, pltpu.roll(one, half, 1), two)
        end = jnp.broadcast_to(right[12:13], (SUBS, LANES))
        return jnp.concatenate([left[0:8], right[0:8], left[8:12], right[8:12], end], axis=0)

    def fold(block):
        left = jnp.concatenate([block[0:8], block[16:21]], axis=0)
        right = jnp.concatenate([block[8:16], block[20:25]], axis=0)
        low_here = low[0 : left.shape[0]]
        return (
            jnp.where(low_here, left, pltpu.roll(right, half, 1)),
            jnp.where(low_here, pltpu.roll(left, half, 1), right),
        )

    def in_pieces(blocks):
        everywhere = jnp.concatenate(blocks, axis=1)
        return jnp.concatenate(split(everywhere), axis=0).astype(jnp.bfloat16)

    def gathered(pieces, first, count):
        return jnp.dot(pieces, mask[:, pl.ds(pl.multiple_of(first, count), count)], preferred_element_type=F32)

    def joined(out):
        return out[0:32] + out[32:64]

    many = 2 * LANES // share
    each = LANES // share

    def kept(out, k):
        tile = out[:, k // each * LANES : (k // each + 1) * LANES]
        result = jnp.zeros((SUBS, LANES), F32)
        for g in range(4):
            piece = tile[g * SUBS : (g + 1) * SUBS]
            result = jnp.where(quarter == g, turn(piece, (g - k % each) * 32), result)
        return result

    shifts = hist_len // 2 + 1
    entry = None
    for iteration in range(iters):
        stack_row = stack_rows.at[iteration]
        sheet_row = sheet_rows.at[iteration]
        sent = part_send.at[iteration]
        received = part_recv.at[iteration]
        last = iteration == iters - 1

        if iteration == 0:
            loads[0].wait()
            loads[1].wait()

            def gram(step, acc):
                acc = list(acc)
                for u in range(8):
                    t = step * 8 + u
                    x = res[:, lane_tile(t)]
                    y = x * w[pl.ds(t, 1), :]
                    for r in range(shifts):
                        acc[r] = acc[r] + y * (pltpu.roll(x, r, 0) if r else x)
                return tuple(acc)

            acc = tuple(jnp.zeros((SUBS, LANES), F32) for _ in range(shifts))
            acc = lax.fori_loop(0, tiles // 16, gram, acc)
            loads[2].wait()
            acc = lax.fori_loop(tiles // 16, tiles // 8, gram, acc)
            loads[3].wait()
            loads[4].wait()
            id_row = jnp.zeros((1, LANES), F32)
            for b in range(batches):
                id_row = jnp.where(lane_row == half + b, owner_slot[batch_atom[b]].astype(F32), id_row)
            id_rows[pl.ds(in_sheet, 1)] = id_row[None]
            packed = jnp.zeros((SUBS, LANES), F32)
            for r in range(shifts):
                packed = jnp.where(lane == hist_len * r + sub, jnp.sum(acc[r], axis=1, keepdims=True), packed)
            stack_row[pl.ds(in_stack, 1)] = (jnp.sum(packed, axis=0, keepdims=True) + id_row)[None]
            pltpu.make_async_copy(basis_hbm, basis, basis_sem).wait()
            weigh()
            for load in loads[5:]:
                load.start()
            pl.semaphore_wait(barrier, sum(group[0] - 1 for group in groups))
        else:
            slot = slot_index[iteration - 1]
            slot_row = jnp.zeros((1, LANES), jnp.int32) + slot

            def refresh(step, acc):
                acc, own = acc
                sums = [acc] + [jnp.zeros((SUBS, LANES), F32) for _ in range(3)]
                for u in range(32):
                    t = step * 32 + u
                    sums[u % 4] = sums[u % 4] + fresh_w[pl.ds(t, 1), :] * res[:, lane_tile(t)]
                for u in range(0, 32, SUBS):
                    at = pl.ds(pl.multiple_of(step * 32 + u, SUBS), SUBS)
                    own = own + fresh_w[at, :] * fresh[at, :]
                return tree(sums), own

            zero = jnp.zeros((SUBS, LANES), F32)
            acc, own = lax.fori_loop(0, tiles // 32, refresh, (zero, zero))
            acc = jnp.where(sub == slot, jnp.sum(own, axis=0, keepdims=True), acc)
            packed = jnp.where(lane == sub, jnp.sum(acc, axis=1, keepdims=True), 0.0)
            stack_row[pl.ds(in_stack, 1)] = jnp.sum(packed, axis=0, keepdims=True)[None]
        wait = exchange(stack_row, stack_group)
        if iteration == 0:
            wait_ids = exchange(id_rows, sheet_group)

        if iteration == 0:
            mine = hist_all.at[in_stack]
            for pair in range(hist_len // 2):
                turned = jnp.concatenate(
                    [
                        turn(hist_moments[(2 * pair + h) * rows : (2 * pair + h + 1) * rows], -32 * q)
                        for h in range(2)
                        for q in range(4)
                    ],
                    axis=0,
                )
                mine[pair] = jnp.transpose(turned)[0:harmonics]
            passed, passed_late, across = channel(), channel(), channel()
            sibling = stack_peer((0, 1))[1]

            def block_of(step):
                return hist_all.at[stack_peer((-step % planes, 0))[0]]

            def move(block, step, arrival):
                copy_to(block, block, across, stack_peer((step % planes, 0))[1], pass_sem.at[arrival]).start()

            def landed(block, arrival):
                pltpu.make_async_copy(block, block, pass_sem.at[arrival]).wait()

            def relay(k):
                for sign in (1, -1):
                    block = block_of(sign * hops).at[parts[k]]
                    landed(block, sign * hops % planes if k else planes + (sign < 0))
                    if (sign < 0) == bool(k):
                        move(block, sign * hops, far)
                    move(block, sign * (far - 1 - hops), sign * (far - 1) % planes)
                    pass_on(block)

            def pass_on(block, late=False):
                copy_to(block, block, passed_late if late else passed, sibling).start()

            parts = [pl.ds(k * hist_len // 4, hist_len // 4) for k in range(2)]
            hops = far // 2
            for k in range(2):
                for sign in (1, -1):
                    move(mine.at[parts[k]], sign * hops, sign * hops % planes if k else planes + (sign < 0))
            for sign in (1, -1):
                move(mine, sign, sign % planes)
            pass_on(mine)
            drained(hist_all.at[pl.ds(0, planes - 1)], across)
            wait_passed = waiter(hist_all, hist_all, passed, early // cores)
            wait_late = waiter(hist_all, hist_all, passed_late, planes - early // cores)
        else:
            fresh_rows = weigh_fresh()
            first_lanes = lax.broadcasted_iota(jnp.int32, (rows, LANES), 1) < SUBS
            turned = [
                jnp.where(first_lanes, turn(fresh_rows, -32 * q - 8 * h), turn(fresh_rows, -32 * q - 8 - 4 * h))
                for h in range(2)
                for q in range(4)
            ]
            new_moment = fresh_all.at[iteration - 1]
            new_moment[pl.ds(in_stack, 1)] = jnp.transpose(jnp.concatenate(turned, axis=0))[0:13][None]
            wait_fresh = exchange(new_moment, stack_group)

        if iteration == 0:
            relay(0)
        wait()
        sheet_row[pl.ds(in_sheet, 1)] = total(stack_row, stack)[None]
        wait = exchange(sheet_row, sheet_group)

        if iteration == 0:
            relay(1)

            for cols, order in ((source_cols, range(stack)), (near_cols, sources)):
                ids = jnp.transpose(jnp.concatenate([stack_row[k] for k in order] * (LANES // stack), axis=0))
                for k in range(stack):
                    cols[k * batches : (k + 1) * batches] = jnp.broadcast_to(
                        ids[half : half + batches, k : k + 1], (batches, LANES)
                    )
            wait_ids()

            def fill(cols, lanes, wanted):
                for k in range(mask.shape[0] // (2 * SUBS)):
                    at = slice(2 * SUBS * k, 2 * SUBS * (k + 1))
                    mask[at, lanes] = jnp.where(cols[at] == wanted, 1.0, 0.0).astype(jnp.bfloat16)

            @pl.loop(0, near_lanes // LANES)
            def _(t):
                pair = jnp.where(low_row, pltpu.roll(id_rows[2 * t], half, 1), id_rows[2 * t + 1])
                fill(near_cols, lane_tile(t), pair)

            @pl.loop(0, sheet * share // LANES)
            def _(t):
                at = t * (LANES // share) + lane_row // share
                member = (at % spans) * cores + my_core
                held = member * owned + ((at // spans) * depth + lax.rem(my_plane, depth)) * share
                fill(source_cols, lane_tile(t + near_lanes // LANES), (held + lane_row % share).astype(F32))

            for load in loads[5:]:
                load.wait()

        if iteration:
            wait_fresh()
            fresh_blocks = [unfold(new_moment[k], new_moment[k + 1]) for k in range(0, stack, 2)]
            pieces = in_pieces(fresh_blocks)
            send, wait_own = scatter(own_send, own_recv, sheet_group)
            out = joined(gathered(pieces, near_lanes, sheet * share))
            for k in range(sheet):
                own_send[k] = kept(out, k)
            own_recv[pl.ds(in_sheet, 1)] = own_send[pl.ds(in_sheet, 1)]
            for step in sheet_group[3]:
                send(step)
            wait_old()
            held_old = [tree(old_recv[k, i] for k in range(sheet)) for i in range(hist_len)]

        if iteration == 0:
            for step in (1, planes - 1, far - 1, planes - far + 1, far):
                block = block_of(step)
                landed(block, step)
                pass_on(block, step not in (1, planes - 1))
        wait()
        row = total(sheet_row, sheet)
        if iteration == 0:
            entry = [[None] * (i + 1) for i in range(hist_len)]
            for i in range(hist_len):
                for j in range(i + 1):
                    r = i - j
                    at = hist_len * r + i if r < shifts else hist_len * (hist_len - r) + j
                    entry[i][j] = splat(row, at)
        else:
            news = [splat(row, k) for k in range(hist_len)]
            entry = [
                [
                    jnp.where(slot_row == i, news[j], jnp.where(slot_row == j, news[i], entry[i][j]))
                    for j in range(i + 1)
                ]
                for i in range(hist_len)
            ]
        coeffs = solve_coeffs(entry, hist_len)

        if iteration == 0:
            wait_passed()
            old = coeffs
        else:
            old = [jnp.where(slot_row == i, 0.0, coeffs[i]) for i in range(hist_len)]
            new = coeffs[0]
            for i in range(1, hist_len):
                new = jnp.where(slot_row == i, coeffs[i], new)

        coeff_col = jnp.zeros((SUBS, LANES), F32)
        for i in range(hist_len):
            coeff_col = jnp.where(sub == i, old[i], coeff_col)

        gains = [jnp.where(low_row, old[2 * pair], old[2 * pair + 1]) for pair in range(hist_len // 2)]

        def mixed(at):
            top = tree(gains[pair] * hist_all[at, pair, 0:24] for pair in range(hist_len // 2))
            end = tree(gains[pair] * hist_all[at, pair, 24:25] for pair in range(hist_len // 2))
            return jnp.concatenate([top, jnp.broadcast_to(end, (SUBS, LANES))], axis=0)

        def near_pieces(order):
            blocks = []
            for k in range(0, len(order), 2):
                one, two = mixed(order[k]), mixed(order[k + 1])
                block = jnp.where(low_wide, one, two) + pltpu.roll(jnp.where(low_wide, two, one), half, 1)
                if iteration:
                    block = block + new * unfold(new_moment[order[k]], new_moment[order[k + 1]])
                blocks.append(block)
            return in_pieces(blocks)

        split_at = 0 if iteration else early
        if split_at:
            early_sum[...] = jnp.dot(
                near_pieces(sources[:split_at]),
                mask[0 : split_at * batches, 0:near_lanes],
                preferred_element_type=F32,
            )
            wait_late()
        out = jnp.dot(
            near_pieces(sources[split_at:]),
            mask[split_at * batches :, 0:near_lanes],
            preferred_element_type=F32,
        )
        near_sum[...] = joined(out + early_sum[...] if split_at else out)

        send, wait = scatter(sent, received, sheet_group)
        for line_step in sorted(range(lines), key=lambda step: -ring(step, lines)):
            first = lax.rem(my_line + line_step, lines) * spans
            lanes = pl.ds(pl.multiple_of(first * batches, spans * batches), spans * batches)
            out = near_sum[:, lanes]
            for k in range(0, spans, 2):
                pair = fold(out[:, k * batches : (k + 2) * batches])
                sent[first + k], sent[first + k + 1] = pair
            for step in sheet_group[3]:
                if step[0] == line_step:
                    send(step)
        received[pl.ds(in_sheet, 1)] = sent[pl.ds(in_sheet, 1)]

        def base_step(step, carry):
            spans_at = [lane_tile(step * SUBS + u) for u in range(SUBS)]
            parts = [coeff_col * (rho[:, at] + mixing_beta * res[:, at]) for at in spans_at]
            base_rows[pl.ds(pl.multiple_of(step * SUBS, SUBS), SUBS), :] = column_sums(parts)
            return carry

        lax.fori_loop(0, tiles // 8, base_step, 0)

        if iteration == 0:
            @pl.loop(0, hist_len // 2)
            def _(pair):
                ones = [hist_all[k, pair, 0:24] for k in range(stack)]
                ends = [jnp.broadcast_to(hist_all[k, pair, 24:25], (SUBS, LANES)) for k in range(stack)]
                rows_of = [jnp.concatenate([ones[k], ends[k]], axis=0) for k in range(stack)]
                firsts, seconds = [], []
                for k in range(0, stack, 2):
                    one, two = rows_of[k], rows_of[k + 1]
                    firsts.append(jnp.where(low_wide, one, pltpu.roll(two, half, 1)))
                    seconds.append(jnp.where(low_wide, pltpu.roll(one, half, 1), two))
                old_pieces[pl.ds(pl.multiple_of(pair * 128, 128), 64)] = in_pieces(firsts)
                old_pieces[pl.ds(pl.multiple_of(pair * 128 + 64, 64), 64)] = in_pieces(seconds)

            send, wait_old = scatter(old_send, old_recv, sheet_group)
            for first in range(0, sheet, many):
                out = gathered(old_pieces[...], near_lanes + first * share, many * share)
                for i in range(hist_len):
                    part = joined(out[i * 64 : (i + 1) * 64])
                    for k in range(many):
                        old_send[first + k, i] = kept(part, k)
            old_recv[pl.ds(in_sheet, 1)] = old_send[pl.ds(in_sheet, 1)]
            for step in sheet_group[3]:
                send(step)

        if last:
            wait_own()
            held = new * total(own_recv, sheet) + tree(old[i] * held_old[i] for i in range(hist_len))
            chunks[pl.ds(my_share, 1)] = (held * scale)[None]
            wait_chunks = exchange(chunks, share_group)

        wait()
        summed = total(received, sheet)
        at_batch = unfold(summed, summed) * scale
        comp = lax.broadcasted_iota(jnp.int32, (32, LANES), 0)
        degree = sum((comp >= (l + 1) * (l + 1)).astype(F32) for l in range(4))
        damped = jnp.where(comp < harmonics, at_batch * (mixing_beta / (1.0 + degree)), 0.0)

        parts = []
        for b in range(batches):
            col = jnp.broadcast_to(damped[:, b : b + 1], (32, LANES))
            for t in range(b * per_batch, (b + 1) * per_batch):
                at = slice(t * LANES, (t + 1) * LANES)
                part = col[24:32] * basis[24:25, at]
                for g in range(3):
                    part = part + col[g * SUBS : (g + 1) * SUBS] * basis[g * SUBS : (g + 1) * SUBS, at]
                parts.append(part)
                if len(parts) == SUBS:
                    correct[t + 1 - SUBS : t + 1] = column_sums(parts)
                    parts = []
        density = base_rows[...] - correct[...]
        if iteration:
            density = density + new * (density_out[...] + mixing_beta * fresh[...])
        density_out[...] = density
        if last:
            wait_chunks()
            for t in range(owned // LANES):
                held = [chunks[t * each + k] for k in range(each)]
                for g in range(4):
                    tile = jnp.zeros((SUBS, LANES), F32)
                    for k in range(each):
                        tile = jnp.where(quarter == k, turn(held[k], (k - g) * 32), tile)
                    top = min(SUBS, harmonics - g * SUBS)
                    moments_out[g * SUBS : g * SUBS + top, t * LANES : (t + 1) * LANES] = tile[0:top]
        else:
            made = target[...] + coupling[...] * jnp.tanh(density) - density
            fresh[...] = made
            fresh_w[...] = made * w[...]
    for src, sem in sends:
        pltpu.make_async_copy(src, src, sem).wait()


def finish(density, moments, density_out, moments_out):
    density_out[...] = density[...]
    moments_out[...] = moments[...]


def local(weights, target, coupling, multipole_basis, rho_hist, res_hist, batch_atom, owner_slot, slot_index):
    harmonics, points = multipole_basis.shape
    hist_len = res_hist.shape[0]
    batches = batch_atom.shape[0]
    groups = lax.axis_size("grid")
    members = lax.axis_size("atom")
    lines, cores = 4, 2
    planes = groups // lines
    spans = members // cores
    stack, sheet = planes * cores, lines * spans
    shares = 4 * lines
    owned = owner_slot.shape[0] // members
    scale = 1.0 / math.sqrt(points * groups // owned)
    iters = slot_index.shape[0]
    cfg = (iters, hist_len, harmonics, batches, points // batches, owned, planes, lines, spans, cores, scale)
    tiles = points // LANES
    flat = (tiles, LANES)
    kinds = 3 * iters + 7 + (iters - 1)
    any_space = pl.BlockSpec(memory_space=pltpu.HBM)
    vmem = pl.BlockSpec(memory_space=pltpu.VMEM)
    density, moments = pl.pallas_call(
        functools.partial(kernel, cfg),
        out_shape=(jax.ShapeDtypeStruct(flat, F32), jax.ShapeDtypeStruct((harmonics, owned), F32)),
        in_specs=[any_space] * 9,
        out_specs=(vmem, vmem),
        scratch_shapes=[
            pltpu.VMEM(flat, F32),
            pltpu.VMEM(flat, F32),
            pltpu.VMEM(flat, F32),
            pltpu.VMEM((harmonics, points), F32),
            pltpu.VMEM((hist_len, points), F32),
            pltpu.VMEM((hist_len, points), F32),
            pltpu.VMEM(flat, F32),
            pltpu.VMEM(flat, F32),
            pltpu.VMEM((iters, stack, 1, LANES), F32),
            pltpu.VMEM((iters, sheet, 1, LANES), F32),
            pltpu.VMEM((sheet, 1, LANES), F32),
            pltpu.VMEM((stack, hist_len // 2, harmonics, LANES), F32),
            pltpu.VMEM((iters - 1, stack, 13, LANES), F32),
            pltpu.VMEM((iters, sheet, 13, LANES), F32),
            pltpu.VMEM((iters, sheet, 13, LANES), F32),
            pltpu.VMEM((sheet, SUBS, LANES), F32),
            pltpu.VMEM((sheet, SUBS, LANES), F32),
            pltpu.VMEM((sheet, hist_len, SUBS, LANES), F32),
            pltpu.VMEM((sheet, hist_len, SUBS, LANES), F32),
            pltpu.VMEM((hist_len * 64, stack * batches), jnp.bfloat16),
            pltpu.VMEM((2, batches // 4 * LANES, points // batches), jnp.bfloat16),
            pltpu.VMEM((64, sheet * batches), F32),
            pltpu.VMEM((32, sheet * batches), F32),
            pltpu.VMEM((shares, SUBS, LANES), F32),
            pltpu.VMEM((stack * batches, LANES), F32),
            pltpu.VMEM((stack * batches, LANES), F32),
            pltpu.VMEM((stack * batches, sheet * (batches + owned // shares)), jnp.bfloat16),
            pltpu.VMEM((batches // 4 * hist_len, LANES), F32),
            pltpu.VMEM(flat, F32),
            pltpu.VMEM(flat, F32),
            pltpu.SMEM(batch_atom.shape, jnp.int32),
            pltpu.SMEM(owner_slot.shape, jnp.int32),
            pltpu.SMEM(slot_index.shape, jnp.int32),
            pltpu.SemaphoreType.DMA((9,)),
            pltpu.SemaphoreType.DMA,
            pltpu.SemaphoreType.DMA((kinds,)),
            pltpu.SemaphoreType.DMA((kinds,)),
            pltpu.SemaphoreType.DMA((planes + 2,)),
        ],
        compiler_params=pltpu.CompilerParams(
            collective_id=0, has_side_effects=True, vmem_limit_bytes=16777216
        ),
    )(
        *(
            pltpu.with_memory_space_constraint(array, pltpu.HBM)
            for array in (
                batch_atom,
                owner_slot,
                slot_index,
                weights.reshape(flat),
                target.reshape(flat),
                coupling.reshape(flat),
                multipole_basis,
                rho_hist,
                res_hist,
            )
        )
    )
    density, moments = pl.pallas_call(
        finish,
        out_shape=(jax.ShapeDtypeStruct(flat, F32), jax.ShapeDtypeStruct((harmonics, owned), F32)),
        in_specs=[vmem] * 2,
        out_specs=(vmem, vmem),
        compiler_params=pltpu.CompilerParams(vmem_limit_bytes=1048576),
    )(density, moments)
    return density.reshape(points), moments


def solution(mesh):
    both = ("grid", "atom")
    placed = (P(both), P(both), P(both), P(None, both), P(None, both), P(None, both), P(both), P(), P())
    return jax.shard_map(
        local,
        mesh=mesh,
        in_specs=placed,
        out_specs=(P(both), P(None, "atom")),
        check_vma=False,
    )
```
